32 devices in a mesh: fsdp: 32 (over z, y, x, core).
Axes of the slice: x: 2, y: 2, z: 4, core: 2. Of those that a mesh axis runs over, the one named last changes fastest.
Arguments:
- tokens: int32 [32, 256], P('fsdp')
- embed_table: float32 [32000, 2048], P('fsdp')
- norm_gain: float32 [2048], P('fsdp')
- w_query: float32 [2048, 2048], P('fsdp')
- w_key: float32 [2048, 256], P('fsdp')
- w_value: float32 [2048, 256], P('fsdp')
- d_query: bfloat16 [32, 256, 2048], P('fsdp')
- d_key: bfloat16 [32, 256, 256], P('fsdp')
- d_value: bfloat16 [32, 256, 256], P('fsdp')
Outputs:
- output 1: bfloat16 [32, 256, 2048], P('fsdp')
- output 2: bfloat16 [32, 256, 256], P('fsdp')
- output 3: bfloat16 [32, 256, 256], P('fsdp')
- output 4: float32 [32000, 2048], P('fsdp')
- output 5: float32 [2048], P('fsdp')
- output 6: float32 [2048, 2048], P('fsdp')
- output 7: float32 [2048, 256], P('fsdp')
- output 8: float32 [2048, 256], P('fsdp')
All inputs are finite; a program needn't handle non-finite values.
Results may differ from the reference program's by a relative error of at most 0.00411384.
Values are sent between devices in bfloat16 or wider.
A program may use at most 1 GiB of HBM per device.

```python
import math
import jax
import jax.numpy as jnp
from jax import lax

VOCAB_SIZE = 32000
MODEL_DIM = 2048
NUM_HEADS = 32
KV_HEADS = 4
HEAD_DIM = 64
BATCH_SIZE = 32
SEQ_LEN = 256


def draw_tokens(tok_key):
    num_levels = int(math.ceil(math.log2(VOCAB_SIZE)))
    level_key, id_key = jax.random.split(tok_key)
    tok_shape = (BATCH_SIZE, SEQ_LEN)
    tok_level = jax.random.randint(level_key, tok_shape, 0, num_levels + 1)
    id_upper = jnp.minimum(jnp.left_shift(jnp.ones(tok_shape, jnp.int32), tok_level), VOCAB_SIZE)
    token_ids = jax.random.randint(id_key, tok_shape, 0, id_upper)
    token_ids = token_ids.at[0, 0].set(0)
    return token_ids.at[BATCH_SIZE - 1, SEQ_LEN - 1].set(VOCAB_SIZE - 1)


def setup_inputs(seed: int = 0) -> dict:
    sub_keys = jax.random.split(jax.random.key(seed), 9)
    q_width = NUM_HEADS * HEAD_DIM
    kv_width = KV_HEADS * HEAD_DIM
    w_scale = MODEL_DIM ** -0.5
    cot_scale = (BATCH_SIZE * SEQ_LEN) ** -0.5
    act_shape = (BATCH_SIZE, SEQ_LEN)
    tokens = draw_tokens(sub_keys[0])
    embed_table = jax.random.normal(sub_keys[1], (VOCAB_SIZE, MODEL_DIM), jnp.float32)
    norm_gain = 1.0 + 0.3 * jax.random.normal(sub_keys[2], (MODEL_DIM,), jnp.float32)
    w_query = w_scale * jax.random.normal(sub_keys[3], (MODEL_DIM, q_width), jnp.float32)
    w_key = w_scale * jax.random.normal(sub_keys[4], (MODEL_DIM, kv_width), jnp.float32)
    w_value = w_scale * jax.random.normal(sub_keys[5], (MODEL_DIM, kv_width), jnp.float32)
    d_query = (cot_scale * jax.random.normal(sub_keys[6], act_shape + (q_width,), jnp.float32)).astype(jnp.bfloat16)
    d_key = (cot_scale * jax.random.normal(sub_keys[7], act_shape + (kv_width,), jnp.float32)).astype(jnp.bfloat16)
    d_value = (cot_scale * jax.random.normal(sub_keys[8], act_shape + (kv_width,), jnp.float32)).astype(jnp.bfloat16)
    return dict(tokens=tokens, embed_table=embed_table, norm_gain=norm_gain, w_query=w_query, w_key=w_key, w_value=w_value, d_query=d_query, d_key=d_key, d_value=d_value)


def reference(tokens, embed_table, norm_gain, w_query, w_key, w_value, d_query, d_key, d_value):
    w_query_bf = w_query.astype(jnp.bfloat16)
    w_key_bf = w_key.astype(jnp.bfloat16)
    w_value_bf = w_value.astype(jnp.bfloat16)

    def seq_step(acc_carry, row_in):
        grad_q, grad_k, grad_v, grad_gain = acc_carry
        tok_row, dq_row, dk_row, dv_row = row_in
        x_rows = embed_table[tok_row].astype(jnp.bfloat16).astype(jnp.float32)
        inv_rms = lax.rsqrt(jnp.mean(x_rows * x_rows, axis=-1, keepdims=True) + 1e-5)
        h_rows = x_rows * inv_rms
        normed = (h_rows * norm_gain).astype(jnp.bfloat16)
        q_rows = jnp.dot(normed, w_query_bf, preferred_element_type=jnp.float32).astype(jnp.bfloat16)
        k_rows = jnp.dot(normed, w_key_bf, preferred_element_type=jnp.float32).astype(jnp.bfloat16)
        v_rows = jnp.dot(normed, w_value_bf, preferred_element_type=jnp.float32).astype(jnp.bfloat16)
        grad_q = grad_q + jnp.dot(normed.T, dq_row, preferred_element_type=jnp.float32)
        grad_k = grad_k + jnp.dot(normed.T, dk_row, preferred_element_type=jnp.float32)
        grad_v = grad_v + jnp.dot(normed.T, dv_row, preferred_element_type=jnp.float32)
        d_normed = (jnp.dot(dq_row, w_query_bf.T, preferred_element_type=jnp.float32)
                    + jnp.dot(dk_row, w_key_bf.T, preferred_element_type=jnp.float32)
                    + jnp.dot(dv_row, w_value_bf.T, preferred_element_type=jnp.float32))
        grad_gain = grad_gain + jnp.sum(d_normed * h_rows, axis=0)
        u_rows = d_normed * norm_gain
        d_x = inv_rms * (u_rows - h_rows * jnp.mean(u_rows * h_rows, axis=-1, keepdims=True))
        return (grad_q, grad_k, grad_v, grad_gain), (q_rows, k_rows, v_rows, d_x)

    acc_init = (jnp.zeros(w_query.shape, jnp.float32), jnp.zeros(w_key.shape, jnp.float32),
                jnp.zeros(w_value.shape, jnp.float32), jnp.zeros(norm_gain.shape, jnp.float32))
    grad_sums, per_row = lax.scan(seq_step, acc_init, (tokens, d_query, d_key, d_value))
    query_proj, key_proj, value_proj, d_x_all = per_row
    d_embed = jnp.zeros(embed_table.shape, jnp.float32).at[tokens].add(d_x_all)
    grad_q, grad_k, grad_v, grad_gain = grad_sums
    return (query_proj, key_proj, value_proj, d_embed, grad_gain, grad_q, grad_k, grad_v)
```

```python
import functools

import jax
import jax.numpy as jnp
from jax import lax
from jax.experimental import pallas as pl
from jax.experimental.pallas import tpu as pltpu
from jax.sharding import PartitionSpec as P

AXIS_NAME = "fsdp"
NUM_DEV = 32
PLANE = 8
NUM_PLANES = 4
HOT_ROWS = 512
HOT_BLOCK = HOT_ROWS // NUM_DEV
ROW_GROUP = 8
CLASSES = ((0, 2, 5, 0), (2, 4, 3, 10), (4, 8, 2, 16), (8, 32, 1, 24))
SEND_GROUPS = 5
RECV_GROUPS = 48
PLANE_GROUPS = (21, 4, 3, 3)
PLANE_FIRST = (0, 21, 25, 28)
PLANE_TOTAL = 31
MESH = pl.DeviceIdType.MESH
ANY = pl.BlockSpec(memory_space=pl.ANY)
BF16_MAX = 3.3895313892515355e38


def owner_class(owner):
    for first, last, groups, start in CLASSES:
        if first <= owner < last:
            return groups, start + (owner - first) * groups


def remote(src, dst, send_sem, recv_sem, dev):
    return pltpu.make_async_remote_copy(src_ref=src, dst_ref=dst, send_sem=send_sem, recv_sem=recv_sem,
                                        device_id=(dev,), device_id_type=MESH)


def spread_kernel(tok_ref, gain_ref, tok_out, gain_out, send_sems, recv_sems, own_sems):
    me = lax.axis_index(AXIS_NAME)
    own = [pltpu.make_async_copy(tok_ref, tok_out.at[me], own_sems.at[0]),
           pltpu.make_async_copy(gain_ref, gain_out.at[me], own_sems.at[1])]
    for copy in own:
        copy.start()
    copies = []
    for step in range(1, NUM_DEV):
        dev = lax.rem(me + step, NUM_DEV)
        copies.append(remote(tok_ref, tok_out.at[me], send_sems.at[0, step], recv_sems.at[0, step], dev))
        copies.append(remote(gain_ref, gain_out.at[me], send_sems.at[1, step], recv_sems.at[1, step], dev))
    for copy in copies:
        copy.start()
    for step in range(1, NUM_DEV):
        src = lax.rem(me + NUM_DEV - step, NUM_DEV)
        remote(tok_ref, tok_out.at[src], send_sems.at[0, step], recv_sems.at[0, step], src).wait()
        remote(gain_ref, gain_out.at[src], send_sems.at[1, step], recv_sems.at[1, step], src).wait()
    for copy in own:
        copy.wait()


def rows_kernel(hot_ref, cold_ref, hot_out, cold_out, send_sems, recv_sems, hot_send, hot_recv,
                z_send, z_recv, p_send, p_recv, c_send, c_recv):
    me = lax.axis_index(AXIS_NAME)
    pos = lax.rem(me, PLANE)
    plane = me // PLANE
    core = lax.rem(me, 2)

    @pl.when(me == 0)
    def _():
        for dev in range(1, NUM_DEV):
            remote(hot_ref.at[dev], hot_out.at[dev], hot_send.at[dev], hot_recv, dev).start()
        pltpu.make_async_copy(hot_ref.at[0], hot_out.at[0], hot_recv).start()

    for first, last, groups, start in CLASSES:
        @pl.when((me >= first) & (me < last))
        def _():
            base = start + (me - first) * groups
            src_rows, dst_rows = pl.ds(0, groups), pl.ds(base, groups)
            pltpu.make_async_copy(cold_ref.at[me, src_rows], cold_out.at[dst_rows], recv_sems.at[me]).start()
            for step in range(1, NUM_DEV):
                dev = lax.rem(me + step, NUM_DEV)
                remote(cold_ref.at[dev, src_rows], cold_out.at[dst_rows], send_sems.at[step], recv_sems.at[me], dev).start()

    pltpu.make_async_copy(hot_ref.at[me], hot_out.at[me], hot_recv).wait()
    along = []
    for step in range(1, NUM_PLANES):
        dev = lax.rem(me + step * PLANE, NUM_DEV)
        along.append(remote(hot_out.at[me], hot_out.at[me], z_send.at[step], z_recv.at[step], dev))
    for copy in along:
        copy.start()
    for step in range(1, NUM_PLANES):
        src = lax.rem(me + NUM_DEV - step * PLANE, NUM_DEV)
        remote(hot_out.at[src], hot_out.at[src], z_send.at[step], z_recv.at[step], src).wait_recv()
    across = []
    for step in range(1, 4):
        dev = plane * PLANE + lax.rem(pos + 2 * step, PLANE)
        src = lax.rem(pos + PLANE - 2 * step, PLANE)
        for z in range(NUM_PLANES):
            block = hot_out.at[z * PLANE + pos]
            across.append((remote(block, block, p_send.at[step, z], p_recv.at[step, z], dev), z * PLANE + src, step, z))
    for copy, _, _, _ in across:
        copy.start()
    for _, src, step, z in across:
        block = hot_out.at[src]
        remote(block, block, p_send.at[step, z], p_recv.at[step, z], me).wait_recv()
    partner = me + 1 - 2 * core
    mine = []
    for k in range(NUM_DEV // 2):
        block = hot_out.at[2 * k + core]
        mine.append(remote(block, block, c_send.at[k], c_recv.at[k], partner))
    for copy in mine:
        copy.start()
    for k in range(NUM_DEV // 2):
        block = hot_out.at[2 * k + 1 - core]
        remote(block, block, c_send.at[k], c_recv.at[k], partner).wait_recv()

    for owner in range(NUM_DEV):
        groups, base = owner_class(owner)
        rows = cold_out.at[pl.ds(base, groups)]
        pltpu.make_async_copy(rows, rows, recv_sems.at[owner]).wait()
    for copy in along:
        copy.wait_send()
    for copy, _, _, _ in across:
        copy.wait_send()
    for copy in mine:
        copy.wait_send()
    for first, last, groups, start in CLASSES:
        @pl.when((me >= first) & (me < last))
        def _():
            rows = cold_ref.at[0, pl.ds(0, groups)]
            for step in range(1, NUM_DEV):
                pltpu.make_async_copy(rows, rows, send_sems.at[step]).wait()

    @pl.when(me == 0)
    def _():
        for dev in range(1, NUM_DEV):
            pltpu.make_async_copy(hot_ref.at[dev], hot_ref.at[dev], hot_send.at[dev]).wait()


def plane_kernel(src_ref, out_ref, send_sems, recv_sems):
    me = lax.axis_index(AXIS_NAME)
    pos = lax.rem(me, PLANE)
    base = me - pos
    own = pltpu.make_async_copy(src_ref.at[pos], out_ref.at[pos], recv_sems.at[0])
    own.start()
    copies = []
    for step in range(1, PLANE):
        peer = lax.rem(pos + step, PLANE)
        copies.append(remote(src_ref.at[peer], out_ref.at[pos], send_sems.at[step], recv_sems.at[step], base + peer))
    for copy in copies:
        copy.start()
    for step in range(1, PLANE):
        peer = lax.rem(pos + PLANE - step, PLANE)
        remote(src_ref.at[peer], out_ref.at[peer], send_sems.at[step], recv_sems.at[step], base + peer).wait()
    own.wait()


def owners_kernel(src_ref, out_ref, send_sems, recv_sems):
    me = lax.axis_index(AXIS_NAME)
    pos = lax.rem(me, PLANE)
    plane = me // PLANE
    for dst, (groups, first) in enumerate(zip(PLANE_GROUPS, PLANE_FIRST)):
        rows, into = src_ref.at[pl.ds(first, groups)], out_ref.at[plane, pl.ds(0, groups)]

        @pl.when(plane == dst)
        def _():
            pltpu.make_async_copy(rows, into, recv_sems.at[plane]).start()

        @pl.when(plane != dst)
        def _():
            remote(rows, into, send_sems.at[dst], recv_sems.at[plane], dst * PLANE + pos).start()

    for dst, (groups, first) in enumerate(zip(PLANE_GROUPS, PLANE_FIRST)):
        @pl.when(plane == dst)
        def _():
            for src in range(NUM_PLANES):
                into = out_ref.at[src, pl.ds(0, groups)]
                pltpu.make_async_copy(into, into, recv_sems.at[src]).wait()

        @pl.when(plane != dst)
        def _():
            rows = src_ref.at[pl.ds(first, groups)]
            pltpu.make_async_copy(rows, rows, send_sems.at[dst]).wait()


def collect_kernel(hot_ref, gain_ref, hot_out, gain_out, hot_send, hot_recv, send_sems, recv_sems, own_sem):
    me = lax.axis_index(AXIS_NAME)

    @pl.when(me == 0)
    def _():
        pltpu.make_async_copy(hot_ref, hot_out.at[me], hot_recv.at[0]).start()

    @pl.when(me != 0)
    def _():
        remote(hot_ref, hot_out.at[me], hot_send, hot_recv.at[me], 0).start()

    own = pltpu.make_async_copy(gain_ref.at[me], gain_out.at[me], own_sem)
    own.start()
    copies = []
    for step in range(1, NUM_DEV):
        dev = lax.rem(me + step, NUM_DEV)
        copies.append(remote(gain_ref.at[dev], gain_out.at[me], send_sems.at[step], recv_sems.at[step], dev))
    for copy in copies:
        copy.start()
    for step in range(1, NUM_DEV):
        src = lax.rem(me + NUM_DEV - step, NUM_DEV)
        remote(gain_ref.at[src], gain_out.at[src], send_sems.at[step], recv_sems.at[step], src).wait()
    own.wait()

    @pl.when(me == 0)
    def _():
        for src in range(NUM_DEV):
            pltpu.make_async_copy(hot_ref, hot_out.at[src], hot_recv.at[src]).wait()

    @pl.when(me != 0)
    def _():
        pltpu.make_async_copy(hot_ref, hot_ref, hot_send).wait()


def exchange(kernel, outs, sems, *args):
    return pl.pallas_call(
        kernel, out_shape=[jax.ShapeDtypeStruct(*out) for out in outs],
        in_specs=[ANY] * len(args), out_specs=[ANY] * len(outs),
        scratch_shapes=[pltpu.SemaphoreType.DMA(shape) if shape else pltpu.SemaphoreType.DMA for shape in sems],
        compiler_params=pltpu.CompilerParams(has_side_effects=True))(*args)


def split3(value):
    def top(v):
        return jnp.clip(lax.reduce_precision(v, 8, 7), -BF16_MAX, BF16_MAX)
    high = top(value)
    rest = value - high
    mid = top(rest)
    return [part.astype(jnp.bfloat16) for part in (high, mid, rest - mid)]


def ranks(mask):
    n = mask.shape[-1]
    lower = (jnp.arange(n)[:, None] < jnp.arange(n)[None, :]).astype(jnp.bfloat16)
    return jnp.dot(mask.astype(jnp.bfloat16), lower, preferred_element_type=jnp.float32).astype(jnp.int32)


def dot_rows(a, b):
    return lax.dot_general(a, b, (((1,), (1,)), ((), ())), preferred_element_type=jnp.float32)


def dot_tokens(a, b):
    return lax.dot_general(a, b, (((0,), (0,)), ((), ())), preferred_element_type=jnp.float32)


def norm_forward(x_rows):
    inv_rms = lax.rsqrt(jnp.mean(x_rows * x_rows, axis=-1, keepdims=True) + 1e-5)
    return inv_rms, x_rows * inv_rms


def norm_backward(d_normed, h_rows, inv_rms, gain_full):
    u_rows = d_normed * gain_full
    return inv_rms * (u_rows - h_rows * jnp.mean(u_rows * h_rows, axis=-1, keepdims=True))


def solution(mesh):
    ring = [(d, (d + 1) % NUM_DEV) for d in range(NUM_DEV)]
    plane_groups = [[z * PLANE + p for p in range(PLANE)] for z in range(NUM_PLANES)]
    column_groups = [[z * PLANE + p for z in range(NUM_PLANES)] for p in range(PLANE)]
    caps = jnp.array([owner_class(d)[0] * ROW_GROUP for d in range(NUM_DEV)], jnp.int32)
    starts = jnp.array([HOT_ROWS + owner_class(d)[1] * ROW_GROUP for d in range(NUM_DEV)], jnp.int32)
    plane_caps = jnp.array([g * ROW_GROUP for g in PLANE_GROUPS], jnp.int32)
    slot_plane = jnp.array([z for z, g in enumerate(PLANE_GROUPS) for _ in range(g * ROW_GROUP)], jnp.int32)
    slot_rank = jnp.array([c for g in PLANE_GROUPS for c in range(g * ROW_GROUP)], jnp.int32)

    def local_step(tokens, embed_shard, gain_shard, wq_shard, wk_shard, wv_shard, d_query, d_key, d_value):
        vocab_local, width = embed_shard.shape
        seq = tokens.shape[1]
        q_width, kv_width = wq_shard.shape[1], wk_shard.shape[1]
        out_width = q_width + 2 * kv_width
        block = width // NUM_DEV
        me = lax.axis_index(AXIS_NAME)
        pos, plane = me % PLANE, me // PLANE
        bf16, f32 = jnp.bfloat16, jnp.float32

        cot_mine = jnp.concatenate([d_query[0], d_key[0], d_value[0]], axis=1)
        cot_plane = lax.all_gather(cot_mine, AXIS_NAME, axis=0, tiled=True, axis_index_groups=plane_groups)
        w_mine = jnp.concatenate([wq_shard.astype(bf16), wk_shard.astype(bf16), wv_shard.astype(bf16)], axis=1)
        w_full = lax.all_gather(w_mine, AXIS_NAME, axis=0, tiled=True)

        gain_row = jnp.pad(gain_shard, (0, 128 - block))[None]
        all_tokens, gain_rows = exchange(
            spread_kernel, [((NUM_DEV, 1, seq), jnp.int32), ((NUM_DEV, 1, 128), f32)],
            [(2, NUM_DEV), (2, NUM_DEV), (2,)], tokens, gain_row)
        all_tokens = all_tokens[:, 0]
        gain_full = gain_rows[:, 0, :block].reshape(1, width)

        all_owner = all_tokens // vocab_local
        all_cold = all_tokens >= HOT_ROWS
        counts = jnp.sum((all_owner[:, :, None] == jnp.arange(NUM_DEV)) & all_cold[:, :, None], axis=1, dtype=jnp.int32)
        plane_counts = counts.reshape(NUM_PLANES, PLANE, NUM_PLANES, PLANE).sum(1)
        rows_fit = jnp.all(counts <= caps[None])
        cots_fit = jnp.all(plane_counts <= plane_caps[None, :, None])

        to_mine = (all_owner == me) & all_cold
        to_rank = ranks(to_mine)
        slots = jnp.arange(SEND_GROUPS * ROW_GROUP)
        picks = (to_rank[:, None, :] == slots[None, :, None]) & to_mine[:, None, :]
        local_ids = all_tokens - me * vocab_local
        pick_ids = jnp.sum(jnp.where(picks, local_ids[:, None, :], 0), axis=2)
        send_rows = embed_shard[pick_ids.reshape(-1)].astype(bf16)
        hot_mine = embed_shard[:HOT_ROWS].astype(bf16)
        hot_rows, cold_rows = exchange(
            rows_kernel,
            [((NUM_DEV, HOT_BLOCK, width), bf16), ((RECV_GROUPS, ROW_GROUP, width), bf16)],
            [(NUM_DEV,), (NUM_DEV,), (NUM_DEV,), (), (4,), (4,), (4, 4), (4, 4), (16,), (16,)],
            hot_mine.reshape(NUM_DEV, HOT_BLOCK, width),
            send_rows.reshape(NUM_DEV, SEND_GROUPS, ROW_GROUP, width))

        my_ids = tokens[0]
        my_owner = my_ids // vocab_local
        my_cold = my_ids >= HOT_ROWS
        before = jnp.arange(seq)[None, :] < jnp.arange(seq)[:, None]
        my_rank = jnp.sum(before & my_cold[None, :] & (my_owner[None, :] == my_owner[:, None]), axis=1, dtype=jnp.int32)

        def fetched_rows(_):
            start = jnp.sum(jnp.where(my_owner[:, None] == jnp.arange(NUM_DEV), starts[None], 0), axis=1)
            place = jnp.where(my_cold, start + my_rank, my_ids)
            table = jnp.concatenate([hot_rows.reshape(HOT_ROWS, width), cold_rows.reshape(-1, width)])
            select = (place[:, None] == jnp.arange(table.shape[0])).astype(bf16)
            return jnp.dot(select, table, preferred_element_type=f32)

        def ring_rows(_):
            def hop(_, carry):
                ids, rows = carry
                mine = ids // vocab_local == me
                own = embed_shard[jnp.where(mine, ids - me * vocab_local, 0)].astype(bf16)
                rows = jnp.where(mine[:, None], own, rows)
                return lax.ppermute(ids, AXIS_NAME, ring), lax.ppermute(rows, AXIS_NAME, ring)
            return lax.fori_loop(0, NUM_DEV, hop, (my_ids, jnp.zeros((seq, width), bf16)))[1].astype(f32)

        x_rows = lax.cond(rows_fit, fetched_rows, ring_rows, None)
        inv_rms, h_rows = norm_forward(x_rows)
        normed = (h_rows * gain_full).astype(bf16)

        slices = normed.reshape(seq, NUM_PLANES, PLANE, block).transpose(2, 0, 1, 3).reshape(PLANE, seq, NUM_PLANES * block)
        n_plane, = exchange(plane_kernel, [((PLANE, seq, NUM_PLANES * block), bf16)], [(PLANE,), (PLANE,)], slices)
        n_plane = n_plane.reshape(PLANE * seq, NUM_PLANES * block)

        plane_tokens = lax.dynamic_slice_in_dim(all_tokens, plane * PLANE, PLANE, 0).reshape(PLANE * seq)
        z_ids, block_ids = jnp.arange(NUM_PLANES * HOT_BLOCK) // HOT_BLOCK, jnp.arange(NUM_PLANES * HOT_BLOCK) % HOT_BLOCK
        hot_ids = (z_ids * PLANE + pos) * HOT_BLOCK + block_ids
        hot_select = (plane_tokens[:, None] == hot_ids[None, :]).astype(bf16)
        d_w_part = dot_tokens(n_plane, cot_plane).reshape(NUM_PLANES, block, out_width)
        hot_part = dot_tokens(hot_select, cot_plane).reshape(NUM_PLANES, HOT_BLOCK, out_width)
        parts = jnp.concatenate([d_w_part, hot_part], axis=1).reshape(-1, out_width)
        summed = lax.psum_scatter(parts, AXIS_NAME, scatter_dimension=0, tiled=True, axis_index_groups=column_groups)
        d_w, hot_cot = summed[:block], summed[block:]

        plane_owner = plane_tokens // vocab_local
        here = (plane_owner % PLANE == pos) & (plane_tokens >= HOT_ROWS)
        to_plane = (plane_owner // PLANE)[None] == jnp.arange(NUM_PLANES)[:, None]
        plane_rank = jnp.sum(jnp.where(to_plane, ranks(to_plane & here), 0), axis=0)
        pack = (here & (plane_owner // PLANE == slot_plane[:, None]) & (plane_rank == slot_rank[:, None])).astype(bf16)
        packed = jnp.dot(pack, cot_plane, preferred_element_type=f32).astype(bf16)
        got, = exchange(owners_kernel, [((NUM_PLANES, PLANE_GROUPS[0], ROW_GROUP, out_width), bf16)],
                        [(NUM_PLANES,), (NUM_PLANES,)], packed.reshape(PLANE_TOTAL, ROW_GROUP, out_width))

        from_mine = to_mine.reshape(NUM_PLANES, PLANE * seq)
        from_rank = ranks(from_mine)
        from_slots = jnp.arange(PLANE_GROUPS[0] * ROW_GROUP)
        from_picks = (from_rank[:, None, :] == from_slots[None, :, None]) & from_mine[:, None, :]
        got_ids = jnp.sum(jnp.where(from_picks, local_ids.reshape(NUM_PLANES, 1, -1), 0), axis=2).reshape(-1)
        limit = jnp.sum(jnp.where(plane == jnp.arange(NUM_PLANES), plane_caps, 0))
        got_valid = ((from_slots[None] < jnp.sum(from_mine, axis=1, dtype=jnp.int32)[:, None])
                     & (from_slots < limit)[None]).reshape(-1, 1)
        got_inv, got_h = norm_forward(embed_shard[got_ids].astype(bf16).astype(f32))
        got_dn = jnp.where(got_valid, dot_rows(got.reshape(-1, out_width), w_full), 0.0)
        got_dx = norm_backward(got_dn, got_h, got_inv, gain_full)

        my_hot = lax.dynamic_index_in_dim(hot_rows, me, 0, keepdims=False).astype(f32)
        hot_inv, hot_h = norm_forward(my_hot)
        hot_dn3 = dot_rows(jnp.concatenate(split3(hot_cot)), w_full).reshape(3, HOT_BLOCK, width)
        hot_dn = hot_dn3[0] + hot_dn3[1] + hot_dn3[2]
        hot_dx = norm_backward(hot_dn, hot_h, hot_inv, gain_full)

        gain_part = jnp.sum(got_dn * got_h, axis=0) + jnp.sum(hot_dn * hot_h, axis=0)
        gain_part = jnp.pad(gain_part.reshape(NUM_DEV, 1, block), ((0, 0), (0, 0), (0, 128 - block)))
        hot_back, gain_back = exchange(
            collect_kernel, [((NUM_DEV, HOT_BLOCK, width), f32), ((NUM_DEV, 1, 128), f32)],
            [(), (NUM_DEV,), (NUM_DEV,), (NUM_DEV,), ()], hot_dx, gain_part)

        place = ((jnp.arange(vocab_local)[:, None] == got_ids[None, :]) & got_valid[:, 0][None]).astype(bf16)
        cold_grad = jnp.dot(jnp.concatenate([place] * 3, axis=1), jnp.concatenate(split3(got_dx)), preferred_element_type=f32)

        def owner_sums(_):
            top = jnp.where(me == 0, hot_back.reshape(HOT_ROWS, width), cold_grad[:HOT_ROWS])
            return jnp.concatenate([top, cold_grad[HOT_ROWS:]]), jnp.sum(gain_back[:, 0, :block], axis=0)

        def ring_sums(_):
            d_normed = dot_rows(cot_mine, w_full)
            d_gain = lax.psum(jnp.sum(d_normed * h_rows, axis=0), AXIS_NAME)
            d_x = norm_backward(d_normed, h_rows, inv_rms, gain_full)

            def hop(_, carry):
                ids, rows, total = carry
                mine = ids // vocab_local == me
                total = total.at[jnp.where(mine, ids - me * vocab_local, vocab_local)].add(rows, mode="drop")
                return lax.ppermute(ids, AXIS_NAME, ring), lax.ppermute(rows, AXIS_NAME, ring), total
            total = lax.fori_loop(0, NUM_DEV, hop, (my_ids, d_x, jnp.zeros(embed_shard.shape, f32)))[2]
            return total, lax.dynamic_slice_in_dim(d_gain, me * block, block)

        d_embed, d_norm_gain = lax.cond(cots_fit, owner_sums, ring_sums, None)

        proj = jnp.dot(normed, w_full, preferred_element_type=f32).astype(bf16)[None]
        return (proj[..., :q_width], proj[..., q_width:q_width + kv_width], proj[..., q_width + kv_width:], d_embed, d_norm_gain,
                d_w[:, :q_width], d_w[:, q_width:q_width + kv_width], d_w[:, q_width + kv_width:])

    row_spec = P(AXIS_NAME, None)
    act_spec = P(AXIS_NAME, None, None)
    vec_spec = P(AXIS_NAME)
    return jax.shard_map(local_step, mesh=mesh,
                         in_specs=(row_spec, row_spec, vec_spec, row_spec, row_spec, row_spec, act_spec, act_spec, act_spec),
                         out_specs=(act_spec, act_spec, act_spec, row_spec, vec_spec, row_spec, row_spec, row_spec),
                         check_vma=False)
```

```python
import functools

import jax
import jax.numpy as jnp
from jax import lax
from jax.experimental import pallas as pl
from jax.experimental.pallas import tpu as pltpu
from jax.sharding import PartitionSpec as P

AXIS_NAME = "fsdp"
NUM_DEV = 32
PLANE = 8
NUM_PLANES = 4
HOT_ROWS = 512
HOT_BLOCK = HOT_ROWS // NUM_DEV
ROW_GROUP = 8
CLASSES = ((0, 2, 21, 0), (2, 4, 12, 42), (4, 8, 7, 66), (8, 16, 4, 94), (16, 32, 3, 126))
SEND_GROUPS = 21
RECV_GROUPS = 174
RANK_PAD = 256
PLANE_GROUPS = (21, 4, 3, 3)
PLANE_FIRST = (0, 21, 25, 28)
PLANE_TOTAL = 31
MESH = pl.DeviceIdType.MESH
ANY = pl.BlockSpec(memory_space=pl.ANY)
BF16_MAX = 3.3895313892515355e38


def owner_class(owner):
    for first, last, groups, start in CLASSES:
        if first <= owner < last:
            return groups, start + (owner - first) * groups


def remote(src, dst, send_sem, recv_sem, dev):
    return pltpu.make_async_remote_copy(src_ref=src, dst_ref=dst, send_sem=send_sem, recv_sem=recv_sem,
                                        device_id=(dev,), device_id_type=MESH)


def spread_kernel(src_ref, out_ref, send_sems, recv_sems, own_sem):
    me = lax.axis_index(AXIS_NAME)
    own = pltpu.make_async_copy(src_ref, out_ref.at[me], own_sem)
    own.start()
    copies = []
    for step in range(1, NUM_DEV):
        dev = lax.rem(me + step, NUM_DEV)
        copies.append(remote(src_ref, out_ref.at[me], send_sems.at[step], recv_sems.at[step], dev))
    for copy in copies:
        copy.start()
    for step in range(1, NUM_DEV):
        src = lax.rem(me + NUM_DEV - step, NUM_DEV)
        remote(src_ref, out_ref.at[src], send_sems.at[step], recv_sems.at[step], src).wait()
    own.wait()


def slice_kernel(x_ref, out_ref):
    low = lax.broadcasted_iota(jnp.int32, (x_ref.shape[0], 128), 1) < 64
    for chip in range(PLANE // 2):
        for half in range(NUM_PLANES // 2):
            at = (PLANE // 2 * 2 * half + chip) * 128
            one = x_ref[:, at:at + 128].astype(jnp.bfloat16).astype(jnp.float32)
            at += PLANE // 2 * 128
            two = x_ref[:, at:at + 128].astype(jnp.bfloat16).astype(jnp.float32)
            cols = slice(half * 128, half * 128 + 128)
            out_ref[2 * chip, :, cols] = jnp.where(low, one, pltpu.roll(two, 64, 1)).astype(jnp.bfloat16)
            out_ref[2 * chip + 1, :, cols] = jnp.where(low, pltpu.roll(one, 64, 1), two).astype(jnp.bfloat16)


def column_slices(table, rows, step):
    width = table.shape[1]
    return pl.pallas_call(
        slice_kernel, grid=(rows // step,), in_specs=[pl.BlockSpec((step, width), lambda i: (i, 0))],
        out_specs=pl.BlockSpec((PLANE, step, width // PLANE), lambda i: (0, i, 0)),
        out_shape=jax.ShapeDtypeStruct((PLANE, rows, width // PLANE), jnp.bfloat16))(table)


def rows_kernel(hot_ref, hot_inv_ref, cold_ref, cold_inv_ref, hot_out, hot_inv_out, cold_out, cold_inv_out,
                hot_send, hot_recv, pass_send, hot_inv_send, hot_inv_recv, send_sems, recv_sems, inv_send, inv_recv):
    me = lax.axis_index(AXIS_NAME)
    pos = lax.rem(me, PLANE)
    plane = me // PLANE

    @pl.when(me == 0)
    def _():
        for dev in range(1, PLANE):
            remote(hot_ref.at[dev], hot_out, hot_send.at[dev], hot_recv, dev).start()
        pltpu.make_async_copy(hot_ref.at[0], hot_out, hot_recv).start()
        for dev in range(1, NUM_DEV):
            remote(hot_inv_ref, hot_inv_out, hot_inv_send.at[dev], hot_inv_recv, dev).start()
        pltpu.make_async_copy(hot_inv_ref, hot_inv_out, hot_inv_recv).start()

    def pass_on():
        pltpu.make_async_copy(hot_out, hot_out, hot_recv).wait()

        @pl.when(plane < NUM_PLANES - 1)
        def _():
            remote(hot_out, hot_out, pass_send, hot_recv, lax.rem(me + PLANE, NUM_DEV)).start()

    @pl.when(plane == 0)
    def _():
        pass_on()

    own_inv = pltpu.make_async_copy(cold_inv_ref.at[plane], cold_inv_out.at[me], inv_recv.at[me])
    own_inv.start()
    for first, last, groups, start in CLASSES:
        @pl.when((me >= first) & (me < last))
        def _():
            src_rows, dst_rows = pl.ds(0, groups), pl.ds(start + (me - first) * groups, groups)
            pltpu.make_async_copy(cold_ref.at[pos, plane, src_rows], cold_out.at[dst_rows], recv_sems.at[me]).start()

            @pl.loop(1, NUM_DEV)
            def _(step):
                dev = lax.rem(me + step, NUM_DEV)
                remote(cold_ref.at[lax.rem(dev, PLANE), dev // PLANE, src_rows], cold_out.at[dst_rows],
                       send_sems.at[step], recv_sems.at[me], dev).start()

    @pl.loop(1, NUM_DEV)
    def _(step):
        dev = lax.rem(me + step, NUM_DEV)
        remote(cold_inv_ref.at[dev // PLANE], cold_inv_out.at[me], inv_send.at[step], inv_recv.at[me], dev).start()

    @pl.when(plane > 0)
    def _():
        pass_on()

    for owner in range(NUM_DEV):
        groups, base = owner_class(owner)
        rows = cold_out.at[pl.ds(base, groups)]
        pltpu.make_async_copy(rows, rows, recv_sems.at[owner]).wait()

    @pl.loop(0, NUM_DEV)
    def _(owner):
        pltpu.make_async_copy(cold_inv_out.at[owner], cold_inv_out.at[owner], inv_recv.at[owner]).wait()

    @pl.loop(1, NUM_DEV)
    def _(step):
        pltpu.make_async_copy(cold_inv_ref.at[0], cold_inv_ref.at[0], inv_send.at[step]).wait()

    for first, last, groups, start in CLASSES:
        @pl.when((me >= first) & (me < last))
        def _():
            rows = cold_ref.at[0, 0, pl.ds(0, groups)]

            @pl.loop(1, NUM_DEV)
            def _(step):
                pltpu.make_async_copy(rows, rows, send_sems.at[step]).wait()

    pltpu.make_async_copy(hot_inv_out, hot_inv_out, hot_inv_recv).wait()

    @pl.when(plane < NUM_PLANES - 1)
    def _():
        pltpu.make_async_copy(hot_out, hot_out, pass_send).wait()

    @pl.when(me == 0)
    def _():
        for dev in range(1, PLANE):
            pltpu.make_async_copy(hot_out, hot_out, hot_send.at[dev]).wait()
        for dev in range(1, NUM_DEV):
            pltpu.make_async_copy(hot_inv_ref, hot_inv_ref, hot_inv_send.at[dev]).wait()


def plane_kernel(src_ref, hot_ref, out_ref, hot_out, send_sems, recv_sems, hot_send, hot_recv):
    me = lax.axis_index(AXIS_NAME)
    pos = lax.rem(me, PLANE)
    base = me - pos
    own = pltpu.make_async_copy(src_ref.at[pos], out_ref.at[pos], recv_sems.at[0])
    own.start()
    copies = []
    for step in range(1, PLANE):
        peer = lax.rem(pos + step, PLANE)
        copies.append(remote(src_ref.at[peer], out_ref.at[pos], send_sems.at[step], recv_sems.at[step], base + peer))
    for copy in copies:
        copy.start()

    @pl.when(me == 0)
    def _():
        pltpu.make_async_copy(hot_ref.at[0], hot_out, hot_recv).start()
        for dev in range(1, NUM_DEV):
            remote(hot_ref.at[dev], hot_out, hot_send.at[dev], hot_recv, dev).start()

    for step in range(1, PLANE):
        peer = lax.rem(pos + PLANE - step, PLANE)
        remote(src_ref.at[peer], out_ref.at[peer], send_sems.at[step], recv_sems.at[step], base + peer).wait()
    own.wait()
    pltpu.make_async_copy(hot_out, hot_out, hot_recv).wait()

    @pl.when(me == 0)
    def _():
        for dev in range(1, NUM_DEV):
            pltpu.make_async_copy(hot_out, hot_out, hot_send.at[dev]).wait()


def owners_kernel(src_ref, out_ref, send_sems, recv_sems):
    me = lax.axis_index(AXIS_NAME)
    pos = lax.rem(me, PLANE)
    plane = me // PLANE
    for dst, (groups, first) in enumerate(zip(PLANE_GROUPS, PLANE_FIRST)):
        rows, into = src_ref.at[pl.ds(first, groups)], out_ref.at[plane, pl.ds(0, groups)]

        @pl.when(plane == dst)
        def _():
            pltpu.make_async_copy(rows, into, recv_sems.at[plane]).start()

        @pl.when(plane != dst)
        def _():
            remote(rows, into, send_sems.at[dst], recv_sems.at[plane], dst * PLANE + pos).start()

    for dst, (groups, first) in enumerate(zip(PLANE_GROUPS, PLANE_FIRST)):
        @pl.when(plane == dst)
        def _():
            for src in range(NUM_PLANES):
                into = out_ref.at[src, pl.ds(0, groups)]
                pltpu.make_async_copy(into, into, recv_sems.at[src]).wait()

        @pl.when(plane != dst)
        def _():
            rows = src_ref.at[pl.ds(first, groups)]
            pltpu.make_async_copy(rows, rows, send_sems.at[dst]).wait()


def collect_kernel(hot_ref, gain_ref, hot_out, gain_out, hot_send, hot_recv, send_sems, recv_sems, own_sem):
    me = lax.axis_index(AXIS_NAME)

    @pl.when(me == 0)
    def _():
        pltpu.make_async_copy(hot_ref, hot_out.at[me], hot_recv.at[0]).start()

    @pl.when(me != 0)
    def _():
        remote(hot_ref, hot_out.at[me], hot_send, hot_recv.at[me], 0).start()

    own = pltpu.make_async_copy(gain_ref.at[me], gain_out.at[me], own_sem)
    own.start()
    copies = []
    for step in range(1, NUM_DEV):
        dev = lax.rem(me + step, NUM_DEV)
        copies.append(remote(gain_ref.at[dev], gain_out.at[me], send_sems.at[step], recv_sems.at[step], dev))
    for copy in copies:
        copy.start()
    for step in range(1, NUM_DEV):
        src = lax.rem(me + NUM_DEV - step, NUM_DEV)
        remote(gain_ref.at[src], gain_out.at[src], send_sems.at[step], recv_sems.at[step], src).wait()
    own.wait()

    @pl.when(me == 0)
    def _():
        for src in range(NUM_DEV):
            pltpu.make_async_copy(hot_ref, hot_out.at[src], hot_recv.at[src]).wait()

    @pl.when(me != 0)
    def _():
        pltpu.make_async_copy(hot_ref, hot_ref, hot_send).wait()


def exchange(kernel, outs, sems, *args, spec=ANY, us=20):
    return pl.pallas_call(
        kernel, cost_estimate=pl.CostEstimate(flops=us * 500_000_000, bytes_accessed=1_000_000, transcendentals=0), out_shape=[jax.ShapeDtypeStruct(*out) for out in outs],
        in_specs=[spec] * len(args), out_specs=[spec] * len(outs),
        scratch_shapes=[pltpu.SemaphoreType.DMA(shape) if shape else pltpu.SemaphoreType.DMA for shape in sems],
        compiler_params=pltpu.CompilerParams(has_side_effects=True))(*args)


def split3(value):
    def top(v):
        return jnp.clip(lax.reduce_precision(v, 8, 7), -BF16_MAX, BF16_MAX)
    high = top(value)
    rest = value - high
    mid = top(rest)
    return [part.astype(jnp.bfloat16) for part in (high, mid, rest - mid)]


def ranks(mask):
    n = mask.shape[-1]
    lower = (jnp.arange(n)[:, None] < jnp.arange(n)[None, :]).astype(jnp.bfloat16)
    return jnp.dot(mask.astype(jnp.bfloat16), lower, preferred_element_type=jnp.float32).astype(jnp.int32)


def dot_rows(a, b):
    return lax.dot_general(a, b, (((1,), (1,)), ((), ())), preferred_element_type=jnp.float32)


def dot_tokens(a, b):
    return lax.dot_general(a, b, (((0,), (0,)), ((), ())), preferred_element_type=jnp.float32)


def norm_forward(x_rows):
    inv_rms = lax.rsqrt(jnp.mean(x_rows * x_rows, axis=-1, keepdims=True) + 1e-5)
    return inv_rms, x_rows * inv_rms


def norm_backward(d_normed, h_rows, inv_rms, gain_full):
    u_rows = d_normed * gain_full
    return inv_rms * (u_rows - h_rows * jnp.mean(u_rows * h_rows, axis=-1, keepdims=True))


def solution(mesh):
    ring = [(d, (d + 1) % NUM_DEV) for d in range(NUM_DEV)]
    plane_groups = [[z * PLANE + p for p in range(PLANE)] for z in range(NUM_PLANES)]
    column_groups = [[z * PLANE + p for z in range(NUM_PLANES)] for p in range(PLANE)]
    caps = jnp.array([owner_class(d)[0] * ROW_GROUP for d in range(NUM_DEV)], jnp.int32)
    starts = jnp.array([HOT_ROWS + owner_class(d)[1] * ROW_GROUP for d in range(NUM_DEV)], jnp.int32)
    slot_plane = jnp.array([z for z, g in enumerate(PLANE_GROUPS) for _ in range(g * ROW_GROUP)], jnp.int32)
    slot_rank = jnp.array([c for g in PLANE_GROUPS for c in range(g * ROW_GROUP)], jnp.int32)

    def local_step(tokens, embed_shard, gain_shard, wq_shard, wk_shard, wv_shard, d_query, d_key, d_value):
        vocab_local, width = embed_shard.shape
        seq = tokens.shape[1]
        q_width, kv_width = wq_shard.shape[1], wk_shard.shape[1]
        out_width = q_width + 2 * kv_width
        block = width // NUM_DEV
        part, plane_seq, slot_rows = width // PLANE, PLANE * seq, SEND_GROUPS * ROW_GROUP
        me = lax.axis_index(AXIS_NAME)
        pos, plane = me % PLANE, me // PLANE
        bf16, f32 = jnp.bfloat16, jnp.float32

        cot_mine = jnp.concatenate([d_query[0], d_key[0], d_value[0]], axis=1)
        cot_plane = lax.all_gather(cot_mine, AXIS_NAME, axis=0, tiled=True, axis_index_groups=plane_groups)
        w_mine = jnp.concatenate([wq_shard.astype(bf16), wk_shard.astype(bf16), wv_shard.astype(bf16)], axis=1)
        w_full = lax.all_gather(w_mine, AXIS_NAME, axis=0, tiled=True)

        message = jnp.concatenate([tokens.astype(f32), jnp.pad(gain_shard, (0, 128 - block))[None]], axis=1)
        spread, = exchange(spread_kernel, [((NUM_DEV, 1, seq + 128), f32)], [(NUM_DEV,), (NUM_DEV,), ()], message,
                           spec=pl.BlockSpec(memory_space=pltpu.VMEM))
        all_tokens = spread[:, 0, :seq].astype(jnp.int32)
        gain_full = spread[:, 0, seq:seq + block].reshape(1, width)
        my_gain = gain_full.reshape(NUM_PLANES, PLANE, block)
        my_gain = lax.dynamic_index_in_dim(my_gain, pos, 1, keepdims=False).reshape(1, part)

        all_owner = all_tokens // vocab_local
        all_cold = all_tokens >= HOT_ROWS
        counts = jnp.sum((all_owner[:, :, None] == jnp.arange(NUM_DEV)) & all_cold[:, :, None], axis=1, dtype=jnp.int32)
        fits = jnp.all(counts.reshape(NUM_PLANES, PLANE, NUM_DEV).sum(1) <= caps[None])

        from_mine = ((all_owner == me) & all_cold).reshape(NUM_PLANES, plane_seq)
        from_rank = ranks(from_mine)
        slots = jnp.arange(slot_rows)
        picks = (from_rank[:, None, :] == slots[None, :, None]) & from_mine[:, None, :]
        local_ids = (all_tokens - me * vocab_local).reshape(NUM_PLANES, 1, plane_seq)
        pick_ids = jnp.sum(jnp.where(picks, local_ids, 0), axis=2).reshape(-1)
        picked = embed_shard[pick_ids].astype(bf16)
        hot_mine = embed_shard[:HOT_ROWS].astype(bf16)
        hot_slices = column_slices(embed_shard, HOT_ROWS, 128)
        cold_slices = column_slices(picked, NUM_PLANES * slot_rows, slot_rows)
        hot_inv_mine = norm_forward(hot_mine.astype(f32))[0]
        picked_inv = norm_forward(picked.astype(f32))[0]
        hot_cols, hot_inv, cold_cols, cold_inv = exchange(
            rows_kernel,
            [((HOT_ROWS, part), bf16), ((1, HOT_ROWS), f32), ((RECV_GROUPS, ROW_GROUP, part), bf16), ((NUM_DEV, 1, RANK_PAD), f32)],
            [(PLANE,), (), (), (NUM_DEV,), (), (NUM_DEV,), (NUM_DEV,), (NUM_DEV,), (NUM_DEV,)],
            hot_slices, hot_inv_mine.reshape(1, HOT_ROWS),
            cold_slices.reshape(PLANE, NUM_PLANES, SEND_GROUPS, ROW_GROUP, part),
            jnp.pad(picked_inv.reshape(NUM_PLANES, 1, slot_rows), ((0, 0), (0, 0), (0, RANK_PAD - slot_rows))), us=60)

        plane_tokens = lax.dynamic_slice_in_dim(all_tokens, plane * PLANE, PLANE, 0).reshape(plane_seq)
        plane_owner = plane_tokens // vocab_local
        plane_cold = plane_tokens >= HOT_ROWS
        of_owner = plane_owner[None] == jnp.arange(NUM_DEV)[:, None]
        plane_rank = jnp.sum(jnp.where(of_owner, ranks(of_owner & plane_cold[None]), 0), axis=0)

        def fetched_rows(_):
            start = jnp.sum(jnp.where(of_owner, starts[:, None], 0), axis=0)
            place = jnp.where(plane_cold, start + plane_rank, plane_tokens)
            table = jnp.concatenate([hot_cols, cold_cols.reshape(-1, part)])
            select = (place[:, None] == jnp.arange(table.shape[0])).astype(bf16)
            x_cols = jnp.dot(select, table, preferred_element_type=f32)
            by_owner = jnp.dot(of_owner.astype(bf16).T, jnp.concatenate(split3(cold_inv[:, 0]), axis=1), preferred_element_type=f32)
            by_owner = by_owner.reshape(plane_seq, 3, RANK_PAD)
            by_owner = by_owner[:, 0] + by_owner[:, 1] + by_owner[:, 2]
            cold_part = jnp.sum(jnp.where(plane_rank[:, None] == jnp.arange(RANK_PAD), by_owner, 0.0), axis=1, keepdims=True)
            hot_part = jnp.sum(jnp.where(plane_tokens[:, None] == jnp.arange(HOT_ROWS), hot_inv, 0.0), axis=1, keepdims=True)
            return x_cols, jnp.where(plane_cold[:, None], cold_part, hot_part)

        def ring_cols(_):
            def hop(step, carry):
                ids, cols, inv = carry
                mine = ids // vocab_local == me
                own = embed_shard[jnp.where(mine, ids - me * vocab_local, 0)].astype(bf16)
                own_inv = norm_forward(own.astype(f32))[0]
                own = own.reshape(plane_seq, NUM_PLANES, PLANE, block)
                own = lax.dynamic_index_in_dim(own, (me + NUM_DEV - step) % PLANE, 2, keepdims=False).reshape(plane_seq, part)
                cols = jnp.where(mine[:, None], own, cols)
                inv = jnp.where(mine[:, None], own_inv, inv)
                return tuple(lax.ppermute(v, AXIS_NAME, ring) for v in (ids, cols, inv))
            start = (plane_tokens, jnp.zeros((plane_seq, part), bf16), jnp.zeros((plane_seq, 1), f32))
            _, cols, inv = lax.fori_loop(0, NUM_DEV, hop, start)
            return cols.astype(f32), inv

        x_cols, x_inv = lax.cond(fits, fetched_rows, ring_cols, None)
        n_plane = (x_cols * x_inv * my_gain).astype(bf16)

        places = jnp.arange(NUM_PLANES * HOT_BLOCK)
        hot_ids = (places // HOT_BLOCK * PLANE + pos) * HOT_BLOCK + places % HOT_BLOCK
        hot_select = plane_tokens[:, None] == hot_ids[None, :]
        here = (plane_owner % PLANE == pos) & plane_cold
        pack = here[:, None] & ((plane_owner // PLANE)[:, None] == slot_plane[None]) & (plane_rank[:, None] == slot_rank[None])
        left = jnp.concatenate([n_plane, hot_select.astype(bf16), pack.astype(bf16)], axis=1)
        product = dot_tokens(left, cot_plane)
        parts = jnp.concatenate([product[:part].reshape(NUM_PLANES, block, out_width),
                                 product[part:part + NUM_PLANES * HOT_BLOCK].reshape(NUM_PLANES, HOT_BLOCK, out_width)], axis=1)
        packed = product[part + NUM_PLANES * HOT_BLOCK:].astype(bf16)
        parts, packed, n_plane, hot_mine = lax.optimization_barrier((parts, packed, n_plane, hot_mine))
        summed = lax.psum_scatter(parts.reshape(-1, out_width), AXIS_NAME, scatter_dimension=0, tiled=True, axis_index_groups=column_groups)
        d_w, hot_cot = summed[:block], summed[block:]

        n_cols, my_hot = exchange(plane_kernel, [((PLANE, seq, part), bf16), ((HOT_BLOCK, width), bf16)],
                                  [(PLANE,), (PLANE,), (NUM_DEV,), ()], n_plane.reshape(PLANE, seq, part),
                                  hot_mine.reshape(NUM_DEV, HOT_BLOCK, width))
        normed = n_cols.reshape(PLANE, seq, NUM_PLANES, block).transpose(1, 2, 0, 3).reshape(seq, width)

        got, = exchange(owners_kernel, [((NUM_PLANES, PLANE_GROUPS[0], ROW_GROUP, out_width), bf16)],
                        [(NUM_PLANES,), (NUM_PLANES,)], packed.reshape(PLANE_TOTAL, ROW_GROUP, out_width), us=60)
        got, pick_ids, from_mine = lax.optimization_barrier((got, pick_ids, from_mine))
        my_cap = jnp.sum(jnp.where(me == jnp.arange(NUM_DEV), caps, 0))
        got_valid = ((slots[None] < jnp.sum(from_mine, axis=1, dtype=jnp.int32)[:, None]) & (slots < my_cap)[None]).reshape(-1, 1)
        got_h = picked.astype(f32) * picked_inv
        got_dn = jnp.where(got_valid, dot_rows(got.reshape(-1, out_width), w_full), 0.0)
        got_dx = norm_backward(got_dn, got_h, picked_inv, gain_full)

        my_hot_inv, hot_h = norm_forward(my_hot.astype(f32))
        hot_dn3 = dot_rows(jnp.concatenate(split3(hot_cot)), w_full).reshape(3, HOT_BLOCK, width)
        hot_dn = hot_dn3[0] + hot_dn3[1] + hot_dn3[2]
        hot_dx = norm_backward(hot_dn, hot_h, my_hot_inv, gain_full)

        gain_part = jnp.sum(got_dn * got_h, axis=0) + jnp.sum(hot_dn * hot_h, axis=0)
        gain_part = jnp.pad(gain_part.reshape(NUM_DEV, 1, block), ((0, 0), (0, 0), (0, 128 - block)))
        hot_back, gain_back = exchange(
            collect_kernel, [((NUM_DEV, HOT_BLOCK, width), f32), ((NUM_DEV, 1, 128), f32)],
            [(), (NUM_DEV,), (NUM_DEV,), (NUM_DEV,), ()], hot_dx, gain_part)

        place = ((jnp.arange(vocab_local)[:, None] == pick_ids[None, :]) & got_valid[:, 0][None]).astype(bf16)
        cold_grad = jnp.dot(jnp.concatenate([place] * 3, axis=1), jnp.concatenate(split3(got_dx)), preferred_element_type=f32)

        def owner_sums(_):
            top = jnp.where(me == 0, hot_back.reshape(HOT_ROWS, width), cold_grad[:HOT_ROWS])
            return cold_grad.at[:HOT_ROWS].set(top), jnp.sum(gain_back[:, 0, :block], axis=0)

        def ring_sums(_):
            my_ids = tokens[0]

            def fetch(_, carry):
                ids, rows = carry
                mine = ids // vocab_local == me
                own = embed_shard[jnp.where(mine, ids - me * vocab_local, 0)].astype(bf16)
                rows = jnp.where(mine[:, None], own, rows)
                return lax.ppermute(ids, AXIS_NAME, ring), lax.ppermute(rows, AXIS_NAME, ring)
            x_rows = lax.fori_loop(0, NUM_DEV, fetch, (my_ids, jnp.zeros((seq, width), bf16)))[1].astype(f32)
            inv_rms, h_rows = norm_forward(x_rows)
            d_normed = dot_rows(cot_mine, w_full)
            d_gain = lax.psum(jnp.sum(d_normed * h_rows, axis=0), AXIS_NAME)
            d_x = norm_backward(d_normed, h_rows, inv_rms, gain_full)

            def hop(_, carry):
                ids, rows, total = carry
                mine = ids // vocab_local == me
                total = total.at[jnp.where(mine, ids - me * vocab_local, vocab_local)].add(rows, mode="drop")
                return lax.ppermute(ids, AXIS_NAME, ring), lax.ppermute(rows, AXIS_NAME, ring), total
            total = lax.fori_loop(0, NUM_DEV, hop, (my_ids, d_x, jnp.zeros(embed_shard.shape, f32)))[2]
            return total, lax.dynamic_slice_in_dim(d_gain, me * block, block)

        d_embed, d_norm_gain = lax.cond(fits, owner_sums, ring_sums, None)

        proj = jnp.dot(normed, w_full, preferred_element_type=f32).astype(bf16)[None]
        return (proj[..., :q_width], proj[..., q_width:q_width + kv_width], proj[..., q_width + kv_width:], d_embed, d_norm_gain,
                d_w[:, :q_width], d_w[:, q_width:q_width + kv_width], d_w[:, q_width + kv_width:])

    row_spec = P(AXIS_NAME, None)
    act_spec = P(AXIS_NAME, None, None)
    vec_spec = P(AXIS_NAME)
    return jax.shard_map(local_step, mesh=mesh,
                         in_specs=(row_spec, row_spec, vec_spec, row_spec, row_spec, row_spec, act_spec, act_spec, act_spec),
                         out_specs=(act_spec, act_spec, act_spec, row_spec, vec_spec, row_spec, row_spec, row_spec),
                         check_vma=False)
```

```python
import functools

import jax
import jax.numpy as jnp
from jax import lax
from jax.experimental import pallas as pl
from jax.experimental.pallas import tpu as pltpu
from jax.sharding import PartitionSpec as P

AXIS_NAME = "fsdp"
NUM_DEV = 32
PLANE = 8
NUM_PLANES = 4
HOT_ROWS = 512
HOT_BLOCK = HOT_ROWS // NUM_DEV
ROW_GROUP = 8
CLASSES = ((0, 2, 21, 0), (2, 4, 12, 42), (4, 8, 7, 66), (8, 16, 4, 94), (16, 32, 3, 126))
SEND_GROUPS = 21
RECV_GROUPS = 174
RANK_PAD = 256
PLANE_GROUPS = (21, 4, 3, 3)
PLANE_FIRST = (0, 21, 25, 28)
PLANE_TOTAL = 31
MESH = pl.DeviceIdType.MESH
ANY = pl.BlockSpec(memory_space=pl.ANY)
BF16_MAX = 3.3895313892515355e38


def owner_class(owner):
    for first, last, groups, start in CLASSES:
        if first <= owner < last:
            return groups, start + (owner - first) * groups


def remote(src, dst, send_sem, recv_sem, dev):
    return pltpu.make_async_remote_copy(src_ref=src, dst_ref=dst, send_sem=send_sem, recv_sem=recv_sem,
                                        device_id=(dev,), device_id_type=MESH)


def spread_kernel(src_ref, out_ref, send_sems, recv_sems, own_sem):
    me = lax.axis_index(AXIS_NAME)
    own = pltpu.make_async_copy(src_ref, out_ref.at[me], own_sem)
    own.start()
    copies = []
    for step in range(1, NUM_DEV):
        dev = lax.rem(me + step, NUM_DEV)
        copies.append(remote(src_ref, out_ref.at[me], send_sems.at[step], recv_sems.at[step], dev))
    for copy in copies:
        copy.start()
    for step in range(1, NUM_DEV):
        src = lax.rem(me + NUM_DEV - step, NUM_DEV)
        remote(src_ref, out_ref.at[src], send_sems.at[step], recv_sems.at[step], src).wait()
    own.wait()


def slice_kernel(x_ref, out_ref):
    low = lax.broadcasted_iota(jnp.int32, (x_ref.shape[0], 128), 1) < 64
    for chip in range(PLANE // 2):
        for half in range(NUM_PLANES // 2):
            at = (PLANE // 2 * 2 * half + chip) * 128
            one = x_ref[:, at:at + 128].astype(jnp.bfloat16).astype(jnp.float32)
            at += PLANE // 2 * 128
            two = x_ref[:, at:at + 128].astype(jnp.bfloat16).astype(jnp.float32)
            cols = slice(half * 128, half * 128 + 128)
            out_ref[2 * chip, :, cols] = jnp.where(low, one, pltpu.roll(two, 64, 1)).astype(jnp.bfloat16)
            out_ref[2 * chip + 1, :, cols] = jnp.where(low, pltpu.roll(one, 64, 1), two).astype(jnp.bfloat16)


def column_slices(table, rows, step):
    width = table.shape[1]
    return pl.pallas_call(
        slice_kernel, grid=(rows // step,), in_specs=[pl.BlockSpec((step, width), lambda i: (i, 0))],
        out_specs=pl.BlockSpec((PLANE, step, width // PLANE), lambda i: (0, i, 0)),
        out_shape=jax.ShapeDtypeStruct((PLANE, rows, width // PLANE), jnp.bfloat16))(table)


def rows_kernel(hot_ref, hot_inv_ref, cold_ref, cold_inv_ref, cot_ref, sum_ref,
                hot_out, hot_inv_out, cold_out, cold_inv_out, cot_out, sum_out,
                hot_send, hot_recv, pass_send, hot_inv_send, hot_inv_recv, send_sems, recv_sems, inv_send, inv_recv,
                cot_send, cot_recv, sum_send, sum_recv):
    me = lax.axis_index(AXIS_NAME)
    pos = lax.rem(me, PLANE)
    plane = me // PLANE

    @pl.when(me == 0)
    def _():
        for dev in range(1, PLANE):
            remote(hot_ref.at[dev], hot_out, hot_send.at[dev], hot_recv, dev).start()
        pltpu.make_async_copy(hot_ref.at[0], hot_out, hot_recv).start()
        for dev in range(1, NUM_DEV):
            remote(hot_inv_ref, hot_inv_out, hot_inv_send.at[dev], hot_inv_recv, dev).start()
        pltpu.make_async_copy(hot_inv_ref, hot_inv_out, hot_inv_recv).start()

    def pass_on():
        pltpu.make_async_copy(hot_out, hot_out, hot_recv).wait()

        @pl.when(plane < NUM_PLANES - 1)
        def _():
            remote(hot_out, hot_out, pass_send, hot_recv, lax.rem(me + PLANE, NUM_DEV)).start()

    @pl.when(plane == 0)
    def _():
        pass_on()

    for dst, (groups, first) in enumerate(zip(PLANE_GROUPS, PLANE_FIRST)):
        rows, into = cot_ref.at[pl.ds(first, groups)], cot_out.at[plane, pl.ds(0, groups)]

        @pl.when(plane == dst)
        def _():
            pltpu.make_async_copy(rows, into, cot_recv.at[plane]).start()
            pltpu.make_async_copy(sum_ref.at[dst], sum_out.at[plane], sum_recv.at[plane]).start()

        @pl.when(plane != dst)
        def _():
            remote(sum_ref.at[dst], sum_out.at[plane], sum_send.at[dst], sum_recv.at[plane], dst * PLANE + pos).start()
            remote(rows, into, cot_send.at[dst], cot_recv.at[plane], dst * PLANE + pos).start()

    own_inv = pltpu.make_async_copy(cold_inv_ref.at[plane], cold_inv_out.at[me], inv_recv.at[me])
    own_inv.start()
    for first, last, groups, start in CLASSES:
        @pl.when((me >= first) & (me < last))
        def _():
            src_rows, dst_rows = pl.ds(0, groups), pl.ds(start + (me - first) * groups, groups)
            pltpu.make_async_copy(cold_ref.at[pos, plane, src_rows], cold_out.at[dst_rows], recv_sems.at[me]).start()

            @pl.loop(1, NUM_DEV)
            def _(step):
                dev = lax.rem(me + step, NUM_DEV)
                remote(cold_ref.at[lax.rem(dev, PLANE), dev // PLANE, src_rows], cold_out.at[dst_rows],
                       send_sems.at[step], recv_sems.at[me], dev).start()

    @pl.loop(1, NUM_DEV)
    def _(step):
        dev = lax.rem(me + step, NUM_DEV)
        remote(cold_inv_ref.at[dev // PLANE], cold_inv_out.at[me], inv_send.at[step], inv_recv.at[me], dev).start()

    @pl.when(plane > 0)
    def _():
        pass_on()

    for owner in range(NUM_DEV):
        groups, base = owner_class(owner)
        rows = cold_out.at[pl.ds(base, groups)]
        pltpu.make_async_copy(rows, rows, recv_sems.at[owner]).wait()

    @pl.loop(0, NUM_DEV)
    def _(owner):
        pltpu.make_async_copy(cold_inv_out.at[owner], cold_inv_out.at[owner], inv_recv.at[owner]).wait()

    @pl.loop(1, NUM_DEV)
    def _(step):
        pltpu.make_async_copy(cold_inv_ref.at[0], cold_inv_ref.at[0], inv_send.at[step]).wait()

    for first, last, groups, start in CLASSES:
        @pl.when((me >= first) & (me < last))
        def _():
            rows = cold_ref.at[0, 0, pl.ds(0, groups)]

            @pl.loop(1, NUM_DEV)
            def _(step):
                pltpu.make_async_copy(rows, rows, send_sems.at[step]).wait()

    for dst, (groups, first) in enumerate(zip(PLANE_GROUPS, PLANE_FIRST)):
        @pl.when(plane == dst)
        def _():
            for src in range(NUM_PLANES):
                into = cot_out.at[src, pl.ds(0, groups)]
                pltpu.make_async_copy(into, into, cot_recv.at[src]).wait()
                pltpu.make_async_copy(sum_out.at[src], sum_out.at[src], sum_recv.at[src]).wait()

        @pl.when(plane != dst)
        def _():
            rows = cot_ref.at[pl.ds(first, groups)]
            pltpu.make_async_copy(rows, rows, cot_send.at[dst]).wait()
            pltpu.make_async_copy(sum_ref.at[dst], sum_ref.at[dst], sum_send.at[dst]).wait()

    pltpu.make_async_copy(hot_inv_out, hot_inv_out, hot_inv_recv).wait()

    @pl.when(plane < NUM_PLANES - 1)
    def _():
        pltpu.make_async_copy(hot_out, hot_out, pass_send).wait()

    @pl.when(me == 0)
    def _():
        for dev in range(1, PLANE):
            pltpu.make_async_copy(hot_out, hot_out, hot_send.at[dev]).wait()
        for dev in range(1, NUM_DEV):
            pltpu.make_async_copy(hot_inv_ref, hot_inv_ref, hot_inv_send.at[dev]).wait()


def plane_kernel(src_ref, hot_ref, out_ref, hot_out, send_sems, recv_sems, hot_send, hot_recv):
    me = lax.axis_index(AXIS_NAME)
    pos = lax.rem(me, PLANE)
    base = me - pos
    own = pltpu.make_async_copy(src_ref.at[pos], out_ref.at[pos], recv_sems.at[0])
    own.start()
    copies = []
    for step in range(1, PLANE):
        peer = lax.rem(pos + step, PLANE)
        copies.append(remote(src_ref.at[peer], out_ref.at[pos], send_sems.at[step], recv_sems.at[step], base + peer))
    for copy in copies:
        copy.start()

    @pl.when(me == 0)
    def _():
        pltpu.make_async_copy(hot_ref.at[0], hot_out, hot_recv).start()
        for dev in range(1, NUM_DEV):
            remote(hot_ref.at[dev], hot_out, hot_send.at[dev], hot_recv, dev).start()

    for step in range(1, PLANE):
        peer = lax.rem(pos + PLANE - step, PLANE)
        remote(src_ref.at[peer], out_ref.at[peer], send_sems.at[step], recv_sems.at[step], base + peer).wait()
    own.wait()
    pltpu.make_async_copy(hot_out, hot_out, hot_recv).wait()

    @pl.when(me == 0)
    def _():
        for dev in range(1, NUM_DEV):
            pltpu.make_async_copy(hot_out, hot_out, hot_send.at[dev]).wait()


def collect_kernel(hot_ref, gain_ref, hot_out, gain_out, hot_send, hot_recv, send_sems, recv_sems, own_sem):
    me = lax.axis_index(AXIS_NAME)

    @pl.when(me == 0)
    def _():
        pltpu.make_async_copy(hot_ref, hot_out.at[me], hot_recv.at[0]).start()

    @pl.when(me != 0)
    def _():
        remote(hot_ref, hot_out.at[me], hot_send, hot_recv.at[me], 0).start()

    own = pltpu.make_async_copy(gain_ref.at[me], gain_out.at[me], own_sem)
    own.start()
    copies = []
    for step in range(1, NUM_DEV):
        dev = lax.rem(me + step, NUM_DEV)
        copies.append(remote(gain_ref.at[dev], gain_out.at[me], send_sems.at[step], recv_sems.at[step], dev))
    for copy in copies:
        copy.start()
    for step in range(1, NUM_DEV):
        src = lax.rem(me + NUM_DEV - step, NUM_DEV)
        remote(gain_ref.at[src], gain_out.at[src], send_sems.at[step], recv_sems.at[step], src).wait()
    own.wait()

    @pl.when(me == 0)
    def _():
        for src in range(NUM_DEV):
            pltpu.make_async_copy(hot_ref, hot_out.at[src], hot_recv.at[src]).wait()

    @pl.when(me != 0)
    def _():
        pltpu.make_async_copy(hot_ref, hot_ref, hot_send).wait()


def exchange(kernel, outs, sems, *args, spec=ANY, us=20):
    return pl.pallas_call(
        kernel, cost_estimate=pl.CostEstimate(flops=us * 500_000_000, bytes_accessed=1_000_000, transcendentals=0), out_shape=[jax.ShapeDtypeStruct(*out) for out in outs],
        in_specs=[spec] * len(args), out_specs=[spec] * len(outs),
        scratch_shapes=[pltpu.SemaphoreType.DMA(shape) if shape else pltpu.SemaphoreType.DMA for shape in sems],
        compiler_params=pltpu.CompilerParams(has_side_effects=True))(*args)


def split3(value):
    def top(v):
        return jnp.clip(lax.reduce_precision(v, 8, 7), -BF16_MAX, BF16_MAX)
    high = top(value)
    rest = value - high
    mid = top(rest)
    return [part.astype(jnp.bfloat16) for part in (high, mid, rest - mid)]


def ranks(mask):
    n = mask.shape[-1]
    lower = (jnp.arange(n)[:, None] < jnp.arange(n)[None, :]).astype(jnp.bfloat16)
    return jnp.dot(mask.astype(jnp.bfloat16), lower, preferred_element_type=jnp.float32).astype(jnp.int32)


def dot_rows(a, b):
    return lax.dot_general(a, b, (((1,), (1,)), ((), ())), preferred_element_type=jnp.float32)


def dot_tokens(a, b):
    return lax.dot_general(a, b, (((0,), (0,)), ((), ())), preferred_element_type=jnp.float32)


def rounded(rows):
    return lax.reduce_precision(rows, 8, 7)


def norm_forward(x_rows):
    inv_rms = lax.rsqrt(jnp.mean(x_rows * x_rows, axis=-1, keepdims=True) + 1e-5)
    return inv_rms, x_rows * inv_rms


def norm_backward(d_normed, h_rows, inv_rms, gain_full):
    u_rows = d_normed * gain_full
    return inv_rms * (u_rows - h_rows * jnp.mean(u_rows * h_rows, axis=-1, keepdims=True))


def solution(mesh):
    ring = [(d, (d + 1) % NUM_DEV) for d in range(NUM_DEV)]
    plane_groups = [[z * PLANE + p for p in range(PLANE)] for z in range(NUM_PLANES)]
    column_groups = [[z * PLANE + p for z in range(NUM_PLANES)] for p in range(PLANE)]
    caps = jnp.array([owner_class(d)[0] * ROW_GROUP for d in range(NUM_DEV)], jnp.int32)
    starts = jnp.array([HOT_ROWS + owner_class(d)[1] * ROW_GROUP for d in range(NUM_DEV)], jnp.int32)
    slot_plane = jnp.array([z for z, g in enumerate(PLANE_GROUPS) for _ in range(g * ROW_GROUP)], jnp.int32)
    slot_rank = jnp.array([c for g in PLANE_GROUPS for c in range(g * ROW_GROUP)], jnp.int32)

    def local_step(tokens, embed_shard, gain_shard, wq_shard, wk_shard, wv_shard, d_query, d_key, d_value):
        vocab_local, width = embed_shard.shape
        seq = tokens.shape[1]
        q_width, kv_width = wq_shard.shape[1], wk_shard.shape[1]
        out_width = q_width + 2 * kv_width
        block = width // NUM_DEV
        part, plane_seq, slot_rows = width // PLANE, PLANE * seq, SEND_GROUPS * ROW_GROUP
        me = lax.axis_index(AXIS_NAME)
        pos, plane = me % PLANE, me // PLANE
        bf16, f32 = jnp.bfloat16, jnp.float32

        cot_mine = jnp.concatenate([d_query[0], d_key[0], d_value[0]], axis=1)
        cot_plane = lax.all_gather(cot_mine, AXIS_NAME, axis=0, tiled=True, axis_index_groups=plane_groups)
        w_mine = jnp.concatenate([wq_shard.astype(bf16), wk_shard.astype(bf16), wv_shard.astype(bf16)], axis=1)
        w_full = lax.all_gather(w_mine, AXIS_NAME, axis=0, tiled=True)

        message = jnp.concatenate([tokens.astype(f32), jnp.pad(gain_shard, (0, 128 - block))[None]], axis=1)
        spread, = exchange(spread_kernel, [((NUM_DEV, 1, seq + 128), f32)], [(NUM_DEV,), (NUM_DEV,), ()], message,
                           spec=pl.BlockSpec(memory_space=pltpu.VMEM))
        all_tokens = spread[:, 0, :seq].astype(jnp.int32)
        gain_full = spread[:, 0, seq:seq + block].reshape(1, width)
        my_gain = gain_full.reshape(NUM_PLANES, PLANE, block)
        my_gain = lax.dynamic_index_in_dim(my_gain, pos, 1, keepdims=False).reshape(1, part)

        all_owner = all_tokens // vocab_local
        all_cold = all_tokens >= HOT_ROWS
        counts = jnp.sum((all_owner[:, :, None] == jnp.arange(NUM_DEV)) & all_cold[:, :, None], axis=1, dtype=jnp.int32)
        fits = jnp.all(counts.reshape(NUM_PLANES, PLANE, NUM_DEV).sum(1) <= caps[None])

        plane_tokens = lax.dynamic_slice_in_dim(all_tokens, plane * PLANE, PLANE, 0).reshape(plane_seq)
        plane_owner = plane_tokens // vocab_local
        plane_cold = plane_tokens >= HOT_ROWS
        of_owner = plane_owner[None] == jnp.arange(NUM_DEV)[:, None]
        plane_rank = jnp.sum(jnp.where(of_owner, ranks(of_owner & plane_cold[None]), 0), axis=0)

        places = jnp.arange(NUM_PLANES * HOT_BLOCK)
        hot_ids = (places // HOT_BLOCK * PLANE + pos) * HOT_BLOCK + places % HOT_BLOCK
        hot_select = plane_tokens[:, None] == hot_ids[None, :]
        here = (plane_owner % PLANE == pos) & plane_cold
        pack = here[:, None] & ((plane_owner // PLANE)[:, None] == slot_plane[None]) & (plane_rank[:, None] == slot_rank[None])
        cot_sums = dot_tokens(hot_select.astype(bf16), cot_plane).reshape(NUM_PLANES, HOT_BLOCK, out_width)
        packed = dot_tokens(pack.astype(bf16), cot_plane).astype(bf16)

        from_mine = ((all_owner == me) & all_cold).reshape(NUM_PLANES, plane_seq)
        from_rank = ranks(from_mine)
        slots = jnp.arange(slot_rows)
        picks = (from_rank[:, None, :] == slots[None, :, None]) & from_mine[:, None, :]
        local_ids = (all_tokens - me * vocab_local).reshape(NUM_PLANES, 1, plane_seq)
        pick_ids = jnp.sum(jnp.where(picks, local_ids, 0), axis=2).reshape(-1)
        picked = rounded(embed_shard[pick_ids]).astype(bf16)
        hot_mine = rounded(embed_shard[:HOT_ROWS]).astype(bf16)
        hot_slices = column_slices(embed_shard, HOT_ROWS, 128)
        cold_slices = column_slices(picked, NUM_PLANES * slot_rows, slot_rows)
        hot_inv_mine = norm_forward(hot_mine.astype(f32))[0]
        picked_inv = norm_forward(picked.astype(f32))[0]
        hot_cols, hot_inv, cold_cols, cold_inv, got, hot_sums = exchange(
            rows_kernel,
            [((HOT_ROWS, part), bf16), ((1, HOT_ROWS), f32), ((RECV_GROUPS, ROW_GROUP, part), bf16), ((NUM_DEV, 1, RANK_PAD), f32),
             ((NUM_PLANES, SEND_GROUPS, ROW_GROUP, out_width), bf16), ((NUM_PLANES, HOT_BLOCK, out_width), f32)],
            [(PLANE,), (), (), (NUM_DEV,), (), (NUM_DEV,), (NUM_DEV,), (NUM_DEV,), (NUM_DEV,)] + [(NUM_PLANES,)] * 4,
            hot_slices, hot_inv_mine.reshape(1, HOT_ROWS),
            cold_slices.reshape(PLANE, NUM_PLANES, SEND_GROUPS, ROW_GROUP, part),
            jnp.pad(picked_inv.reshape(NUM_PLANES, 1, slot_rows), ((0, 0), (0, 0), (0, RANK_PAD - slot_rows))),
            packed.reshape(PLANE_TOTAL, ROW_GROUP, out_width), cot_sums, us=60)
        hot_cot = jnp.sum(hot_sums, axis=0)

        def fetched_rows(_):
            start = jnp.sum(jnp.where(of_owner, starts[:, None], 0), axis=0)
            place = jnp.where(plane_cold, start + plane_rank, plane_tokens)
            table = jnp.concatenate([hot_cols, cold_cols.reshape(-1, part)])
            select = (place[:, None] == jnp.arange(table.shape[0])).astype(bf16)
            x_cols = jnp.dot(select, table, preferred_element_type=f32)
            by_owner = jnp.dot(of_owner.astype(bf16).T, jnp.concatenate(split3(cold_inv[:, 0]), axis=1), preferred_element_type=f32)
            by_owner = by_owner.reshape(plane_seq, 3, RANK_PAD)
            by_owner = by_owner[:, 0] + by_owner[:, 1] + by_owner[:, 2]
            cold_part = jnp.sum(jnp.where(plane_rank[:, None] == jnp.arange(RANK_PAD), by_owner, 0.0), axis=1, keepdims=True)
            hot_part = jnp.sum(jnp.where(plane_tokens[:, None] == jnp.arange(HOT_ROWS), hot_inv, 0.0), axis=1, keepdims=True)
            return x_cols, jnp.where(plane_cold[:, None], cold_part, hot_part)

        def ring_cols(_):
            def hop(step, carry):
                ids, cols, inv = carry
                mine = ids // vocab_local == me
                own = rounded(embed_shard[jnp.where(mine, ids - me * vocab_local, 0)]).astype(bf16)
                own_inv = norm_forward(own.astype(f32))[0]
                own = own.reshape(plane_seq, NUM_PLANES, PLANE, block)
                own = lax.dynamic_index_in_dim(own, (me + NUM_DEV - step) % PLANE, 2, keepdims=False).reshape(plane_seq, part)
                cols = jnp.where(mine[:, None], own, cols)
                inv = jnp.where(mine[:, None], own_inv, inv)
                return tuple(lax.ppermute(v, AXIS_NAME, ring) for v in (ids, cols, inv))
            start = (plane_tokens, jnp.zeros((plane_seq, part), bf16), jnp.zeros((plane_seq, 1), f32))
            _, cols, inv = lax.fori_loop(0, NUM_DEV, hop, start)
            return cols.astype(f32), inv

        x_cols, x_inv = lax.cond(fits, fetched_rows, ring_cols, None)
        n_plane = (x_cols * x_inv * my_gain).astype(bf16)

        parts = dot_tokens(n_plane, cot_plane)
        parts, n_plane, hot_mine = lax.optimization_barrier((parts, n_plane, hot_mine))
        d_w = lax.psum_scatter(parts, AXIS_NAME, scatter_dimension=0, tiled=True, axis_index_groups=column_groups)

        n_cols, my_hot = exchange(plane_kernel, [((PLANE, seq, part), bf16), ((HOT_BLOCK, width), bf16)],
                                  [(PLANE,), (PLANE,), (NUM_DEV,), ()], n_plane.reshape(PLANE, seq, part),
                                  hot_mine.reshape(NUM_DEV, HOT_BLOCK, width))
        normed = n_cols.reshape(PLANE, seq, NUM_PLANES, block).transpose(1, 2, 0, 3).reshape(seq, width)

        my_cap = jnp.sum(jnp.where(me == jnp.arange(NUM_DEV), caps, 0))
        got_valid = ((slots[None] < jnp.sum(from_mine, axis=1, dtype=jnp.int32)[:, None]) & (slots < my_cap)[None]).reshape(-1, 1)
        got_h = picked.astype(f32) * picked_inv
        got_dn = jnp.where(got_valid, dot_rows(got.reshape(-1, out_width), w_full), 0.0)
        got_dx = norm_backward(got_dn, got_h, picked_inv, gain_full)

        my_hot_inv, hot_h = norm_forward(my_hot.astype(f32))
        hot_dn3 = dot_rows(jnp.concatenate(split3(hot_cot)), w_full).reshape(3, HOT_BLOCK, width)
        hot_dn = hot_dn3[0] + hot_dn3[1] + hot_dn3[2]
        hot_dx = norm_backward(hot_dn, hot_h, my_hot_inv, gain_full)

        gain_part = jnp.sum(got_dn * got_h, axis=0) + jnp.sum(hot_dn * hot_h, axis=0)
        gain_part = jnp.pad(gain_part.reshape(NUM_DEV, 1, block), ((0, 0), (0, 0), (0, 128 - block)))
        hot_back, gain_back = exchange(
            collect_kernel, [((NUM_DEV, HOT_BLOCK, width), f32), ((NUM_DEV, 1, 128), f32)],
            [(), (NUM_DEV,), (NUM_DEV,), (NUM_DEV,), ()], hot_dx, gain_part)

        place = ((jnp.arange(vocab_local)[:, None] == pick_ids[None, :]) & got_valid[:, 0][None]).astype(bf16)
        cold_grad = jnp.dot(jnp.concatenate([place] * 3, axis=1), jnp.concatenate(split3(got_dx)), preferred_element_type=f32)

        def ring_sums(_):
            my_ids = tokens[0]

            def fetch(_, carry):
                ids, rows = carry
                mine = ids // vocab_local == me
                own = rounded(embed_shard[jnp.where(mine, ids - me * vocab_local, 0)]).astype(bf16)
                rows = jnp.where(mine[:, None], own, rows)
                return lax.ppermute(ids, AXIS_NAME, ring), lax.ppermute(rows, AXIS_NAME, ring)
            x_rows = lax.fori_loop(0, NUM_DEV, fetch, (my_ids, jnp.zeros((seq, width), bf16)))[1].astype(f32)
            inv_rms, h_rows = norm_forward(x_rows)
            d_normed = dot_rows(cot_mine, w_full)
            d_gain = lax.psum(jnp.sum(d_normed * h_rows, axis=0), AXIS_NAME)
            d_x = norm_backward(d_normed, h_rows, inv_rms, gain_full)

            def hop(_, carry):
                ids, rows, total = carry
                mine = ids // vocab_local == me
                total = total.at[jnp.where(mine, ids - me * vocab_local, vocab_local)].add(rows, mode="drop")
                return lax.ppermute(ids, AXIS_NAME, ring), lax.ppermute(rows, AXIS_NAME, ring), total
            total = lax.fori_loop(0, NUM_DEV, hop, (my_ids, d_x, jnp.zeros(embed_shard.shape, f32)))[2]
            return total, lax.dynamic_slice_in_dim(d_gain, me * block, block)

        top = jnp.where(me == 0, hot_back.reshape(HOT_ROWS, width), cold_grad[:HOT_ROWS])
        sums = (fits, cold_grad.at[:HOT_ROWS].set(top), jnp.sum(gain_back[:, 0, :block], axis=0))
        _, d_embed, d_norm_gain = lax.while_loop(lambda v: jnp.logical_not(v[0]), lambda v: (True,) + ring_sums(v), sums)

        proj = jnp.dot(normed, w_full, preferred_element_type=f32).astype(bf16)[None]
        return (proj[..., :q_width], proj[..., q_width:q_width + kv_width], proj[..., q_width + kv_width:], d_embed, d_norm_gain,
                d_w[:, :q_width], d_w[:, q_width:q_width + kv_width], d_w[:, q_width + kv_width:])

    row_spec = P(AXIS_NAME, None)
    act_spec = P(AXIS_NAME, None, None)
    vec_spec = P(AXIS_NAME)
    return jax.shard_map(local_step, mesh=mesh,
                         in_specs=(row_spec, row_spec, vec_spec, row_spec, row_spec, row_spec, act_spec, act_spec, act_spec),
                         out_specs=(act_spec, act_spec, act_spec, row_spec, vec_spec, row_spec, row_spec, row_spec),
                         check_vma=False)
```

```python
import functools

import jax
import jax.numpy as jnp
from jax import lax
from jax.experimental import pallas as pl
from jax.experimental.pallas import tpu as pltpu
from jax.sharding import PartitionSpec as P

AXIS_NAME = "fsdp"
NUM_DEV = 32
PLANE = 8
NUM_PLANES = 4
HOT_ROWS = 512
HOT_BLOCK = HOT_ROWS // NUM_DEV
ROW_GROUP = 8
CLASSES = ((0, 2, 21, 0), (2, 4, 12, 42), (4, 8, 7, 66), (8, 16, 4, 94), (16, 32, 3, 126))
SEND_GROUPS = 21
RECV_GROUPS = 174
RANK_PAD = 256
PLANE_GROUPS = (12, 4, 3, 3)
PLANE_FIRST = (0, 12, 16, 19)
PLANE_TOTAL = 22
OWN_GROUPS = 7
HELP_GROUPS = (5, 4)
MESH = pl.DeviceIdType.MESH
ANY = pl.BlockSpec(memory_space=pl.ANY)
BF16_MAX = 3.3895313892515355e38


def owner_class(owner):
    for first, last, groups, start in CLASSES:
        if first <= owner < last:
            return groups, start + (owner - first) * groups


def remote(src, dst, send_sem, recv_sem, dev):
    return pltpu.make_async_remote_copy(src_ref=src, dst_ref=dst, send_sem=send_sem, recv_sem=recv_sem,
                                        device_id=(dev,), device_id_type=MESH)


def spread_kernel(src_ref, hot_ref, out_ref, hot_out, send_sems, recv_sems, own_sem, hot_send, hot_recv):
    me = lax.axis_index(AXIS_NAME)
    own = pltpu.make_async_copy(src_ref, out_ref.at[me], own_sem)
    own.start()

    @pl.loop(1, NUM_DEV)
    def _(step):
        dev = lax.rem(me + step, NUM_DEV)
        remote(src_ref, out_ref.at[me], send_sems.at[step], recv_sems.at[step], dev).start()

    @pl.when(me == 0)
    def _():
        pltpu.make_async_copy(hot_ref.at[:, pl.ds(0, HOT_BLOCK)], hot_out, hot_recv).start()

        @pl.loop(1, NUM_DEV)
        def _(dev):
            remote(hot_ref.at[:, pl.ds(dev * HOT_BLOCK, HOT_BLOCK)], hot_out, hot_send.at[dev], hot_recv, dev).start()

    @pl.loop(1, NUM_DEV)
    def _(step):
        src = lax.rem(me + NUM_DEV - step, NUM_DEV)
        remote(src_ref, out_ref.at[src], send_sems.at[step], recv_sems.at[step], src).wait()

    own.wait()
    pltpu.make_async_copy(hot_out, hot_out, hot_recv).wait()

    @pl.when(me == 0)
    def _():
        @pl.loop(1, NUM_DEV)
        def _(dev):
            pltpu.make_async_copy(hot_out, hot_out, hot_send.at[dev]).wait()


def slice_kernel(x_ref, out_ref):
    low = lax.broadcasted_iota(jnp.int32, (x_ref.shape[0], 128), 1) < 64
    for chip in range(PLANE // 2):
        for half in range(NUM_PLANES // 2):
            at = (PLANE // 2 * 2 * half + chip) * 128
            one = x_ref[:, at:at + 128].astype(jnp.bfloat16).astype(jnp.float32)
            at += PLANE // 2 * 128
            two = x_ref[:, at:at + 128].astype(jnp.bfloat16).astype(jnp.float32)
            cols = slice(half * 128, half * 128 + 128)
            out_ref[2 * chip, :, cols] = jnp.where(low, one, pltpu.roll(two, 64, 1)).astype(jnp.bfloat16)
            out_ref[2 * chip + 1, :, cols] = jnp.where(low, pltpu.roll(one, 64, 1), two).astype(jnp.bfloat16)


def column_slices(table, rows, step):
    width = table.shape[1]
    return pl.pallas_call(
        slice_kernel, grid=(rows // step,), in_specs=[pl.BlockSpec((step, width), lambda i: (i, 0))],
        out_specs=pl.BlockSpec((PLANE, step, width // PLANE), lambda i: (0, i, 0)),
        out_shape=jax.ShapeDtypeStruct((PLANE, rows, width // PLANE), jnp.bfloat16))(table)


def rows_kernel(hot_ref, hot_inv_ref, cold_ref, cold_inv_ref, cot_ref, sum_ref,
                hot_out, hot_inv_out, cold_out, cold_inv_out, cot_out, sum_out,
                hot_send, hot_recv, pass_send, hot_inv_send, hot_inv_recv, send_sems, recv_sems, inv_send, inv_recv,
                cot_send, cot_recv, sum_send, sum_recv, help_send, help_recv):
    me = lax.axis_index(AXIS_NAME)
    pos = lax.rem(me, PLANE)
    plane = me // PLANE

    @pl.when(me == 0)
    def _():
        for dev in range(1, PLANE):
            remote(hot_ref.at[dev], hot_out, hot_send.at[dev], hot_recv, dev).start()
        pltpu.make_async_copy(hot_ref.at[0], hot_out, hot_recv).start()
        for dev in range(1, NUM_DEV):
            remote(hot_inv_ref, hot_inv_out, hot_inv_send.at[dev], hot_inv_recv, dev).start()
        pltpu.make_async_copy(hot_inv_ref, hot_inv_out, hot_inv_recv).start()

    def pass_on():
        pltpu.make_async_copy(hot_out, hot_out, hot_recv).wait()

        @pl.when(plane < NUM_PLANES - 1)
        def _():
            remote(hot_out, hot_out, pass_send, hot_recv, lax.rem(me + PLANE, NUM_DEV)).start()

    @pl.when(plane == 0)
    def _():
        pass_on()

    def move(rows, into, send_sem, recv_sem, dst, dev):
        @pl.when(plane == dst)
        def _():
            pltpu.make_async_copy(rows, into, recv_sem).start()

        @pl.when(plane != dst)
        def _():
            remote(rows, into, send_sem, recv_sem, dev).start()

    for dst, (groups, first) in enumerate(zip(PLANE_GROUPS, PLANE_FIRST)):
        dev = dst * PLANE + pos
        move(sum_ref.at[dst], sum_out.at[plane], sum_send.at[dst], sum_recv.at[plane], dst, dev)
        if dst:
            move(cot_ref.at[pl.ds(first, groups)], cot_out.at[plane, pl.ds(0, groups)], cot_send.at[dst], cot_recv.at[plane], dst, dev)
            continue

        @pl.when(pos < 4)
        def _():
            move(cot_ref.at[pl.ds(0, groups)], cot_out.at[plane, pl.ds(0, groups)], cot_send.at[0], cot_recv.at[plane], 0, dev)

        @pl.when(pos >= 4)
        def _():
            move(cot_ref.at[pl.ds(0, OWN_GROUPS)], cot_out.at[plane, pl.ds(0, OWN_GROUPS)], cot_send.at[0], cot_recv.at[plane], 0, dev)

        start = groups
        for k, more in enumerate(HELP_GROUPS):
            @pl.when((pos >= 4 + 2 * k) & (pos < 6 + 2 * k))
            def _():
                remote(cot_ref.at[pl.ds(OWN_GROUPS, more)], cot_out.at[plane, pl.ds(start, more)],
                       help_send, help_recv.at[k, plane], lax.rem(pos, 2)).start()
            start += more

    own_inv = pltpu.make_async_copy(cold_inv_ref.at[plane], cold_inv_out.at[me], inv_recv.at[me])
    own_inv.start()
    for first, last, groups, start in CLASSES:
        @pl.when((me >= first) & (me < last))
        def _():
            src_rows, dst_rows = pl.ds(0, groups), pl.ds(start + (me - first) * groups, groups)
            pltpu.make_async_copy(cold_ref.at[pos, plane, src_rows], cold_out.at[dst_rows], recv_sems.at[me]).start()

            @pl.loop(1, NUM_DEV)
            def _(step):
                dev = lax.rem(me + step, NUM_DEV)
                remote(cold_ref.at[lax.rem(dev, PLANE), dev // PLANE, src_rows], cold_out.at[dst_rows],
                       send_sems.at[step], recv_sems.at[me], dev).start()

    @pl.loop(1, NUM_DEV)
    def _(step):
        dev = lax.rem(me + step, NUM_DEV)
        remote(cold_inv_ref.at[dev // PLANE], cold_inv_out.at[me], inv_send.at[step], inv_recv.at[me], dev).start()

    @pl.when(plane > 0)
    def _():
        pass_on()

    for owner in range(NUM_DEV):
        groups, base = owner_class(owner)
        rows = cold_out.at[pl.ds(base, groups)]
        pltpu.make_async_copy(rows, rows, recv_sems.at[owner]).wait()

    @pl.loop(0, NUM_DEV)
    def _(owner):
        pltpu.make_async_copy(cold_inv_out.at[owner], cold_inv_out.at[owner], inv_recv.at[owner]).wait()

    @pl.loop(1, NUM_DEV)
    def _(step):
        pltpu.make_async_copy(cold_inv_ref.at[0], cold_inv_ref.at[0], inv_send.at[step]).wait()

    for first, last, groups, start in CLASSES:
        @pl.when((me >= first) & (me < last))
        def _():
            rows = cold_ref.at[0, 0, pl.ds(0, groups)]

            @pl.loop(1, NUM_DEV)
            def _(step):
                pltpu.make_async_copy(rows, rows, send_sems.at[step]).wait()

    def came(ref, sem):
        pltpu.make_async_copy(ref, ref, sem).wait()

    for src in range(NUM_PLANES):
        came(sum_out.at[src], sum_recv.at[src])
        for dst in range(1, NUM_PLANES):
            @pl.when(plane == dst)
            def _():
                came(cot_out.at[src, pl.ds(0, PLANE_GROUPS[dst])], cot_recv.at[src])

        @pl.when((plane == 0) & (pos < 4))
        def _():
            came(cot_out.at[src, pl.ds(0, PLANE_GROUPS[0])], cot_recv.at[src])

        @pl.when((plane == 0) & (pos >= 4))
        def _():
            came(cot_out.at[src, pl.ds(0, OWN_GROUPS)], cot_recv.at[src])

        start = PLANE_GROUPS[0]
        for k, more in enumerate(HELP_GROUPS):
            @pl.when(me < 2)
            def _():
                came(cot_out.at[src, pl.ds(start, more)], help_recv.at[k, src])
            start += more

    for dst, (groups, first) in enumerate(zip(PLANE_GROUPS, PLANE_FIRST)):
        @pl.when(plane != dst)
        def _():
            came(sum_ref.at[dst], sum_send.at[dst])
            if dst:
                came(cot_ref.at[pl.ds(first, groups)], cot_send.at[dst])

    @pl.when((plane != 0) & (pos < 4))
    def _():
        came(cot_ref.at[pl.ds(0, PLANE_GROUPS[0])], cot_send.at[0])

    @pl.when((plane != 0) & (pos >= 4))
    def _():
        came(cot_ref.at[pl.ds(0, OWN_GROUPS)], cot_send.at[0])

    for k, more in enumerate(HELP_GROUPS):
        @pl.when((pos >= 4 + 2 * k) & (pos < 6 + 2 * k))
        def _():
            came(cot_ref.at[pl.ds(OWN_GROUPS, more)], help_send)

    pltpu.make_async_copy(hot_inv_out, hot_inv_out, hot_inv_recv).wait()

    @pl.when(plane < NUM_PLANES - 1)
    def _():
        pltpu.make_async_copy(hot_out, hot_out, pass_send).wait()

    @pl.when(me == 0)
    def _():
        for dev in range(1, PLANE):
            pltpu.make_async_copy(hot_out, hot_out, hot_send.at[dev]).wait()
        for dev in range(1, NUM_DEV):
            pltpu.make_async_copy(hot_inv_ref, hot_inv_ref, hot_inv_send.at[dev]).wait()


def collect_kernel(hot_ref, gain_ref, n_ref, hot_out, gain_out, n_out, hot_send, hot_recv, send_sems, recv_sems, own_sem, n_send, n_recv):
    me = lax.axis_index(AXIS_NAME)
    pos = lax.rem(me, PLANE)
    base = me - pos

    @pl.when(me == 0)
    def _():
        pltpu.make_async_copy(hot_ref, hot_out.at[me], hot_recv.at[0]).start()

    @pl.when(me != 0)
    def _():
        remote(hot_ref, hot_out.at[me], hot_send, hot_recv.at[me], 0).start()

    own = pltpu.make_async_copy(gain_ref.at[me], gain_out.at[me], own_sem)
    own.start()
    own_n = pltpu.make_async_copy(n_ref.at[pos], n_out.at[pos], n_recv.at[0])
    own_n.start()
    copies = []
    for step in range(1, PLANE):
        peer = lax.rem(pos + step, PLANE)
        copies.append(remote(n_ref.at[peer], n_out.at[pos], n_send.at[step], n_recv.at[step], base + peer))
    for step in range(1, NUM_DEV):
        dev = lax.rem(me + step, NUM_DEV)
        copies.append(remote(gain_ref.at[dev], gain_out.at[me], send_sems.at[step], recv_sems.at[step], dev))
    for copy in copies:
        copy.start()
    for step in range(1, NUM_DEV):
        src = lax.rem(me + NUM_DEV - step, NUM_DEV)
        remote(gain_ref.at[src], gain_out.at[src], send_sems.at[step], recv_sems.at[step], src).wait()
    own.wait()
    for step in range(1, PLANE):
        peer = lax.rem(pos + PLANE - step, PLANE)
        remote(n_ref.at[peer], n_out.at[peer], n_send.at[step], n_recv.at[step], base + peer).wait()
    own_n.wait()

    @pl.when(me == 0)
    def _():
        for src in range(NUM_DEV):
            pltpu.make_async_copy(hot_ref, hot_out.at[src], hot_recv.at[src]).wait()

    @pl.when(me != 0)
    def _():
        pltpu.make_async_copy(hot_ref, hot_ref, hot_send).wait()


def exchange(kernel, outs, sems, *args, spec=ANY, us=20):
    return pl.pallas_call(
        kernel, cost_estimate=pl.CostEstimate(flops=us * 500_000_000, bytes_accessed=1_000_000, transcendentals=0), out_shape=[jax.ShapeDtypeStruct(*out) for out in outs],
        in_specs=[spec] * len(args), out_specs=[spec] * len(outs),
        scratch_shapes=[pltpu.SemaphoreType.DMA(shape) if shape else pltpu.SemaphoreType.DMA for shape in sems],
        compiler_params=pltpu.CompilerParams(has_side_effects=True))(*args)


def split3(value):
    def top(v):
        return jnp.clip(lax.reduce_precision(v, 8, 7), -BF16_MAX, BF16_MAX)
    high = top(value)
    rest = value - high
    mid = top(rest)
    return [part.astype(jnp.bfloat16) for part in (high, mid, rest - mid)]


def ranks(mask):
    n = mask.shape[-1]
    lower = (jnp.arange(n)[:, None] < jnp.arange(n)[None, :]).astype(jnp.bfloat16)
    return jnp.dot(mask.astype(jnp.bfloat16), lower, preferred_element_type=jnp.float32).astype(jnp.int32)


def dot_rows(a, b):
    return lax.dot_general(a, b, (((1,), (1,)), ((), ())), preferred_element_type=jnp.float32)


def dot_tokens(a, b):
    return lax.dot_general(a, b, (((0,), (0,)), ((), ())), preferred_element_type=jnp.float32)


def rounded(rows):
    return lax.reduce_precision(rows, 8, 7)


def norm_forward(x_rows):
    inv_rms = lax.rsqrt(jnp.mean(x_rows * x_rows, axis=-1, keepdims=True) + 1e-5)
    return inv_rms, x_rows * inv_rms


def norm_backward(d_normed, h_rows, inv_rms, gain_full):
    u_rows = d_normed * gain_full
    return inv_rms * (u_rows - h_rows * jnp.mean(u_rows * h_rows, axis=-1, keepdims=True))


def solution(mesh):
    ring = [(d, (d + 1) % NUM_DEV) for d in range(NUM_DEV)]
    plane_groups = [[z * PLANE + p for p in range(PLANE)] for z in range(NUM_PLANES)]
    column_groups = [[z * PLANE + p for z in range(NUM_PLANES)] for p in range(PLANE)]
    caps = jnp.array([owner_class(d)[0] * ROW_GROUP for d in range(NUM_DEV)], jnp.int32)
    starts = jnp.array([HOT_ROWS + owner_class(d)[1] * ROW_GROUP for d in range(NUM_DEV)], jnp.int32)
    slot_plane = jnp.array([z for z, g in enumerate(PLANE_GROUPS) for _ in range(g * ROW_GROUP)], jnp.int32)
    slot_rank = jnp.array([c for g in PLANE_GROUPS for c in range(g * ROW_GROUP)], jnp.int32)

    def local_step(tokens, embed_shard, gain_shard, wq_shard, wk_shard, wv_shard, d_query, d_key, d_value):
        vocab_local, width = embed_shard.shape
        seq = tokens.shape[1]
        q_width, kv_width = wq_shard.shape[1], wk_shard.shape[1]
        out_width = q_width + 2 * kv_width
        block = width // NUM_DEV
        part, plane_seq, slot_rows = width // PLANE, PLANE * seq, SEND_GROUPS * ROW_GROUP
        me = lax.axis_index(AXIS_NAME)
        pos, plane = me % PLANE, me // PLANE
        bf16, f32 = jnp.bfloat16, jnp.float32

        cot_mine = jnp.concatenate([d_query[0], d_key[0], d_value[0]], axis=1)
        cot_plane = lax.all_gather(cot_mine, AXIS_NAME, axis=0, tiled=True, axis_index_groups=plane_groups)
        w_mine = jnp.concatenate([wq_shard.astype(bf16), wk_shard.astype(bf16), wv_shard.astype(bf16)], axis=1)
        w_full = lax.all_gather(w_mine, AXIS_NAME, axis=0, tiled=True)

        message = jnp.concatenate([tokens.astype(f32), jnp.pad(gain_shard, (0, 128 - block))[None]], axis=1)
        hot_slices = column_slices(embed_shard, HOT_ROWS, 128)
        spread, my_hot = exchange(spread_kernel, [((NUM_DEV, 1, seq + 128), f32), ((PLANE, HOT_BLOCK, part), bf16)],
                                  [(NUM_DEV,), (NUM_DEV,), (), (NUM_DEV,), ()], message, hot_slices)
        my_hot = my_hot.reshape(PLANE, HOT_BLOCK, NUM_PLANES, block).transpose(1, 2, 0, 3).reshape(HOT_BLOCK, width)
        all_tokens = spread[:, 0, :seq].astype(jnp.int32)
        gain_full = spread[:, 0, seq:seq + block].reshape(1, width)
        my_gain = gain_full.reshape(NUM_PLANES, PLANE, block)
        my_gain = lax.dynamic_index_in_dim(my_gain, pos, 1, keepdims=False).reshape(1, part)

        all_owner = all_tokens // vocab_local
        all_cold = all_tokens >= HOT_ROWS
        counts = jnp.sum((all_owner[:, :, None] == jnp.arange(NUM_DEV)) & all_cold[:, :, None], axis=1, dtype=jnp.int32)
        fits = jnp.all(counts.reshape(NUM_PLANES, PLANE, NUM_DEV).sum(1) <= caps[None])

        plane_tokens = lax.dynamic_slice_in_dim(all_tokens, plane * PLANE, PLANE, 0).reshape(plane_seq)
        plane_owner = plane_tokens // vocab_local
        plane_cold = plane_tokens >= HOT_ROWS
        of_owner = plane_owner[None] == jnp.arange(NUM_DEV)[:, None]
        plane_rank = jnp.sum(jnp.where(of_owner, ranks(of_owner & plane_cold[None]), 0), axis=0)

        places = jnp.arange(NUM_PLANES * HOT_BLOCK)
        hot_ids = (places // HOT_BLOCK * PLANE + pos) * HOT_BLOCK + places % HOT_BLOCK
        hot_select = plane_tokens[:, None] == hot_ids[None, :]
        helped = (pos >= 4) & (slot_plane == 0) & (slot_rank >= OWN_GROUPS * ROW_GROUP)
        first_rank = (PLANE_GROUPS[0] - OWN_GROUPS) * ROW_GROUP + jnp.where(pos >= 6, HELP_GROUPS[0] * ROW_GROUP, 0)
        pack_owner = jnp.where(helped, pos % 2, slot_plane * PLANE + pos)
        pack_rank = jnp.where(helped, slot_rank + first_rank, slot_rank)
        pack = plane_cold[:, None] & (plane_owner[:, None] == pack_owner[None]) & (plane_rank[:, None] == pack_rank[None])
        cot_sums = dot_tokens(hot_select.astype(bf16), cot_plane).reshape(NUM_PLANES, HOT_BLOCK, out_width)
        packed = dot_tokens(pack.astype(bf16), cot_plane).astype(bf16)

        from_mine = ((all_owner == me) & all_cold).reshape(NUM_PLANES, plane_seq)
        from_rank = ranks(from_mine)
        slots = jnp.arange(slot_rows)
        picks = (from_rank[:, None, :] == slots[None, :, None]) & from_mine[:, None, :]
        local_ids = (all_tokens - me * vocab_local).reshape(NUM_PLANES, 1, plane_seq)
        pick_ids = jnp.sum(jnp.where(picks, local_ids, 0), axis=2).reshape(-1)
        picked = rounded(embed_shard[pick_ids]).astype(bf16)
        hot_mine = rounded(embed_shard[:HOT_ROWS]).astype(bf16)
        cold_slices = column_slices(picked, NUM_PLANES * slot_rows, slot_rows)
        hot_inv_mine = norm_forward(hot_mine.astype(f32))[0]
        picked_inv = norm_forward(picked.astype(f32))[0]
        hot_cols, hot_inv, cold_cols, cold_inv, got, hot_sums = exchange(
            rows_kernel,
            [((HOT_ROWS, part), bf16), ((1, HOT_ROWS), f32), ((RECV_GROUPS, ROW_GROUP, part), bf16), ((NUM_DEV, 1, RANK_PAD), f32),
             ((NUM_PLANES, SEND_GROUPS, ROW_GROUP, out_width), bf16), ((NUM_PLANES, HOT_BLOCK, out_width), f32)],
            [(PLANE,), (), (), (NUM_DEV,), (), (NUM_DEV,), (NUM_DEV,), (NUM_DEV,), (NUM_DEV,)] + [(NUM_PLANES,)] * 4 + [(), (2, NUM_PLANES)],
            hot_slices, hot_inv_mine.reshape(1, HOT_ROWS),
            cold_slices.reshape(PLANE, NUM_PLANES, SEND_GROUPS, ROW_GROUP, part),
            jnp.pad(picked_inv.reshape(NUM_PLANES, 1, slot_rows), ((0, 0), (0, 0), (0, RANK_PAD - slot_rows))),
            packed.reshape(PLANE_TOTAL, ROW_GROUP, out_width), cot_sums, us=60)
        hot_cot = jnp.sum(hot_sums, axis=0)

        def fetched_rows(_):
            start = jnp.sum(jnp.where(of_owner, starts[:, None], 0), axis=0)
            place = jnp.where(plane_cold, start + plane_rank, plane_tokens)
            table = jnp.concatenate([hot_cols, cold_cols.reshape(-1, part)])
            select = (place[:, None] == jnp.arange(table.shape[0])).astype(bf16)
            x_cols = jnp.dot(select, table, preferred_element_type=f32)
            by_owner = jnp.dot(of_owner.astype(bf16).T, jnp.concatenate(split3(cold_inv[:, 0]), axis=1), preferred_element_type=f32)
            by_owner = by_owner.reshape(plane_seq, 3, RANK_PAD)
            by_owner = by_owner[:, 0] + by_owner[:, 1] + by_owner[:, 2]
            cold_part = jnp.sum(jnp.where(plane_rank[:, None] == jnp.arange(RANK_PAD), by_owner, 0.0), axis=1, keepdims=True)
            hot_part = jnp.sum(jnp.where(plane_tokens[:, None] == jnp.arange(HOT_ROWS), hot_inv, 0.0), axis=1, keepdims=True)
            return x_cols, jnp.where(plane_cold[:, None], cold_part, hot_part)

        def ring_cols(_):
            def hop(step, carry):
                ids, cols, inv = carry
                mine = ids // vocab_local == me
                own = rounded(embed_shard[jnp.where(mine, ids - me * vocab_local, 0)]).astype(bf16)
                own_inv = norm_forward(own.astype(f32))[0]
                own = own.reshape(plane_seq, NUM_PLANES, PLANE, block)
                own = lax.dynamic_index_in_dim(own, (me + NUM_DEV - step) % PLANE, 2, keepdims=False).reshape(plane_seq, part)
                cols = jnp.where(mine[:, None], own, cols)
                inv = jnp.where(mine[:, None], own_inv, inv)
                return tuple(lax.ppermute(v, AXIS_NAME, ring) for v in (ids, cols, inv))
            start = (plane_tokens, jnp.zeros((plane_seq, part), bf16), jnp.zeros((plane_seq, 1), f32))
            _, cols, inv = lax.fori_loop(0, NUM_DEV, hop, start)
            return cols.astype(f32), inv

        x_cols, x_inv = lax.cond(fits, fetched_rows, ring_cols, None)
        n_plane = (x_cols * x_inv * my_gain).astype(bf16)

        parts = dot_tokens(n_plane, cot_plane)
        parts, n_plane, pick_ids, from_mine = lax.optimization_barrier((parts, n_plane, pick_ids, from_mine))
        d_w = lax.psum_scatter(parts, AXIS_NAME, scatter_dimension=0, tiled=True, axis_index_groups=column_groups)

        my_cap = jnp.sum(jnp.where(me == jnp.arange(NUM_DEV), caps, 0))
        got_valid = ((slots[None] < jnp.sum(from_mine, axis=1, dtype=jnp.int32)[:, None]) & (slots < my_cap)[None]).reshape(-1, 1)
        got_h = picked.astype(f32) * picked_inv
        got_dn = jnp.where(got_valid, dot_rows(got.reshape(-1, out_width), w_full), 0.0)
        got_dx = norm_backward(got_dn, got_h, picked_inv, gain_full)

        my_hot_inv, hot_h = norm_forward(my_hot.astype(f32))
        hot_dn3 = dot_rows(jnp.concatenate(split3(hot_cot)), w_full).reshape(3, HOT_BLOCK, width)
        hot_dn = hot_dn3[0] + hot_dn3[1] + hot_dn3[2]
        hot_dx = norm_backward(hot_dn, hot_h, my_hot_inv, gain_full)

        gain_part = jnp.sum(got_dn * got_h, axis=0) + jnp.sum(hot_dn * hot_h, axis=0)
        gain_part = jnp.pad(gain_part.reshape(NUM_DEV, 1, block), ((0, 0), (0, 0), (0, 128 - block)))
        hot_back, gain_back, n_cols = exchange(
            collect_kernel, [((NUM_DEV, HOT_BLOCK, width), f32), ((NUM_DEV, 1, 128), f32), ((PLANE, seq, part), bf16)],
            [(), (NUM_DEV,), (NUM_DEV,), (NUM_DEV,), (), (PLANE,), (PLANE,)], hot_dx, gain_part, n_plane.reshape(PLANE, seq, part), us=30)
        normed = n_cols.reshape(PLANE, seq, NUM_PLANES, block).transpose(1, 2, 0, 3).reshape(seq, width)

        place = ((jnp.arange(vocab_local)[:, None] == pick_ids[None, :]) & got_valid[:, 0][None]).astype(bf16)
        cold_grad = jnp.dot(jnp.concatenate([place] * 3, axis=1), jnp.concatenate(split3(got_dx)), preferred_element_type=f32)

        def ring_sums(_):
            my_ids = tokens[0]

            def fetch(_, carry):
                ids, rows = carry
                mine = ids // vocab_local == me
                own = rounded(embed_shard[jnp.where(mine, ids - me * vocab_local, 0)]).astype(bf16)
                rows = jnp.where(mine[:, None], own, rows)
                return lax.ppermute(ids, AXIS_NAME, ring), lax.ppermute(rows, AXIS_NAME, ring)
            x_rows = lax.fori_loop(0, NUM_DEV, fetch, (my_ids, jnp.zeros((seq, width), bf16)))[1].astype(f32)
            inv_rms, h_rows = norm_forward(x_rows)
            d_normed = dot_rows(cot_mine, w_full)
            d_gain = lax.psum(jnp.sum(d_normed * h_rows, axis=0), AXIS_NAME)
            d_x = norm_backward(d_normed, h_rows, inv_rms, gain_full)

            def hop(_, carry):
                ids, rows, total = carry
                mine = ids // vocab_local == me
                total = total.at[jnp.where(mine, ids - me * vocab_local, vocab_local)].add(rows, mode="drop")
                return lax.ppermute(ids, AXIS_NAME, ring), lax.ppermute(rows, AXIS_NAME, ring), total
            total = lax.fori_loop(0, NUM_DEV, hop, (my_ids, d_x, jnp.zeros(embed_shard.shape, f32)))[2]
            return total, lax.dynamic_slice_in_dim(d_gain, me * block, block)

        top = jnp.where(me == 0, hot_back.reshape(HOT_ROWS, width), cold_grad[:HOT_ROWS])
        sums = (fits, cold_grad.at[:HOT_ROWS].set(top), jnp.sum(gain_back[:, 0, :block], axis=0))
        _, d_embed, d_norm_gain = lax.while_loop(lambda v: jnp.logical_not(v[0]), lambda v: (True,) + ring_sums(v), sums)

        proj = jnp.dot(normed, w_full, preferred_element_type=f32).astype(bf16)[None]
        return (proj[..., :q_width], proj[..., q_width:q_width + kv_width], proj[..., q_width + kv_width:], d_embed, d_norm_gain,
                d_w[:, :q_width], d_w[:, q_width:q_width + kv_width], d_w[:, q_width + kv_width:])

    row_spec = P(AXIS_NAME, None)
    act_spec = P(AXIS_NAME, None, None)
    vec_spec = P(AXIS_NAME)
    return jax.shard_map(local_step, mesh=mesh,
                         in_specs=(row_spec, row_spec, vec_spec, row_spec, row_spec, row_spec, act_spec, act_spec, act_spec),
                         out_specs=(act_spec, act_spec, act_spec, row_spec, vec_spec, row_spec, row_spec, row_spec),
                         check_vma=False)
```

```python
import functools

import jax
import jax.numpy as jnp
from jax import lax
from jax.experimental import pallas as pl
from jax.experimental.pallas import tpu as pltpu
from jax.sharding import PartitionSpec as P

AXIS_NAME = "fsdp"
NUM_DEV = 32
PLANE = 8
NUM_PLANES = 4
HOT_ROWS = 512
HOT_BLOCK = HOT_ROWS // NUM_DEV
ROW_GROUP = 8
CLASSES = ((0, 2, 21, 0), (2, 4, 12, 42), (4, 8, 7, 66), (8, 16, 4, 94), (16, 32, 3, 126))
SEND_GROUPS = 21
RECV_GROUPS = 174
RANK_PAD = 256
PLANE_GROUPS = (12, 4, 3, 3)
PLANE_FIRST = (0, 12, 16, 19)
PLANE_TOTAL = 22
OWN_GROUPS = 7
HELP_GROUPS = (5, 4)
MESH = pl.DeviceIdType.MESH
ANY = pl.BlockSpec(memory_space=pl.ANY)
BF16_MAX = 3.3895313892515355e38


def owner_class(owner):
    for first, last, groups, start in CLASSES:
        if first <= owner < last:
            return groups, start + (owner - first) * groups


def remote(src, dst, send_sem, recv_sem, dev):
    return pltpu.make_async_remote_copy(src_ref=src, dst_ref=dst, send_sem=send_sem, recv_sem=recv_sem,
                                        device_id=(dev,), device_id_type=MESH)


def spread_kernel(src_ref, out_ref, send_sems, recv_sems, own_sem):
    me = lax.axis_index(AXIS_NAME)
    own = pltpu.make_async_copy(src_ref, out_ref.at[me], own_sem)
    own.start()

    @pl.loop(1, NUM_DEV)
    def _(step):
        dev = lax.rem(me + step, NUM_DEV)
        remote(src_ref, out_ref.at[me], send_sems.at[step], recv_sems.at[step], dev).start()

    @pl.loop(1, NUM_DEV)
    def _(step):
        src = lax.rem(me + NUM_DEV - step, NUM_DEV)
        remote(src_ref, out_ref.at[src], send_sems.at[step], recv_sems.at[step], src).wait()

    own.wait()


def slice_kernel(x_ref, out_ref, inv_ref):
    total = jnp.zeros((x_ref.shape[0], 128), jnp.float32)
    low = lax.broadcasted_iota(jnp.int32, (x_ref.shape[0], 128), 1) < 64
    for chip in range(PLANE // 2):
        for half in range(NUM_PLANES // 2):
            at = (PLANE // 2 * 2 * half + chip) * 128
            one = x_ref[:, at:at + 128].astype(jnp.bfloat16).astype(jnp.float32)
            at += PLANE // 2 * 128
            two = x_ref[:, at:at + 128].astype(jnp.bfloat16).astype(jnp.float32)
            total += one * one + two * two
            cols = slice(half * 128, half * 128 + 128)
            out_ref[2 * chip, :, cols] = jnp.where(low, one, pltpu.roll(two, 64, 1)).astype(jnp.bfloat16)
            out_ref[2 * chip + 1, :, cols] = jnp.where(low, pltpu.roll(one, 64, 1), two).astype(jnp.bfloat16)
    inv_rms = lax.rsqrt(jnp.sum(total, axis=1, keepdims=True) / x_ref.shape[1] + 1e-5)
    inv_ref[...] = jnp.broadcast_to(inv_rms, inv_ref.shape)


def column_slices(table, rows, step):
    width = table.shape[1]
    return pl.pallas_call(
        slice_kernel, grid=(rows // step,), in_specs=[pl.BlockSpec((step, width), lambda i: (i, 0))],
        out_specs=[pl.BlockSpec((PLANE, step, width // PLANE), lambda i: (0, i, 0)), pl.BlockSpec((step, 128), lambda i: (i, 0))],
        out_shape=[jax.ShapeDtypeStruct((PLANE, rows, width // PLANE), jnp.bfloat16),
                   jax.ShapeDtypeStruct((rows, 128), jnp.float32)])(table)


def rows_kernel(hot_ref, hot_inv_ref, cold_ref, cold_inv_ref, hot_out, hot_inv_out, cold_out, cold_inv_out,
                hot_send, hot_recv, pass_send, hot_inv_send, hot_inv_recv, send_sems, recv_sems, inv_send, inv_recv):
    me = lax.axis_index(AXIS_NAME)
    pos = lax.rem(me, PLANE)
    plane = me // PLANE

    @pl.when(me == 0)
    def _():
        for dev in range(1, PLANE):
            remote(hot_ref.at[dev], hot_out, hot_send.at[dev], hot_recv, dev).start()
        pltpu.make_async_copy(hot_ref.at[0], hot_out, hot_recv).start()
        for dev in range(1, NUM_DEV):
            remote(hot_inv_ref, hot_inv_out, hot_inv_send.at[dev], hot_inv_recv, dev).start()
        pltpu.make_async_copy(hot_inv_ref, hot_inv_out, hot_inv_recv).start()

    def pass_on():
        pltpu.make_async_copy(hot_out, hot_out, hot_recv).wait()

        @pl.when(plane < NUM_PLANES - 1)
        def _():
            remote(hot_out, hot_out, pass_send, hot_recv, lax.rem(me + PLANE, NUM_DEV)).start()

    @pl.when(plane == 0)
    def _():
        pass_on()

    own_inv = pltpu.make_async_copy(cold_inv_ref.at[plane], cold_inv_out.at[me], inv_recv.at[me])
    own_inv.start()
    for first, last, groups, start in CLASSES:
        @pl.when((me >= first) & (me < last))
        def _():
            src_rows, dst_rows = pl.ds(0, groups), pl.ds(start + (me - first) * groups, groups)
            pltpu.make_async_copy(cold_ref.at[pos, plane, src_rows], cold_out.at[dst_rows], recv_sems.at[me]).start()

            @pl.loop(1, NUM_DEV)
            def _(step):
                dev = lax.rem(me + step, NUM_DEV)
                remote(cold_ref.at[lax.rem(dev, PLANE), dev // PLANE, src_rows], cold_out.at[dst_rows],
                       send_sems.at[step], recv_sems.at[me], dev).start()

    @pl.loop(1, NUM_DEV)
    def _(step):
        dev = lax.rem(me + step, NUM_DEV)
        remote(cold_inv_ref.at[dev // PLANE], cold_inv_out.at[me], inv_send.at[step], inv_recv.at[me], dev).start()

    @pl.when(plane > 0)
    def _():
        pass_on()

    for owner in range(NUM_DEV):
        groups, base = owner_class(owner)
        rows = cold_out.at[pl.ds(base, groups)]
        pltpu.make_async_copy(rows, rows, recv_sems.at[owner]).wait()

    @pl.loop(0, NUM_DEV)
    def _(owner):
        pltpu.make_async_copy(cold_inv_out.at[owner], cold_inv_out.at[owner], inv_recv.at[owner]).wait()

    @pl.loop(1, NUM_DEV)
    def _(step):
        pltpu.make_async_copy(cold_inv_ref.at[0], cold_inv_ref.at[0], inv_send.at[step]).wait()

    for first, last, groups, start in CLASSES:
        @pl.when((me >= first) & (me < last))
        def _():
            rows = cold_ref.at[0, 0, pl.ds(0, groups)]

            @pl.loop(1, NUM_DEV)
            def _(step):
                pltpu.make_async_copy(rows, rows, send_sems.at[step]).wait()

    pltpu.make_async_copy(hot_inv_out, hot_inv_out, hot_inv_recv).wait()

    @pl.when(plane < NUM_PLANES - 1)
    def _():
        pltpu.make_async_copy(hot_out, hot_out, pass_send).wait()

    @pl.when(me == 0)
    def _():
        for dev in range(1, PLANE):
            pltpu.make_async_copy(hot_out, hot_out, hot_send.at[dev]).wait()
        for dev in range(1, NUM_DEV):
            pltpu.make_async_copy(hot_inv_ref, hot_inv_ref, hot_inv_send.at[dev]).wait()


def backs_kernel(n_ref, cot_ref, sum_ref, hot_ref, n_out, cot_out, sum_out, hot_out,
                 n_send, n_recv, cot_send, cot_recv, sum_send, sum_recv, help_send, help_recv, hot_send, hot_recv):
    me = lax.axis_index(AXIS_NAME)
    pos = lax.rem(me, PLANE)
    plane = me // PLANE
    base = me - pos
    own_n = pltpu.make_async_copy(n_ref.at[pos], n_out.at[pos], n_recv.at[0])
    own_n.start()
    for step in range(1, PLANE):
        peer = lax.rem(pos + step, PLANE)
        remote(n_ref.at[peer], n_out.at[pos], n_send.at[step], n_recv.at[step], base + peer).start()

    def move(rows, into, send_sem, recv_sem, dst, dev):
        @pl.when(plane == dst)
        def _():
            pltpu.make_async_copy(rows, into, recv_sem).start()

        @pl.when(plane != dst)
        def _():
            remote(rows, into, send_sem, recv_sem, dev).start()

    for dst, (groups, first) in enumerate(zip(PLANE_GROUPS, PLANE_FIRST)):
        dev = dst * PLANE + pos
        move(sum_ref.at[dst], sum_out.at[plane], sum_send.at[dst], sum_recv.at[plane], dst, dev)
        if dst:
            move(cot_ref.at[pl.ds(first, groups)], cot_out.at[plane, pl.ds(0, groups)], cot_send.at[dst], cot_recv.at[plane], dst, dev)
            continue

        @pl.when(pos < 4)
        def _():
            move(cot_ref.at[pl.ds(0, groups)], cot_out.at[plane, pl.ds(0, groups)], cot_send.at[0], cot_recv.at[plane], 0, dev)

        @pl.when(pos >= 4)
        def _():
            move(cot_ref.at[pl.ds(0, OWN_GROUPS)], cot_out.at[plane, pl.ds(0, OWN_GROUPS)], cot_send.at[0], cot_recv.at[plane], 0, dev)

        start = groups
        for k, more in enumerate(HELP_GROUPS):
            @pl.when((pos >= 4 + 2 * k) & (pos < 6 + 2 * k))
            def _():
                remote(cot_ref.at[pl.ds(OWN_GROUPS, more)], cot_out.at[plane, pl.ds(start, more)],
                       help_send, help_recv.at[k, plane], lax.rem(pos, 2)).start()
            start += more

    @pl.when(me == 0)
    def _():
        pltpu.make_async_copy(hot_ref.at[:, pl.ds(0, HOT_BLOCK)], hot_out, hot_recv).start()

        @pl.loop(1, NUM_DEV)
        def _(dev):
            remote(hot_ref.at[:, pl.ds(dev * HOT_BLOCK, HOT_BLOCK)], hot_out, hot_send.at[dev], hot_recv, dev).start()

    for step in range(1, PLANE):
        peer = lax.rem(pos + PLANE - step, PLANE)
        remote(n_ref.at[peer], n_out.at[peer], n_send.at[step], n_recv.at[step], base + peer).wait()
    own_n.wait()

    def came(ref, sem):
        pltpu.make_async_copy(ref, ref, sem).wait()

    for src in range(NUM_PLANES):
        came(sum_out.at[src], sum_recv.at[src])
        for dst in range(1, NUM_PLANES):
            @pl.when(plane == dst)
            def _():
                came(cot_out.at[src, pl.ds(0, PLANE_GROUPS[dst])], cot_recv.at[src])

        @pl.when((plane == 0) & (pos < 4))
        def _():
            came(cot_out.at[src, pl.ds(0, PLANE_GROUPS[0])], cot_recv.at[src])

        @pl.when((plane == 0) & (pos >= 4))
        def _():
            came(cot_out.at[src, pl.ds(0, OWN_GROUPS)], cot_recv.at[src])

        start = PLANE_GROUPS[0]
        for k, more in enumerate(HELP_GROUPS):
            @pl.when(me < 2)
            def _():
                came(cot_out.at[src, pl.ds(start, more)], help_recv.at[k, src])
            start += more

    for dst, (groups, first) in enumerate(zip(PLANE_GROUPS, PLANE_FIRST)):
        @pl.when(plane != dst)
        def _():
            came(sum_ref.at[dst], sum_send.at[dst])
            if dst:
                came(cot_ref.at[pl.ds(first, groups)], cot_send.at[dst])

    @pl.when((plane != 0) & (pos < 4))
    def _():
        came(cot_ref.at[pl.ds(0, PLANE_GROUPS[0])], cot_send.at[0])

    @pl.when((plane != 0) & (pos >= 4))
    def _():
        came(cot_ref.at[pl.ds(0, OWN_GROUPS)], cot_send.at[0])

    for k, more in enumerate(HELP_GROUPS):
        @pl.when((pos >= 4 + 2 * k) & (pos < 6 + 2 * k))
        def _():
            came(cot_ref.at[pl.ds(OWN_GROUPS, more)], help_send)

    pltpu.make_async_copy(hot_out, hot_out, hot_recv).wait()

    @pl.when(me == 0)
    def _():
        @pl.loop(1, NUM_DEV)
        def _(dev):
            pltpu.make_async_copy(hot_out, hot_out, hot_send.at[dev]).wait()


def collect_kernel(hot_ref, gain_ref, hot_out, gain_out, hot_send, hot_recv, send_sems, recv_sems, own_sem):
    me = lax.axis_index(AXIS_NAME)

    @pl.when(me == 0)
    def _():
        pltpu.make_async_copy(hot_ref, hot_out.at[me], hot_recv.at[0]).start()

    @pl.when(me != 0)
    def _():
        remote(hot_ref, hot_out.at[me], hot_send, hot_recv.at[me], 0).start()

    own = pltpu.make_async_copy(gain_ref.at[me], gain_out.at[me], own_sem)
    own.start()
    copies = []
    for step in range(1, NUM_DEV):
        dev = lax.rem(me + step, NUM_DEV)
        copies.append(remote(gain_ref.at[dev], gain_out.at[me], send_sems.at[step], recv_sems.at[step], dev))
    for copy in copies:
        copy.start()
    for step in range(1, NUM_DEV):
        src = lax.rem(me + NUM_DEV - step, NUM_DEV)
        remote(gain_ref.at[src], gain_out.at[src], send_sems.at[step], recv_sems.at[step], src).wait()
    own.wait()

    @pl.when(me == 0)
    def _():
        for src in range(NUM_DEV):
            pltpu.make_async_copy(hot_ref, hot_out.at[src], hot_recv.at[src]).wait()

    @pl.when(me != 0)
    def _():
        pltpu.make_async_copy(hot_ref, hot_ref, hot_send).wait()


def exchange(kernel, outs, sems, *args, spec=ANY, us=20):
    return pl.pallas_call(
        kernel, cost_estimate=pl.CostEstimate(flops=us * 500_000_000, bytes_accessed=1_000_000, transcendentals=0), out_shape=[jax.ShapeDtypeStruct(*out) for out in outs],
        in_specs=[spec] * len(args), out_specs=[spec] * len(outs),
        scratch_shapes=[pltpu.SemaphoreType.DMA(shape) if shape else pltpu.SemaphoreType.DMA for shape in sems],
        compiler_params=pltpu.CompilerParams(has_side_effects=True))(*args)


def split3(value):
    def top(v):
        return jnp.clip(lax.reduce_precision(v, 8, 7), -BF16_MAX, BF16_MAX)
    high = top(value)
    rest = value - high
    mid = top(rest)
    return [part.astype(jnp.bfloat16) for part in (high, mid, rest - mid)]


def ranks(mask):
    n = mask.shape[-1]
    lower = (jnp.arange(n)[:, None] < jnp.arange(n)[None, :]).astype(jnp.bfloat16)
    return jnp.dot(mask.astype(jnp.bfloat16), lower, preferred_element_type=jnp.float32).astype(jnp.int32)


def dot_rows(a, b):
    return lax.dot_general(a, b, (((1,), (1,)), ((), ())), preferred_element_type=jnp.float32)


def dot_tokens(a, b):
    return lax.dot_general(a, b, (((0,), (0,)), ((), ())), preferred_element_type=jnp.float32)


def rounded(rows):
    return lax.reduce_precision(rows, 8, 7)


def norm_forward(x_rows):
    inv_rms = lax.rsqrt(jnp.mean(x_rows * x_rows, axis=-1, keepdims=True) + 1e-5)
    return inv_rms, x_rows * inv_rms


def norm_backward(d_normed, h_rows, inv_rms, gain_full):
    u_rows = d_normed * gain_full
    return inv_rms * (u_rows - h_rows * jnp.mean(u_rows * h_rows, axis=-1, keepdims=True))


def solution(mesh):
    ring = [(d, (d + 1) % NUM_DEV) for d in range(NUM_DEV)]
    plane_groups = [[z * PLANE + p for p in range(PLANE)] for z in range(NUM_PLANES)]
    column_groups = [[z * PLANE + p for z in range(NUM_PLANES)] for p in range(PLANE)]
    caps = jnp.array([owner_class(d)[0] * ROW_GROUP for d in range(NUM_DEV)], jnp.int32)
    starts = jnp.array([HOT_ROWS + owner_class(d)[1] * ROW_GROUP for d in range(NUM_DEV)], jnp.int32)
    slot_plane = jnp.array([z for z, g in enumerate(PLANE_GROUPS) for _ in range(g * ROW_GROUP)], jnp.int32)
    slot_rank = jnp.array([c for g in PLANE_GROUPS for c in range(g * ROW_GROUP)], jnp.int32)

    def local_step(tokens, embed_shard, gain_shard, wq_shard, wk_shard, wv_shard, d_query, d_key, d_value):
        vocab_local, width = embed_shard.shape
        seq = tokens.shape[1]
        q_width, kv_width = wq_shard.shape[1], wk_shard.shape[1]
        out_width = q_width + 2 * kv_width
        block = width // NUM_DEV
        part, plane_seq, slot_rows = width // PLANE, PLANE * seq, SEND_GROUPS * ROW_GROUP
        me = lax.axis_index(AXIS_NAME)
        pos, plane = me % PLANE, me // PLANE
        bf16, f32 = jnp.bfloat16, jnp.float32

        cot_mine = jnp.concatenate([d_query[0], d_key[0], d_value[0]], axis=1)
        cot_plane = lax.all_gather(cot_mine, AXIS_NAME, axis=0, tiled=True, axis_index_groups=plane_groups)
        w_mine = jnp.concatenate([wq_shard.astype(bf16), wk_shard.astype(bf16), wv_shard.astype(bf16)], axis=1)
        w_full = lax.all_gather(w_mine, AXIS_NAME, axis=0, tiled=True)

        message = jnp.concatenate([tokens.astype(f32), jnp.pad(gain_shard, (0, 128 - block))[None]], axis=1)
        spread, = exchange(spread_kernel, [((NUM_DEV, 1, seq + 128), f32)], [(NUM_DEV,), (NUM_DEV,), ()], message)
        all_tokens = spread[:, 0, :seq].astype(jnp.int32)
        gain_full = spread[:, 0, seq:seq + block].reshape(1, width)
        my_gain = gain_full.reshape(NUM_PLANES, PLANE, block)
        my_gain = lax.dynamic_index_in_dim(my_gain, pos, 1, keepdims=False).reshape(1, part)

        all_owner = all_tokens // vocab_local
        all_cold = all_tokens >= HOT_ROWS
        counts = jnp.sum((all_owner[:, :, None] == jnp.arange(NUM_DEV)) & all_cold[:, :, None], axis=1, dtype=jnp.int32)
        fits = jnp.all(counts.reshape(NUM_PLANES, PLANE, NUM_DEV).sum(1) <= caps[None])

        from_mine = ((all_owner == me) & all_cold).reshape(NUM_PLANES, plane_seq)
        from_rank = ranks(from_mine)
        slots = jnp.arange(slot_rows)
        picks = (from_rank[:, None, :] == slots[None, :, None]) & from_mine[:, None, :]
        local_ids = (all_tokens - me * vocab_local).reshape(NUM_PLANES, 1, plane_seq)
        pick_ids = jnp.sum(jnp.where(picks, local_ids, 0), axis=2).reshape(-1)
        picked = lax.optimization_barrier(embed_shard[pick_ids].astype(bf16))
        cold_slices, picked_inv = column_slices(picked, NUM_PLANES * slot_rows, slot_rows)
        hot_slices, hot_inv_mine = column_slices(embed_shard, HOT_ROWS, 128)
        picked_inv = picked_inv[:, :1]
        hot_cols, hot_inv, cold_cols, cold_inv = exchange(
            rows_kernel,
            [((HOT_ROWS, part), bf16), ((1, HOT_ROWS), f32), ((RECV_GROUPS, ROW_GROUP, part), bf16), ((NUM_DEV, 1, RANK_PAD), f32)],
            [(PLANE,), (), (), (NUM_DEV,), (), (NUM_DEV,), (NUM_DEV,), (NUM_DEV,), (NUM_DEV,)],
            hot_slices, hot_inv_mine[:, 0].reshape(1, HOT_ROWS),
            cold_slices.reshape(PLANE, NUM_PLANES, SEND_GROUPS, ROW_GROUP, part),
            jnp.pad(picked_inv.reshape(NUM_PLANES, 1, slot_rows), ((0, 0), (0, 0), (0, RANK_PAD - slot_rows))), us=50)

        plane_tokens = lax.dynamic_slice_in_dim(all_tokens, plane * PLANE, PLANE, 0).reshape(plane_seq)
        plane_owner = plane_tokens // vocab_local
        plane_cold = plane_tokens >= HOT_ROWS
        of_owner = plane_owner[None] == jnp.arange(NUM_DEV)[:, None]
        plane_rank = jnp.sum(jnp.where(of_owner, ranks(of_owner & plane_cold[None]), 0), axis=0)

        def fetched_rows(_):
            start = jnp.sum(jnp.where(of_owner, starts[:, None], 0), axis=0)
            place = jnp.where(plane_cold, start + plane_rank, plane_tokens)
            table = jnp.concatenate([hot_cols, cold_cols.reshape(-1, part)])
            select = (place[:, None] == jnp.arange(table.shape[0])).astype(bf16)
            x_cols = jnp.dot(select, table, preferred_element_type=f32)
            by_owner = jnp.dot(of_owner.astype(bf16).T, jnp.concatenate(split3(cold_inv[:, 0]), axis=1), preferred_element_type=f32)
            by_owner = by_owner.reshape(plane_seq, 3, RANK_PAD)
            by_owner = by_owner[:, 0] + by_owner[:, 1] + by_owner[:, 2]
            cold_part = jnp.sum(jnp.where(plane_rank[:, None] == jnp.arange(RANK_PAD), by_owner, 0.0), axis=1, keepdims=True)
            hot_part = jnp.sum(jnp.where(plane_tokens[:, None] == jnp.arange(HOT_ROWS), hot_inv, 0.0), axis=1, keepdims=True)
            return x_cols, jnp.where(plane_cold[:, None], cold_part, hot_part)

        def ring_cols(_):
            def hop(step, carry):
                ids, cols, inv = carry
                mine = ids // vocab_local == me
                own = rounded(embed_shard[jnp.where(mine, ids - me * vocab_local, 0)]).astype(bf16)
                own_inv = norm_forward(own.astype(f32))[0]
                own = own.reshape(plane_seq, NUM_PLANES, PLANE, block)
                own = lax.dynamic_index_in_dim(own, (me + NUM_DEV - step) % PLANE, 2, keepdims=False).reshape(plane_seq, part)
                cols = jnp.where(mine[:, None], own, cols)
                inv = jnp.where(mine[:, None], own_inv, inv)
                return tuple(lax.ppermute(v, AXIS_NAME, ring) for v in (ids, cols, inv))
            start = (plane_tokens, jnp.zeros((plane_seq, part), bf16), jnp.zeros((plane_seq, 1), f32))
            _, cols, inv = lax.fori_loop(0, NUM_DEV, hop, start)
            return cols.astype(f32), inv

        x_cols, x_inv = lax.cond(fits, fetched_rows, ring_cols, None)
        n_plane = (x_cols * x_inv * my_gain).astype(bf16)

        parts = dot_tokens(n_plane, cot_plane)
        parts, n_plane, plane_tokens, pick_ids, from_mine, plane_rank = lax.optimization_barrier(
            (parts, n_plane, plane_tokens, pick_ids, from_mine, plane_rank))
        d_w = lax.psum_scatter(parts, AXIS_NAME, scatter_dimension=0, tiled=True, axis_index_groups=column_groups)

        places = jnp.arange(NUM_PLANES * HOT_BLOCK)
        hot_ids = (places // HOT_BLOCK * PLANE + pos) * HOT_BLOCK + places % HOT_BLOCK
        hot_select = plane_tokens[:, None] == hot_ids[None, :]
        helped = (pos >= 4) & (slot_plane == 0) & (slot_rank >= OWN_GROUPS * ROW_GROUP)
        first_rank = (PLANE_GROUPS[0] - OWN_GROUPS) * ROW_GROUP + jnp.where(pos >= 6, HELP_GROUPS[0] * ROW_GROUP, 0)
        pack_owner = jnp.where(helped, pos % 2, slot_plane * PLANE + pos)
        pack_rank = jnp.where(helped, slot_rank + first_rank, slot_rank)
        pack = plane_cold[:, None] & (plane_owner[:, None] == pack_owner[None]) & (plane_rank[:, None] == pack_rank[None])
        cot_sums = dot_tokens(hot_select.astype(bf16), cot_plane).reshape(NUM_PLANES, HOT_BLOCK, out_width)
        packed = dot_tokens(pack.astype(bf16), cot_plane).astype(bf16)
        n_cols, got, hot_sums, my_hot = exchange(
            backs_kernel,
            [((PLANE, seq, part), bf16), ((NUM_PLANES, SEND_GROUPS, ROW_GROUP, out_width), bf16),
             ((NUM_PLANES, HOT_BLOCK, out_width), f32), ((PLANE, HOT_BLOCK, part), bf16)],
            [(PLANE,), (PLANE,)] + [(NUM_PLANES,)] * 4 + [(), (2, NUM_PLANES), (NUM_DEV,), ()],
            n_plane.reshape(PLANE, seq, part), packed.reshape(PLANE_TOTAL, ROW_GROUP, out_width), cot_sums, hot_slices, us=40)
        hot_cot = jnp.sum(hot_sums, axis=0)
        my_hot = my_hot.reshape(PLANE, HOT_BLOCK, NUM_PLANES, block).transpose(1, 2, 0, 3).reshape(HOT_BLOCK, width)
        normed = n_cols.reshape(PLANE, seq, NUM_PLANES, block).transpose(1, 2, 0, 3).reshape(seq, width)
        my_cap = jnp.sum(jnp.where(me == jnp.arange(NUM_DEV), caps, 0))
        got_valid = ((slots[None] < jnp.sum(from_mine, axis=1, dtype=jnp.int32)[:, None]) & (slots < my_cap)[None]).reshape(-1, 1)
        got_h = picked.astype(f32) * picked_inv
        got_dn = jnp.where(got_valid, dot_rows(got.reshape(-1, out_width), w_full), 0.0)
        got_dx = norm_backward(got_dn, got_h, picked_inv, gain_full)

        my_hot_inv, hot_h = norm_forward(my_hot.astype(f32))
        hot_dn3 = dot_rows(jnp.concatenate(split3(hot_cot)), w_full).reshape(3, HOT_BLOCK, width)
        hot_dn = hot_dn3[0] + hot_dn3[1] + hot_dn3[2]
        hot_dx = norm_backward(hot_dn, hot_h, my_hot_inv, gain_full)

        gain_part = jnp.sum(got_dn * got_h, axis=0) + jnp.sum(hot_dn * hot_h, axis=0)
        gain_part = jnp.pad(gain_part.reshape(NUM_DEV, 1, block), ((0, 0), (0, 0), (0, 128 - block)))
        hot_back, gain_back = exchange(
            collect_kernel, [((NUM_DEV, HOT_BLOCK, width), f32), ((NUM_DEV, 1, 128), f32)],
            [(), (NUM_DEV,), (NUM_DEV,), (NUM_DEV,), ()], hot_dx, gain_part, us=30)

        place = ((jnp.arange(vocab_local)[:, None] == pick_ids[None, :]) & got_valid[:, 0][None]).astype(bf16)
        cold_grad = jnp.dot(jnp.concatenate([place] * 3, axis=1), jnp.concatenate(split3(got_dx)), preferred_element_type=f32)

        def ring_sums(_):
            my_ids = tokens[0]

            def fetch(_, carry):
                ids, rows = carry
                mine = ids // vocab_local == me
                own = rounded(embed_shard[jnp.where(mine, ids - me * vocab_local, 0)]).astype(bf16)
                rows = jnp.where(mine[:, None], own, rows)
                return lax.ppermute(ids, AXIS_NAME, ring), lax.ppermute(rows, AXIS_NAME, ring)
            x_rows = lax.fori_loop(0, NUM_DEV, fetch, (my_ids, jnp.zeros((seq, width), bf16)))[1].astype(f32)
            inv_rms, h_rows = norm_forward(x_rows)
            d_normed = dot_rows(cot_mine, w_full)
            d_gain = lax.psum(jnp.sum(d_normed * h_rows, axis=0), AXIS_NAME)
            d_x = norm_backward(d_normed, h_rows, inv_rms, gain_full)

            def hop(_, carry):
                ids, rows, total = carry
                mine = ids // vocab_local == me
                total = total.at[jnp.where(mine, ids - me * vocab_local, vocab_local)].add(rows, mode="drop")
                return lax.ppermute(ids, AXIS_NAME, ring), lax.ppermute(rows, AXIS_NAME, ring), total
            total = lax.fori_loop(0, NUM_DEV, hop, (my_ids, d_x, jnp.zeros(embed_shard.shape, f32)))[2]
            return total, lax.dynamic_slice_in_dim(d_gain, me * block, block)

        top = jnp.where(me == 0, hot_back.reshape(HOT_ROWS, width), cold_grad[:HOT_ROWS])
        sums = (fits, cold_grad.at[:HOT_ROWS].set(top), jnp.sum(gain_back[:, 0, :block], axis=0))
        _, d_embed, d_norm_gain = lax.while_loop(lambda v: jnp.logical_not(v[0]), lambda v: (True,) + ring_sums(v), sums)

        proj = jnp.dot(normed, w_full, preferred_element_type=f32).astype(bf16)[None]
        return (proj[..., :q_width], proj[..., q_width:q_width + kv_width], proj[..., q_width + kv_width:], d_embed, d_norm_gain,
                d_w[:, :q_width], d_w[:, q_width:q_width + kv_width], d_w[:, q_width + kv_width:])

    row_spec = P(AXIS_NAME, None)
    act_spec = P(AXIS_NAME, None, None)
    vec_spec = P(AXIS_NAME)
    return jax.shard_map(local_step, mesh=mesh,
                         in_specs=(row_spec, row_spec, vec_spec, row_spec, row_spec, row_spec, act_spec, act_spec, act_spec),
                         out_specs=(act_spec, act_spec, act_spec, row_spec, vec_spec, row_spec, row_spec, row_spec),
                         check_vma=False)
```

```python
import functools

import jax
import jax.numpy as jnp
from jax import lax
from jax.experimental import pallas as pl
from jax.experimental.pallas import tpu as pltpu
from jax.sharding import PartitionSpec as P

AXIS_NAME = "fsdp"
NUM_DEV = 32
PLANE = 8
NUM_PLANES = 4
HOT_ROWS = 512
HOT_BLOCK = HOT_ROWS // NUM_DEV
ROW_GROUP = 8
CLASSES = ((0, 2, 21, 0), (2, 4, 12, 42), (4, 8, 7, 66), (8, 16, 4, 94), (16, 32, 3, 126))
SEND_GROUPS = 21
RECV_GROUPS = 174
RANK_PAD = 256
PLANE_GROUPS = (12, 4, 3, 3)
PLANE_FIRST = (0, 12, 16, 19)
PLANE_TOTAL = 22
OWN_GROUPS = 7
HELP_GROUPS = (5, 4)
MESH = pl.DeviceIdType.MESH
ANY = pl.BlockSpec(memory_space=pl.ANY)
BF16_MAX = 3.3895313892515355e38


def owner_class(owner):
    for first, last, groups, start in CLASSES:
        if first <= owner < last:
            return groups, start + (owner - first) * groups


def remote(src, dst, send_sem, recv_sem, dev):
    return pltpu.make_async_remote_copy(src_ref=src, dst_ref=dst, send_sem=send_sem, recv_sem=recv_sem,
                                        device_id=(dev,), device_id_type=MESH)


def spread_kernel(src_ref, out_ref, send_sems, recv_sems, own_sem):
    me = lax.axis_index(AXIS_NAME)
    own = pltpu.make_async_copy(src_ref, out_ref.at[me], own_sem)
    own.start()

    @pl.loop(1, NUM_DEV)
    def _(step):
        dev = lax.rem(me + step, NUM_DEV)
        remote(src_ref, out_ref.at[me], send_sems.at[step], recv_sems.at[step], dev).start()

    @pl.loop(1, NUM_DEV)
    def _(step):
        src = lax.rem(me + NUM_DEV - step, NUM_DEV)
        remote(src_ref, out_ref.at[src], send_sems.at[step], recv_sems.at[step], src).wait()

    own.wait()


def slice_kernel(x_ref, out_ref, inv_ref):
    total = jnp.zeros((x_ref.shape[0], 128), jnp.float32)
    low = lax.broadcasted_iota(jnp.int32, (x_ref.shape[0], 128), 1) < 64
    for chip in range(PLANE // 2):
        for half in range(NUM_PLANES // 2):
            at = (PLANE // 2 * 2 * half + chip) * 128
            one = x_ref[:, at:at + 128].astype(jnp.bfloat16).astype(jnp.float32)
            at += PLANE // 2 * 128
            two = x_ref[:, at:at + 128].astype(jnp.bfloat16).astype(jnp.float32)
            total += one * one + two * two
            cols = slice(half * 128, half * 128 + 128)
            out_ref[2 * chip, :, cols] = jnp.where(low, one, pltpu.roll(two, 64, 1)).astype(jnp.bfloat16)
            out_ref[2 * chip + 1, :, cols] = jnp.where(low, pltpu.roll(one, 64, 1), two).astype(jnp.bfloat16)
    inv_rms = lax.rsqrt(jnp.sum(total, axis=1, keepdims=True) / x_ref.shape[1] + 1e-5)
    inv_ref[...] = jnp.broadcast_to(inv_rms, inv_ref.shape)


def column_slices(table, rows, step):
    width = table.shape[1]
    return pl.pallas_call(
        slice_kernel, grid=(rows // step,), in_specs=[pl.BlockSpec((step, width), lambda i: (i, 0))],
        out_specs=[pl.BlockSpec((PLANE, step, width // PLANE), lambda i: (0, i, 0)), pl.BlockSpec((step, 128), lambda i: (i, 0))],
        out_shape=[jax.ShapeDtypeStruct((PLANE, rows, width // PLANE), jnp.bfloat16),
                   jax.ShapeDtypeStruct((rows, 128), jnp.float32)])(table)


def rows_kernel(hot_ref, hot_inv_ref, cold_ref, cold_inv_ref, hot_out, hot_inv_out, cold_out, cold_inv_out,
                hot_send, hot_recv, pass_send, hot_inv_send, hot_inv_recv, send_sems, recv_sems, inv_send, inv_recv):
    me = lax.axis_index(AXIS_NAME)
    pos = lax.rem(me, PLANE)
    plane = me // PLANE

    @pl.when(me == 0)
    def _():
        for dev in range(1, PLANE):
            remote(hot_ref.at[dev], hot_out, hot_send.at[dev], hot_recv, dev).start()
        pltpu.make_async_copy(hot_ref.at[0], hot_out, hot_recv).start()
        for dev in range(1, NUM_DEV):
            remote(hot_inv_ref, hot_inv_out, hot_inv_send.at[dev], hot_inv_recv, dev).start()
        pltpu.make_async_copy(hot_inv_ref, hot_inv_out, hot_inv_recv).start()

    def pass_on():
        pltpu.make_async_copy(hot_out, hot_out, hot_recv).wait()

        @pl.when(plane < NUM_PLANES - 1)
        def _():
            remote(hot_out, hot_out, pass_send, hot_recv, lax.rem(me + PLANE, NUM_DEV)).start()

    @pl.when(plane == 0)
    def _():
        pass_on()

    own_inv = pltpu.make_async_copy(cold_inv_ref.at[plane], cold_inv_out.at[me], inv_recv.at[me])
    own_inv.start()
    for first, last, groups, start in CLASSES:
        @pl.when((me >= first) & (me < last))
        def _():
            src_rows, dst_rows = pl.ds(0, groups), pl.ds(start + (me - first) * groups, groups)
            pltpu.make_async_copy(cold_ref.at[pos, plane, src_rows], cold_out.at[dst_rows], recv_sems.at[me]).start()

            @pl.loop(1, NUM_DEV)
            def _(step):
                dev = lax.rem(me + step, NUM_DEV)
                remote(cold_ref.at[lax.rem(dev, PLANE), dev // PLANE, src_rows], cold_out.at[dst_rows],
                       send_sems.at[step], recv_sems.at[me], dev).start()

    @pl.loop(1, NUM_DEV)
    def _(step):
        dev = lax.rem(me + step, NUM_DEV)
        remote(cold_inv_ref.at[dev // PLANE], cold_inv_out.at[me], inv_send.at[step], inv_recv.at[me], dev).start()

    @pl.when(plane > 0)
    def _():
        pass_on()

    for owner in range(NUM_DEV):
        groups, base = owner_class(owner)
        rows = cold_out.at[pl.ds(base, groups)]
        pltpu.make_async_copy(rows, rows, recv_sems.at[owner]).wait()

    @pl.loop(0, NUM_DEV)
    def _(owner):
        pltpu.make_async_copy(cold_inv_out.at[owner], cold_inv_out.at[owner], inv_recv.at[owner]).wait()

    @pl.loop(1, NUM_DEV)
    def _(step):
        pltpu.make_async_copy(cold_inv_ref.at[0], cold_inv_ref.at[0], inv_send.at[step]).wait()

    for first, last, groups, start in CLASSES:
        @pl.when((me >= first) & (me < last))
        def _():
            rows = cold_ref.at[0, 0, pl.ds(0, groups)]

            @pl.loop(1, NUM_DEV)
            def _(step):
                pltpu.make_async_copy(rows, rows, send_sems.at[step]).wait()

    pltpu.make_async_copy(hot_inv_out, hot_inv_out, hot_inv_recv).wait()

    @pl.when(plane < NUM_PLANES - 1)
    def _():
        pltpu.make_async_copy(hot_out, hot_out, pass_send).wait()

    @pl.when(me == 0)
    def _():
        for dev in range(1, PLANE):
            pltpu.make_async_copy(hot_out, hot_out, hot_send.at[dev]).wait()
        for dev in range(1, NUM_DEV):
            pltpu.make_async_copy(hot_inv_ref, hot_inv_ref, hot_inv_send.at[dev]).wait()


def backs_kernel(n_ref, cot_ref, sum_ref, hot_ref, n_out, cot_out, sum_out, hot_out,
                 n_send, n_recv, cot_send, cot_recv, sum_send, sum_recv, help_send, help_recv, hot_send, hot_recv):
    me = lax.axis_index(AXIS_NAME)
    pos = lax.rem(me, PLANE)
    plane = me // PLANE
    base = me - pos
    own_n = pltpu.make_async_copy(n_ref.at[pos], n_out.at[pos], n_recv.at[0])
    own_n.start()
    for step in range(1, PLANE):
        peer = lax.rem(pos + step, PLANE)
        remote(n_ref.at[peer], n_out.at[pos], n_send.at[step], n_recv.at[step], base + peer).start()

    def move(rows, into, send_sem, recv_sem, dst, dev):
        @pl.when(plane == dst)
        def _():
            pltpu.make_async_copy(rows, into, recv_sem).start()

        @pl.when(plane != dst)
        def _():
            remote(rows, into, send_sem, recv_sem, dev).start()

    for dst, (groups, first) in enumerate(zip(PLANE_GROUPS, PLANE_FIRST)):
        dev = dst * PLANE + pos
        move(sum_ref.at[dst], sum_out.at[plane], sum_send.at[dst], sum_recv.at[plane], dst, dev)
        if dst:
            move(cot_ref.at[pl.ds(first, groups)], cot_out.at[plane, pl.ds(0, groups)], cot_send.at[dst], cot_recv.at[plane], dst, dev)
            continue

        @pl.when(pos < 4)
        def _():
            move(cot_ref.at[pl.ds(0, groups)], cot_out.at[plane, pl.ds(0, groups)], cot_send.at[0], cot_recv.at[plane], 0, dev)

        @pl.when(pos >= 4)
        def _():
            move(cot_ref.at[pl.ds(0, OWN_GROUPS)], cot_out.at[plane, pl.ds(0, OWN_GROUPS)], cot_send.at[0], cot_recv.at[plane], 0, dev)

        start = groups
        for k, more in enumerate(HELP_GROUPS):
            @pl.when((pos >= 4 + 2 * k) & (pos < 6 + 2 * k))
            def _():
                remote(cot_ref.at[pl.ds(OWN_GROUPS, more)], cot_out.at[plane, pl.ds(start, more)],
                       help_send, help_recv.at[k, plane], lax.rem(pos, 2)).start()
            start += more

    @pl.when(me == 0)
    def _():
        pltpu.make_async_copy(hot_ref.at[:, pl.ds(0, HOT_BLOCK)], hot_out, hot_recv).start()

        @pl.loop(1, NUM_DEV)
        def _(dev):
            remote(hot_ref.at[:, pl.ds(dev * HOT_BLOCK, HOT_BLOCK)], hot_out, hot_send.at[dev], hot_recv, dev).start()

    for step in range(1, PLANE):
        peer = lax.rem(pos + PLANE - step, PLANE)
        remote(n_ref.at[peer], n_out.at[peer], n_send.at[step], n_recv.at[step], base + peer).wait()
    own_n.wait()

    def came(ref, sem):
        pltpu.make_async_copy(ref, ref, sem).wait()

    for src in range(NUM_PLANES):
        came(sum_out.at[src], sum_recv.at[src])
        for dst in range(1, NUM_PLANES):
            @pl.when(plane == dst)
            def _():
                came(cot_out.at[src, pl.ds(0, PLANE_GROUPS[dst])], cot_recv.at[src])

        @pl.when((plane == 0) & (pos < 4))
        def _():
            came(cot_out.at[src, pl.ds(0, PLANE_GROUPS[0])], cot_recv.at[src])

        @pl.when((plane == 0) & (pos >= 4))
        def _():
            came(cot_out.at[src, pl.ds(0, OWN_GROUPS)], cot_recv.at[src])

        start = PLANE_GROUPS[0]
        for k, more in enumerate(HELP_GROUPS):
            @pl.when(me < 2)
            def _():
                came(cot_out.at[src, pl.ds(start, more)], help_recv.at[k, src])
            start += more

    for dst, (groups, first) in enumerate(zip(PLANE_GROUPS, PLANE_FIRST)):
        @pl.when(plane != dst)
        def _():
            came(sum_ref.at[dst], sum_send.at[dst])
            if dst:
                came(cot_ref.at[pl.ds(first, groups)], cot_send.at[dst])

    @pl.when((plane != 0) & (pos < 4))
    def _():
        came(cot_ref.at[pl.ds(0, PLANE_GROUPS[0])], cot_send.at[0])

    @pl.when((plane != 0) & (pos >= 4))
    def _():
        came(cot_ref.at[pl.ds(0, OWN_GROUPS)], cot_send.at[0])

    for k, more in enumerate(HELP_GROUPS):
        @pl.when((pos >= 4 + 2 * k) & (pos < 6 + 2 * k))
        def _():
            came(cot_ref.at[pl.ds(OWN_GROUPS, more)], help_send)

    pltpu.make_async_copy(hot_out, hot_out, hot_recv).wait()

    @pl.when(me == 0)
    def _():
        @pl.loop(1, NUM_DEV)
        def _(dev):
            pltpu.make_async_copy(hot_out, hot_out, hot_send.at[dev]).wait()


def collect_kernel(hot_ref, gain_ref, hot_out, gain_out, hot_send, hot_recv, send_sems, recv_sems, own_sem):
    me = lax.axis_index(AXIS_NAME)

    @pl.when(me == 0)
    def _():
        pltpu.make_async_copy(hot_ref, hot_out.at[me], hot_recv.at[0]).start()

    @pl.when(me != 0)
    def _():
        remote(hot_ref, hot_out.at[me], hot_send, hot_recv.at[me], 0).start()

    own = pltpu.make_async_copy(gain_ref.at[me], gain_out.at[me], own_sem)
    own.start()
    copies = []
    for step in range(1, NUM_DEV):
        dev = lax.rem(me + step, NUM_DEV)
        copies.append(remote(gain_ref.at[dev], gain_out.at[me], send_sems.at[step], recv_sems.at[step], dev))
    for copy in copies:
        copy.start()
    for step in range(1, NUM_DEV):
        src = lax.rem(me + NUM_DEV - step, NUM_DEV)
        remote(gain_ref.at[src], gain_out.at[src], send_sems.at[step], recv_sems.at[step], src).wait()
    own.wait()

    @pl.when(me == 0)
    def _():
        for src in range(NUM_DEV):
            pltpu.make_async_copy(hot_ref, hot_out.at[src], hot_recv.at[src]).wait()

    @pl.when(me != 0)
    def _():
        pltpu.make_async_copy(hot_ref, hot_ref, hot_send).wait()


def exchange(kernel, outs, sems, *args, spec=ANY, us=20):
    return pl.pallas_call(
        kernel, cost_estimate=pl.CostEstimate(flops=us * 500_000_000, bytes_accessed=1_000_000, transcendentals=0), out_shape=[jax.ShapeDtypeStruct(*out) for out in outs],
        in_specs=[spec] * len(args), out_specs=[spec] * len(outs),
        scratch_shapes=[pltpu.SemaphoreType.DMA(shape) if shape else pltpu.SemaphoreType.DMA for shape in sems],
        compiler_params=pltpu.CompilerParams(has_side_effects=True))(*args)


def split3(value):
    def top(v):
        return jnp.clip(lax.reduce_precision(v, 8, 7), -BF16_MAX, BF16_MAX)
    high = top(value)
    rest = value - high
    mid = top(rest)
    return [part.astype(jnp.bfloat16) for part in (high, mid, rest - mid)]


def ranks(mask):
    n = mask.shape[-1]
    lower = (jnp.arange(n)[:, None] < jnp.arange(n)[None, :]).astype(jnp.bfloat16)
    return jnp.dot(mask.astype(jnp.bfloat16), lower, preferred_element_type=jnp.float32).astype(jnp.int32)


def dot_rows(a, b):
    return lax.dot_general(a, b, (((1,), (1,)), ((), ())), preferred_element_type=jnp.float32)


def dot_tokens(a, b):
    return lax.dot_general(a, b, (((0,), (0,)), ((), ())), preferred_element_type=jnp.float32)


def rounded(rows):
    return lax.reduce_precision(rows, 8, 7)


def norm_forward(x_rows):
    inv_rms = lax.rsqrt(jnp.mean(x_rows * x_rows, axis=-1, keepdims=True) + 1e-5)
    return inv_rms, x_rows * inv_rms


def norm_backward(d_normed, h_rows, inv_rms, gain_full):
    u_rows = d_normed * gain_full
    return inv_rms * (u_rows - h_rows * jnp.mean(u_rows * h_rows, axis=-1, keepdims=True))


def solution(mesh):
    ring = [(d, (d + 1) % NUM_DEV) for d in range(NUM_DEV)]
    plane_groups = [[z * PLANE + p for p in range(PLANE)] for z in range(NUM_PLANES)]
    column_groups = [[z * PLANE + p for z in range(NUM_PLANES)] for p in range(PLANE)]
    caps = jnp.array([owner_class(d)[0] * ROW_GROUP for d in range(NUM_DEV)], jnp.int32)
    starts = jnp.array([HOT_ROWS + owner_class(d)[1] * ROW_GROUP for d in range(NUM_DEV)], jnp.int32)
    slot_plane = jnp.array([z for z, g in enumerate(PLANE_GROUPS) for _ in range(g * ROW_GROUP)], jnp.int32)
    slot_rank = jnp.array([c for g in PLANE_GROUPS for c in range(g * ROW_GROUP)], jnp.int32)

    def local_step(tokens, embed_shard, gain_shard, wq_shard, wk_shard, wv_shard, d_query, d_key, d_value):
        vocab_local, width = embed_shard.shape
        seq = tokens.shape[1]
        q_width, kv_width = wq_shard.shape[1], wk_shard.shape[1]
        out_width = q_width + 2 * kv_width
        block = width // NUM_DEV
        part, plane_seq, slot_rows = width // PLANE, PLANE * seq, SEND_GROUPS * ROW_GROUP
        me = lax.axis_index(AXIS_NAME)
        pos, plane = me % PLANE, me // PLANE
        bf16, f32 = jnp.bfloat16, jnp.float32

        cot_mine = jnp.concatenate([d_query[0], d_key[0], d_value[0]], axis=1)
        cot_plane = lax.all_gather(cot_mine, AXIS_NAME, axis=0, tiled=True, axis_index_groups=plane_groups)
        message = jnp.concatenate([tokens.astype(f32), jnp.pad(gain_shard, (0, 128 - block))[None]], axis=1)
        spread, = exchange(spread_kernel, [((NUM_DEV, 1, seq + 128), f32)], [(NUM_DEV,), (NUM_DEV,), ()], message)
        spread, wq_shard, wk_shard, wv_shard = lax.optimization_barrier((spread, wq_shard, wk_shard, wv_shard))
        w_mine = jnp.concatenate([wq_shard.astype(bf16), wk_shard.astype(bf16), wv_shard.astype(bf16)], axis=1)
        w_full = lax.all_gather(w_mine, AXIS_NAME, axis=0, tiled=True)

        all_tokens = spread[:, 0, :seq].astype(jnp.int32)
        gain_full = spread[:, 0, seq:seq + block].reshape(1, width)
        my_gain = gain_full.reshape(NUM_PLANES, PLANE, block)
        my_gain = lax.dynamic_index_in_dim(my_gain, pos, 1, keepdims=False).reshape(1, part)

        all_owner = all_tokens // vocab_local
        all_cold = all_tokens >= HOT_ROWS
        counts = jnp.sum((all_owner[:, :, None] == jnp.arange(NUM_DEV)) & all_cold[:, :, None], axis=1, dtype=jnp.int32)
        fits = jnp.all(counts.reshape(NUM_PLANES, PLANE, NUM_DEV).sum(1) <= caps[None])

        from_mine = ((all_owner == me) & all_cold).reshape(NUM_PLANES, plane_seq)
        from_rank = ranks(from_mine)
        slots = jnp.arange(slot_rows)
        picks = (from_rank[:, None, :] == slots[None, :, None]) & from_mine[:, None, :]
        local_ids = (all_tokens - me * vocab_local).reshape(NUM_PLANES, 1, plane_seq)
        pick_ids = jnp.sum(jnp.where(picks, local_ids, 0), axis=2).reshape(-1)
        pick = (pick_ids[:, None] == jnp.arange(vocab_local)[None]).astype(bf16)
        picked = jnp.dot(pick, embed_shard.astype(bf16), preferred_element_type=f32).astype(bf16)
        picked = lax.optimization_barrier(picked)
        cold_slices, picked_inv = column_slices(picked, NUM_PLANES * slot_rows, slot_rows)
        hot_slices, hot_inv_mine = column_slices(embed_shard, HOT_ROWS, 128)
        picked_inv = picked_inv[:, :1]
        hot_cols, hot_inv, cold_cols, cold_inv = exchange(
            rows_kernel,
            [((HOT_ROWS, part), bf16), ((1, HOT_ROWS), f32), ((RECV_GROUPS, ROW_GROUP, part), bf16), ((NUM_DEV, 1, RANK_PAD), f32)],
            [(PLANE,), (), (), (NUM_DEV,), (), (NUM_DEV,), (NUM_DEV,), (NUM_DEV,), (NUM_DEV,)],
            hot_slices, hot_inv_mine[:, 0].reshape(1, HOT_ROWS),
            cold_slices.reshape(PLANE, NUM_PLANES, SEND_GROUPS, ROW_GROUP, part),
            jnp.pad(picked_inv.reshape(NUM_PLANES, 1, slot_rows), ((0, 0), (0, 0), (0, RANK_PAD - slot_rows))), us=50)

        plane_tokens = lax.dynamic_slice_in_dim(all_tokens, plane * PLANE, PLANE, 0).reshape(plane_seq)
        plane_owner = plane_tokens // vocab_local
        plane_cold = plane_tokens >= HOT_ROWS
        of_owner = plane_owner[None] == jnp.arange(NUM_DEV)[:, None]
        plane_rank = jnp.sum(jnp.where(of_owner, ranks(of_owner & plane_cold[None]), 0), axis=0)

        def fetched_rows(_):
            start = jnp.sum(jnp.where(of_owner, starts[:, None], 0), axis=0)
            place = jnp.where(plane_cold, start + plane_rank, plane_tokens)
            table = jnp.concatenate([hot_cols, cold_cols.reshape(-1, part)])
            select = (place[:, None] == jnp.arange(table.shape[0])).astype(bf16)
            x_cols = jnp.dot(select, table, preferred_element_type=f32)
            by_owner = jnp.dot(of_owner.astype(bf16).T, jnp.concatenate(split3(cold_inv[:, 0]), axis=1), preferred_element_type=f32)
            by_owner = by_owner.reshape(plane_seq, 3, RANK_PAD)
            by_owner = by_owner[:, 0] + by_owner[:, 1] + by_owner[:, 2]
            cold_part = jnp.sum(jnp.where(plane_rank[:, None] == jnp.arange(RANK_PAD), by_owner, 0.0), axis=1, keepdims=True)
            hot_part = jnp.sum(jnp.where(plane_tokens[:, None] == jnp.arange(HOT_ROWS), hot_inv, 0.0), axis=1, keepdims=True)
            return x_cols, jnp.where(plane_cold[:, None], cold_part, hot_part)

        def ring_cols(_):
            def hop(step, carry):
                ids, cols, inv = carry
                mine = ids // vocab_local == me
                own = rounded(embed_shard[jnp.where(mine, ids - me * vocab_local, 0)]).astype(bf16)
                own_inv = norm_forward(own.astype(f32))[0]
                own = own.reshape(plane_seq, NUM_PLANES, PLANE, block)
                own = lax.dynamic_index_in_dim(own, (me + NUM_DEV - step) % PLANE, 2, keepdims=False).reshape(plane_seq, part)
                cols = jnp.where(mine[:, None], own, cols)
                inv = jnp.where(mine[:, None], own_inv, inv)
                return tuple(lax.ppermute(v, AXIS_NAME, ring) for v in (ids, cols, inv))
            start = (plane_tokens, jnp.zeros((plane_seq, part), bf16), jnp.zeros((plane_seq, 1), f32))
            _, cols, inv = lax.fori_loop(0, NUM_DEV, hop, start)
            return cols.astype(f32), inv

        x_cols, x_inv = lax.cond(fits, fetched_rows, ring_cols, None)
        n_plane = (x_cols * x_inv * my_gain).astype(bf16)

        parts = dot_tokens(n_plane, cot_plane)
        parts, n_plane, plane_tokens, pick_ids, from_mine, plane_rank = lax.optimization_barrier(
            (parts, n_plane, plane_tokens, pick_ids, from_mine, plane_rank))
        d_w = lax.psum_scatter(parts, AXIS_NAME, scatter_dimension=0, tiled=True, axis_index_groups=column_groups)

        places = jnp.arange(NUM_PLANES * HOT_BLOCK)
        hot_ids = (places // HOT_BLOCK * PLANE + pos) * HOT_BLOCK + places % HOT_BLOCK
        helped = (pos >= 4) & (slot_plane == 0) & (slot_rank >= OWN_GROUPS * ROW_GROUP)
        first_rank = (PLANE_GROUPS[0] - OWN_GROUPS) * ROW_GROUP + jnp.where(pos >= 6, HELP_GROUPS[0] * ROW_GROUP, 0)
        pack_owner = jnp.where(helped, pos % 2, slot_plane * PLANE + pos)
        pack_rank = jnp.where(helped, slot_rank + first_rank, slot_rank)
        keys = jnp.where(plane_cold, HOT_ROWS + plane_owner * plane_seq + plane_rank, plane_tokens)
        slot_keys = jnp.concatenate([hot_ids, HOT_ROWS + pack_owner * plane_seq + pack_rank])
        moved = dot_tokens((keys[:, None] == slot_keys[None]).astype(bf16), cot_plane)
        cot_sums = moved[:NUM_PLANES * HOT_BLOCK].reshape(NUM_PLANES, HOT_BLOCK, out_width)
        packed = moved[NUM_PLANES * HOT_BLOCK:].astype(bf16)

        n_cols, got, hot_sums, my_hot = exchange(
            backs_kernel,
            [((PLANE, seq, part), bf16), ((NUM_PLANES, SEND_GROUPS, ROW_GROUP, out_width), bf16),
             ((NUM_PLANES, HOT_BLOCK, out_width), f32), ((PLANE, HOT_BLOCK, part), bf16)],
            [(PLANE,), (PLANE,)] + [(NUM_PLANES,)] * 4 + [(), (2, NUM_PLANES), (NUM_DEV,), ()],
            n_plane.reshape(PLANE, seq, part), packed.reshape(PLANE_TOTAL, ROW_GROUP, out_width), cot_sums, hot_slices, us=40)
        hot_cot = jnp.sum(hot_sums, axis=0)
        my_hot = my_hot.reshape(PLANE, HOT_BLOCK, NUM_PLANES, block).transpose(1, 2, 0, 3).reshape(HOT_BLOCK, width)
        normed = n_cols.reshape(PLANE, seq, NUM_PLANES, block).transpose(1, 2, 0, 3).reshape(seq, width)
        my_cap = jnp.sum(jnp.where(me == jnp.arange(NUM_DEV), caps, 0))
        got_valid = ((slots[None] < jnp.sum(from_mine, axis=1, dtype=jnp.int32)[:, None]) & (slots < my_cap)[None]).reshape(-1, 1)
        got_h = picked.astype(f32) * picked_inv
        all_dn = dot_rows(jnp.concatenate(split3(hot_cot) + [got.reshape(-1, out_width)]), w_full)
        got_dn = jnp.where(got_valid, all_dn[3 * HOT_BLOCK:], 0.0)
        got_dx = norm_backward(got_dn, got_h, picked_inv, gain_full)

        my_hot_inv, hot_h = norm_forward(my_hot.astype(f32))
        hot_dn3 = all_dn[:3 * HOT_BLOCK].reshape(3, HOT_BLOCK, width)
        hot_dn = hot_dn3[0] + hot_dn3[1] + hot_dn3[2]
        hot_dx = norm_backward(hot_dn, hot_h, my_hot_inv, gain_full)

        gain_part = jnp.sum(got_dn * got_h, axis=0) + jnp.sum(hot_dn * hot_h, axis=0)
        gain_part = jnp.pad(gain_part.reshape(NUM_DEV, 1, block), ((0, 0), (0, 0), (0, 128 - block)))
        hot_back, gain_back = exchange(
            collect_kernel, [((NUM_DEV, HOT_BLOCK, width), f32), ((NUM_DEV, 1, 128), f32)],
            [(), (NUM_DEV,), (NUM_DEV,), (NUM_DEV,), ()], hot_dx, gain_part, us=30)

        place = ((jnp.arange(vocab_local)[:, None] == pick_ids[None, :]) & got_valid[:, 0][None]).astype(bf16)
        cold_grad = jnp.dot(jnp.concatenate([place] * 3, axis=1), jnp.concatenate(split3(got_dx)), preferred_element_type=f32)

        def ring_sums(_):
            my_ids = tokens[0]

            def fetch(_, carry):
                ids, rows = carry
                mine = ids // vocab_local == me
                own = rounded(embed_shard[jnp.where(mine, ids - me * vocab_local, 0)]).astype(bf16)
                rows = jnp.where(mine[:, None], own, rows)
                return lax.ppermute(ids, AXIS_NAME, ring), lax.ppermute(rows, AXIS_NAME, ring)
            x_rows = lax.fori_loop(0, NUM_DEV, fetch, (my_ids, jnp.zeros((seq, width), bf16)))[1].astype(f32)
            inv_rms, h_rows = norm_forward(x_rows)
            d_normed = dot_rows(cot_mine, w_full)
            d_gain = lax.psum(jnp.sum(d_normed * h_rows, axis=0), AXIS_NAME)
            d_x = norm_backward(d_normed, h_rows, inv_rms, gain_full)

            def hop(_, carry):
                ids, rows, total = carry
                mine = ids // vocab_local == me
                total = total.at[jnp.where(mine, ids - me * vocab_local, vocab_local)].add(rows, mode="drop")
                return lax.ppermute(ids, AXIS_NAME, ring), lax.ppermute(rows, AXIS_NAME, ring), total
            total = lax.fori_loop(0, NUM_DEV, hop, (my_ids, d_x, jnp.zeros(embed_shard.shape, f32)))[2]
            return total, lax.dynamic_slice_in_dim(d_gain, me * block, block)

        top = jnp.where(me == 0, hot_back.reshape(HOT_ROWS, width), cold_grad[:HOT_ROWS])
        sums = (fits, cold_grad.at[:HOT_ROWS].set(top), jnp.sum(gain_back[:, 0, :block], axis=0))
        _, d_embed, d_norm_gain = lax.while_loop(lambda v: jnp.logical_not(v[0]), lambda v: (True,) + ring_sums(v), sums)

        proj = jnp.dot(normed, w_full, preferred_element_type=f32).astype(bf16)[None]
        return (proj[..., :q_width], proj[..., q_width:q_width + kv_width], proj[..., q_width + kv_width:], d_embed, d_norm_gain,
                d_w[:, :q_width], d_w[:, q_width:q_width + kv_width], d_w[:, q_width + kv_width:])

    row_spec = P(AXIS_NAME, None)
    act_spec = P(AXIS_NAME, None, None)
    vec_spec = P(AXIS_NAME)
    return jax.shard_map(local_step, mesh=mesh,
                         in_specs=(row_spec, row_spec, vec_spec, row_spec, row_spec, row_spec, act_spec, act_spec, act_spec),
                         out_specs=(act_spec, act_spec, act_spec, row_spec, vec_spec, row_spec, row_spec, row_spec),
                         check_vma=False)
```

```python
import functools

import jax
import jax.numpy as jnp
from jax import lax
from jax.experimental import pallas as pl
from jax.experimental.pallas import tpu as pltpu
from jax.sharding import PartitionSpec as P

AXIS_NAME = "fsdp"
NUM_DEV = 32
PLANE = 8
NUM_PLANES = 4
HOT_ROWS = 512
HOT_BLOCK = HOT_ROWS // NUM_DEV
ROW_GROUP = 8
CLASSES = ((0, 2, 21, 0), (2, 4, 12, 42), (4, 8, 7, 66), (8, 16, 4, 94), (16, 32, 3, 126))
SEND_GROUPS = 21
RECV_GROUPS = 174
RANK_PAD = 256
PLANE_GROUPS = (12, 4, 3, 3)
PLANE_FIRST = (0, 12, 16, 19)
PLANE_TOTAL = 22
OWN_GROUPS = 7
HELP_GROUPS = (5, 4)
MESH = pl.DeviceIdType.MESH
ANY = pl.BlockSpec(memory_space=pl.ANY)
BF16_MAX = 3.3895313892515355e38


def owner_class(owner):
    for first, last, groups, start in CLASSES:
        if first <= owner < last:
            return groups, start + (owner - first) * groups


def remote(src, dst, send_sem, recv_sem, dev):
    return pltpu.make_async_remote_copy(src_ref=src, dst_ref=dst, send_sem=send_sem, recv_sem=recv_sem,
                                        device_id=(dev,), device_id_type=MESH)


def spread_kernel(src_ref, out_ref, send_sems, recv_sems, own_sem):
    me = lax.axis_index(AXIS_NAME)
    own = pltpu.make_async_copy(src_ref, out_ref.at[me], own_sem)
    own.start()

    @pl.loop(1, NUM_DEV)
    def _(step):
        dev = lax.rem(me + step, NUM_DEV)
        remote(src_ref, out_ref.at[me], send_sems.at[step], recv_sems.at[step], dev).start()

    @pl.loop(1, NUM_DEV)
    def _(step):
        src = lax.rem(me + NUM_DEV - step, NUM_DEV)
        remote(src_ref, out_ref.at[src], send_sems.at[step], recv_sems.at[step], src).wait()

    own.wait()


def slice_kernel(x_ref, out_ref, inv_ref):
    total = jnp.zeros((x_ref.shape[0], 128), jnp.float32)
    low = lax.broadcasted_iota(jnp.int32, (x_ref.shape[0], 128), 1) < 64
    for chip in range(PLANE // 2):
        for half in range(NUM_PLANES // 2):
            at = (PLANE // 2 * 2 * half + chip) * 128
            one = x_ref[:, at:at + 128].astype(jnp.bfloat16).astype(jnp.float32)
            at += PLANE // 2 * 128
            two = x_ref[:, at:at + 128].astype(jnp.bfloat16).astype(jnp.float32)
            total += one * one + two * two
            cols = slice(half * 128, half * 128 + 128)
            out_ref[2 * chip, :, cols] = jnp.where(low, one, pltpu.roll(two, 64, 1)).astype(jnp.bfloat16)
            out_ref[2 * chip + 1, :, cols] = jnp.where(low, pltpu.roll(one, 64, 1), two).astype(jnp.bfloat16)
    inv_rms = lax.rsqrt(jnp.sum(total, axis=1, keepdims=True) / x_ref.shape[1] + 1e-5)
    inv_ref[...] = jnp.broadcast_to(inv_rms, inv_ref.shape)


def column_slices(table, rows, step):
    width = table.shape[1]
    return pl.pallas_call(
        slice_kernel, grid=(rows // step,), in_specs=[pl.BlockSpec((step, width), lambda i: (i, 0))],
        out_specs=[pl.BlockSpec((PLANE, step, width // PLANE), lambda i: (0, i, 0)), pl.BlockSpec((step, 128), lambda i: (i, 0))],
        out_shape=[jax.ShapeDtypeStruct((PLANE, rows, width // PLANE), jnp.bfloat16),
                   jax.ShapeDtypeStruct((rows, 128), jnp.float32)])(table)


def rows_kernel(hot_ref, hot_inv_ref, cold_ref, cold_inv_ref, hot_out, hot_inv_out, cold_out, cold_inv_out,
                hot_send, hot_recv, pass_send, hot_inv_send, hot_inv_recv, send_sems, recv_sems, inv_send, inv_recv):
    me = lax.axis_index(AXIS_NAME)
    pos = lax.rem(me, PLANE)
    plane = me // PLANE

    @pl.when(me == 0)
    def _():
        for dev in range(1, PLANE):
            remote(hot_ref.at[dev], hot_out, hot_send.at[dev], hot_recv, dev).start()
        pltpu.make_async_copy(hot_ref.at[0], hot_out, hot_recv).start()
        for dev in range(1, NUM_DEV):
            remote(hot_inv_ref, hot_inv_out, hot_inv_send.at[dev], hot_inv_recv, dev).start()
        pltpu.make_async_copy(hot_inv_ref, hot_inv_out, hot_inv_recv).start()

    def pass_on():
        pltpu.make_async_copy(hot_out, hot_out, hot_recv).wait()

        @pl.when(plane < NUM_PLANES - 1)
        def _():
            remote(hot_out, hot_out, pass_send, hot_recv, lax.rem(me + PLANE, NUM_DEV)).start()

    @pl.when(plane == 0)
    def _():
        pass_on()

    own_inv = pltpu.make_async_copy(cold_inv_ref.at[plane], cold_inv_out.at[me], inv_recv.at[me])
    own_inv.start()
    for first, last, groups, start in CLASSES:
        @pl.when((me >= first) & (me < last))
        def _():
            src_rows, dst_rows = pl.ds(0, groups), pl.ds(start + (me - first) * groups, groups)
            pltpu.make_async_copy(cold_ref.at[pos, plane, src_rows], cold_out.at[dst_rows], recv_sems.at[me]).start()

            @pl.loop(1, NUM_DEV)
            def _(step):
                dev = lax.rem(me + step, NUM_DEV)
                remote(cold_ref.at[lax.rem(dev, PLANE), dev // PLANE, src_rows], cold_out.at[dst_rows],
                       send_sems.at[step], recv_sems.at[me], dev).start()

    @pl.loop(1, NUM_DEV)
    def _(step):
        dev = lax.rem(me + step, NUM_DEV)
        remote(cold_inv_ref.at[dev // PLANE], cold_inv_out.at[me], inv_send.at[step], inv_recv.at[me], dev).start()

    @pl.when(plane > 0)
    def _():
        pass_on()

    for owner in range(NUM_DEV):
        groups, base = owner_class(owner)
        rows = cold_out.at[pl.ds(base, groups)]
        pltpu.make_async_copy(rows, rows, recv_sems.at[owner]).wait()

    @pl.loop(0, NUM_DEV)
    def _(owner):
        pltpu.make_async_copy(cold_inv_out.at[owner], cold_inv_out.at[owner], inv_recv.at[owner]).wait()

    @pl.loop(1, NUM_DEV)
    def _(step):
        pltpu.make_async_copy(cold_inv_ref.at[0], cold_inv_ref.at[0], inv_send.at[step]).wait()

    for first, last, groups, start in CLASSES:
        @pl.when((me >= first) & (me < last))
        def _():
            rows = cold_ref.at[0, 0, pl.ds(0, groups)]

            @pl.loop(1, NUM_DEV)
            def _(step):
                pltpu.make_async_copy(rows, rows, send_sems.at[step]).wait()

    pltpu.make_async_copy(hot_inv_out, hot_inv_out, hot_inv_recv).wait()

    @pl.when(plane < NUM_PLANES - 1)
    def _():
        pltpu.make_async_copy(hot_out, hot_out, pass_send).wait()

    @pl.when(me == 0)
    def _():
        for dev in range(1, PLANE):
            pltpu.make_async_copy(hot_out, hot_out, hot_send.at[dev]).wait()
        for dev in range(1, NUM_DEV):
            pltpu.make_async_copy(hot_inv_ref, hot_inv_ref, hot_inv_send.at[dev]).wait()


def backs_kernel(n_ref, cot_ref, sum_ref, hot_ref, n_out, cot_out, sum_out, hot_out,
                 n_send, n_recv, cot_send, cot_recv, sum_send, sum_recv, help_send, help_recv, hot_send, hot_recv):
    me = lax.axis_index(AXIS_NAME)
    pos = lax.rem(me, PLANE)
    plane = me // PLANE
    base = me - pos
    own_n = pltpu.make_async_copy(n_ref.at[pos], n_out.at[pos], n_recv.at[0])
    own_n.start()
    for step in range(1, PLANE):
        peer = lax.rem(pos + step, PLANE)
        remote(n_ref.at[peer], n_out.at[pos], n_send.at[step], n_recv.at[step], base + peer).start()

    def move(rows, into, send_sem, recv_sem, dst, dev):
        @pl.when(plane == dst)
        def _():
            pltpu.make_async_copy(rows, into, recv_sem).start()

        @pl.when(plane != dst)
        def _():
            remote(rows, into, send_sem, recv_sem, dev).start()

    for dst, (groups, first) in enumerate(zip(PLANE_GROUPS, PLANE_FIRST)):
        dev = dst * PLANE + pos
        move(sum_ref.at[dst], sum_out.at[plane], sum_send.at[dst], sum_recv.at[plane], dst, dev)
        if dst:
            move(cot_ref.at[pl.ds(first, groups)], cot_out.at[plane, pl.ds(0, groups)], cot_send.at[dst], cot_recv.at[plane], dst, dev)
            continue

        @pl.when(pos < 4)
        def _():
            move(cot_ref.at[pl.ds(0, groups)], cot_out.at[plane, pl.ds(0, groups)], cot_send.at[0], cot_recv.at[plane], 0, dev)

        @pl.when(pos >= 4)
        def _():
            move(cot_ref.at[pl.ds(0, OWN_GROUPS)], cot_out.at[plane, pl.ds(0, OWN_GROUPS)], cot_send.at[0], cot_recv.at[plane], 0, dev)

        start = groups
        for k, more in enumerate(HELP_GROUPS):
            @pl.when((pos >= 4 + 2 * k) & (pos < 6 + 2 * k))
            def _():
                remote(cot_ref.at[pl.ds(OWN_GROUPS, more)], cot_out.at[plane, pl.ds(start, more)],
                       help_send, help_recv.at[k, plane], lax.rem(pos, 2)).start()
            start += more

    @pl.when(me == 0)
    def _():
        pltpu.make_async_copy(hot_ref.at[:, pl.ds(0, HOT_BLOCK)], hot_out, hot_recv).start()

        @pl.loop(1, NUM_DEV)
        def _(dev):
            remote(hot_ref.at[:, pl.ds(dev * HOT_BLOCK, HOT_BLOCK)], hot_out, hot_send.at[dev], hot_recv, dev).start()

    for step in range(1, PLANE):
        peer = lax.rem(pos + PLANE - step, PLANE)
        remote(n_ref.at[peer], n_out.at[peer], n_send.at[step], n_recv.at[step], base + peer).wait()
    own_n.wait()

    def came(ref, sem):
        pltpu.make_async_copy(ref, ref, sem).wait()

    for src in range(NUM_PLANES):
        came(sum_out.at[src], sum_recv.at[src])
        for dst in range(1, NUM_PLANES):
            @pl.when(plane == dst)
            def _():
                came(cot_out.at[src, pl.ds(0, PLANE_GROUPS[dst])], cot_recv.at[src])

        @pl.when((plane == 0) & (pos < 4))
        def _():
            came(cot_out.at[src, pl.ds(0, PLANE_GROUPS[0])], cot_recv.at[src])

        @pl.when((plane == 0) & (pos >= 4))
        def _():
            came(cot_out.at[src, pl.ds(0, OWN_GROUPS)], cot_recv.at[src])

        start = PLANE_GROUPS[0]
        for k, more in enumerate(HELP_GROUPS):
            @pl.when(me < 2)
            def _():
                came(cot_out.at[src, pl.ds(start, more)], help_recv.at[k, src])
            start += more

    for dst, (groups, first) in enumerate(zip(PLANE_GROUPS, PLANE_FIRST)):
        @pl.when(plane != dst)
        def _():
            came(sum_ref.at[dst], sum_send.at[dst])
            if dst:
                came(cot_ref.at[pl.ds(first, groups)], cot_send.at[dst])

    @pl.when((plane != 0) & (pos < 4))
    def _():
        came(cot_ref.at[pl.ds(0, PLANE_GROUPS[0])], cot_send.at[0])

    @pl.when((plane != 0) & (pos >= 4))
    def _():
        came(cot_ref.at[pl.ds(0, OWN_GROUPS)], cot_send.at[0])

    for k, more in enumerate(HELP_GROUPS):
        @pl.when((pos >= 4 + 2 * k) & (pos < 6 + 2 * k))
        def _():
            came(cot_ref.at[pl.ds(OWN_GROUPS, more)], help_send)

    pltpu.make_async_copy(hot_out, hot_out, hot_recv).wait()

    @pl.when(me == 0)
    def _():
        @pl.loop(1, NUM_DEV)
        def _(dev):
            pltpu.make_async_copy(hot_out, hot_out, hot_send.at[dev]).wait()


def collect_kernel(hot_ref, gain_ref, hot_out, gain_out, hot_send, hot_recv, send_sems, recv_sems, own_sem):
    me = lax.axis_index(AXIS_NAME)

    @pl.when(me == 0)
    def _():
        pltpu.make_async_copy(hot_ref, hot_out.at[me], hot_recv.at[0]).start()

    @pl.when(me != 0)
    def _():
        remote(hot_ref, hot_out.at[me], hot_send, hot_recv.at[me], 0).start()

    own = pltpu.make_async_copy(gain_ref.at[me], gain_out.at[me], own_sem)
    own.start()
    copies = []
    for step in range(1, NUM_DEV):
        dev = lax.rem(me + step, NUM_DEV)
        copies.append(remote(gain_ref.at[dev], gain_out.at[me], send_sems.at[step], recv_sems.at[step], dev))
    for copy in copies:
        copy.start()
    for step in range(1, NUM_DEV):
        src = lax.rem(me + NUM_DEV - step, NUM_DEV)
        remote(gain_ref.at[src], gain_out.at[src], send_sems.at[step], recv_sems.at[step], src).wait()
    own.wait()

    @pl.when(me == 0)
    def _():
        for src in range(NUM_DEV):
            pltpu.make_async_copy(hot_ref, hot_out.at[src], hot_recv.at[src]).wait()

    @pl.when(me != 0)
    def _():
        pltpu.make_async_copy(hot_ref, hot_ref, hot_send).wait()


def exchange(kernel, outs, sems, *args, spec=ANY, us=20):
    return pl.pallas_call(
        kernel, cost_estimate=pl.CostEstimate(flops=us * 500_000_000, bytes_accessed=1_000_000, transcendentals=0), out_shape=[jax.ShapeDtypeStruct(*out) for out in outs],
        in_specs=[spec] * len(args), out_specs=[spec] * len(outs),
        scratch_shapes=[pltpu.SemaphoreType.DMA(shape) if shape else pltpu.SemaphoreType.DMA for shape in sems],
        compiler_params=pltpu.CompilerParams(has_side_effects=True))(*args)


def split3(value):
    def top(v):
        return jnp.clip(lax.reduce_precision(v, 8, 7), -BF16_MAX, BF16_MAX)
    high = top(value)
    rest = value - high
    mid = top(rest)
    return [part.astype(jnp.bfloat16) for part in (high, mid, rest - mid)]


def ranks(mask):
    n = mask.shape[-1]
    lower = (jnp.arange(n)[:, None] < jnp.arange(n)[None, :]).astype(jnp.bfloat16)
    return jnp.dot(mask.astype(jnp.bfloat16), lower, preferred_element_type=jnp.float32).astype(jnp.int32)


def dot_rows(a, b):
    return lax.dot_general(a, b, (((1,), (1,)), ((), ())), preferred_element_type=jnp.float32)


def dot_tokens(a, b):
    return lax.dot_general(a, b, (((0,), (0,)), ((), ())), preferred_element_type=jnp.float32)


def rounded(rows):
    return lax.reduce_precision(rows, 8, 7)


def norm_forward(x_rows):
    inv_rms = lax.rsqrt(jnp.mean(x_rows * x_rows, axis=-1, keepdims=True) + 1e-5)
    return inv_rms, x_rows * inv_rms


def norm_backward(d_normed, h_rows, inv_rms, gain_full):
    u_rows = d_normed * gain_full
    return inv_rms * (u_rows - h_rows * jnp.mean(u_rows * h_rows, axis=-1, keepdims=True))


def solution(mesh):
    ring = [(d, (d + 1) % NUM_DEV) for d in range(NUM_DEV)]
    plane_groups = [[z * PLANE + p for p in range(PLANE)] for z in range(NUM_PLANES)]
    column_groups = [[z * PLANE + p for z in range(NUM_PLANES)] for p in range(PLANE)]
    caps = jnp.array([owner_class(d)[0] * ROW_GROUP for d in range(NUM_DEV)], jnp.int32)
    starts = jnp.array([HOT_ROWS + owner_class(d)[1] * ROW_GROUP for d in range(NUM_DEV)], jnp.int32)
    slot_plane = jnp.array([z for z, g in enumerate(PLANE_GROUPS) for _ in range(g * ROW_GROUP)], jnp.int32)
    slot_rank = jnp.array([c for g in PLANE_GROUPS for c in range(g * ROW_GROUP)], jnp.int32)

    def local_step(tokens, embed_shard, gain_shard, wq_shard, wk_shard, wv_shard, d_query, d_key, d_value):
        vocab_local, width = embed_shard.shape
        seq = tokens.shape[1]
        q_width, kv_width = wq_shard.shape[1], wk_shard.shape[1]
        out_width = q_width + 2 * kv_width
        block = width // NUM_DEV
        part, plane_seq, slot_rows = width // PLANE, PLANE * seq, SEND_GROUPS * ROW_GROUP
        me = lax.axis_index(AXIS_NAME)
        pos, plane = me % PLANE, me // PLANE
        bf16, f32 = jnp.bfloat16, jnp.float32

        cot_mine = jnp.concatenate([d_query[0], d_key[0], d_value[0]], axis=1)
        cot_plane = lax.all_gather(cot_mine, AXIS_NAME, axis=0, tiled=True, axis_index_groups=plane_groups)
        message = jnp.concatenate([tokens.astype(f32), jnp.pad(gain_shard, (0, 128 - block))[None]], axis=1)
        spread, = exchange(spread_kernel, [((NUM_DEV, 1, seq + 128), f32)], [(NUM_DEV,), (NUM_DEV,), ()], message)
        spread, wq_shard, wk_shard, wv_shard = lax.optimization_barrier((spread, wq_shard, wk_shard, wv_shard))
        w_mine = jnp.concatenate([wq_shard.astype(bf16), wk_shard.astype(bf16), wv_shard.astype(bf16)], axis=1)
        w_full = lax.all_gather(w_mine, AXIS_NAME, axis=0, tiled=True)

        all_tokens = spread[:, 0, :seq].astype(jnp.int32)
        gain_full = spread[:, 0, seq:seq + block].reshape(1, width)
        my_gain = gain_full.reshape(NUM_PLANES, PLANE, block)
        my_gain = lax.dynamic_index_in_dim(my_gain, pos, 1, keepdims=False).reshape(1, part)

        all_owner = all_tokens // vocab_local
        all_cold = all_tokens >= HOT_ROWS
        counts = jnp.sum((all_owner[:, :, None] == jnp.arange(NUM_DEV)) & all_cold[:, :, None], axis=1, dtype=jnp.int32)
        fits = jnp.all(counts.reshape(NUM_PLANES, PLANE, NUM_DEV).sum(1) <= caps[None])

        from_mine = ((all_owner == me) & all_cold).reshape(NUM_PLANES, plane_seq)
        from_rank = ranks(from_mine)
        slots = jnp.arange(slot_rows)
        picks = (from_rank[:, None, :] == slots[None, :, None]) & from_mine[:, None, :]
        local_ids = (all_tokens - me * vocab_local).reshape(NUM_PLANES, 1, plane_seq)
        pick_ids = jnp.sum(jnp.where(picks, local_ids, 0), axis=2).reshape(-1)
        pick = (pick_ids[:, None] == jnp.arange(vocab_local)[None]).astype(bf16)
        picked = jnp.dot(pick, embed_shard.astype(bf16), preferred_element_type=f32).astype(bf16)
        picked = lax.optimization_barrier(picked)
        cold_slices, picked_inv = column_slices(picked, NUM_PLANES * slot_rows, slot_rows)
        hot_slices, hot_inv_mine = column_slices(embed_shard, HOT_ROWS, 128)
        picked_inv = picked_inv[:, :1]
        hot_cols, hot_inv, cold_cols, cold_inv = exchange(
            rows_kernel,
            [((HOT_ROWS, part), bf16), ((1, HOT_ROWS), f32), ((RECV_GROUPS, ROW_GROUP, part), bf16), ((NUM_DEV, 1, RANK_PAD), f32)],
            [(PLANE,), (), (), (NUM_DEV,), (), (NUM_DEV,), (NUM_DEV,), (NUM_DEV,), (NUM_DEV,)],
            hot_slices, hot_inv_mine[:, 0].reshape(1, HOT_ROWS),
            cold_slices.reshape(PLANE, NUM_PLANES, SEND_GROUPS, ROW_GROUP, part),
            jnp.pad(picked_inv.reshape(NUM_PLANES, 1, slot_rows), ((0, 0), (0, 0), (0, RANK_PAD - slot_rows))), us=50)

        plane_tokens = lax.dynamic_slice_in_dim(all_tokens, plane * PLANE, PLANE, 0).reshape(plane_seq)
        plane_owner = plane_tokens // vocab_local
        plane_cold = plane_tokens >= HOT_ROWS
        of_owner = plane_owner[None] == jnp.arange(NUM_DEV)[:, None]
        plane_rank = jnp.sum(jnp.where(of_owner, ranks(of_owner & plane_cold[None]), 0), axis=0)

        def fetched_rows(_):
            start = jnp.sum(jnp.where(of_owner, starts[:, None], 0), axis=0)
            place = jnp.where(plane_cold, start + plane_rank, plane_tokens)
            table = jnp.concatenate([hot_cols, cold_cols.reshape(-1, part)])
            select = (place[:, None] == jnp.arange(table.shape[0])).astype(bf16)
            x_cols = jnp.dot(select, table, preferred_element_type=f32)
            by_owner = jnp.dot(of_owner.astype(bf16).T, jnp.concatenate(split3(cold_inv[:, 0]), axis=1), preferred_element_type=f32)
            by_owner = by_owner.reshape(plane_seq, 3, RANK_PAD)
            by_owner = by_owner[:, 0] + by_owner[:, 1] + by_owner[:, 2]
            cold_part = jnp.sum(jnp.where(plane_rank[:, None] == jnp.arange(RANK_PAD), by_owner, 0.0), axis=1, keepdims=True)
            hot_part = jnp.sum(jnp.where(plane_tokens[:, None] == jnp.arange(HOT_ROWS), hot_inv, 0.0), axis=1, keepdims=True)
            return x_cols, jnp.where(plane_cold[:, None], cold_part, hot_part)

        def ring_cols(_):
            def hop(step, carry):
                ids, cols, inv = carry
                mine = ids // vocab_local == me
                own = rounded(embed_shard[jnp.where(mine, ids - me * vocab_local, 0)]).astype(bf16)
                own_inv = norm_forward(own.astype(f32))[0]
                own = own.reshape(plane_seq, NUM_PLANES, PLANE, block)
                own = lax.dynamic_index_in_dim(own, (me + NUM_DEV - step) % PLANE, 2, keepdims=False).reshape(plane_seq, part)
                cols = jnp.where(mine[:, None], own, cols)
                inv = jnp.where(mine[:, None], own_inv, inv)
                return tuple(lax.ppermute(v, AXIS_NAME, ring) for v in (ids, cols, inv))
            start = (plane_tokens, jnp.zeros((plane_seq, part), bf16), jnp.zeros((plane_seq, 1), f32))
            _, cols, inv = lax.fori_loop(0, NUM_DEV, hop, start)
            return cols.astype(f32), inv

        x_cols, x_inv = lax.cond(fits, fetched_rows, ring_cols, None)
        n_plane = (x_cols * x_inv * my_gain).astype(bf16)

        parts = dot_tokens(n_plane, cot_plane)
        parts, n_plane, plane_tokens, pick_ids, from_mine, plane_rank = lax.optimization_barrier(
            (parts, n_plane, plane_tokens, pick_ids, from_mine, plane_rank))
        d_w = lax.psum_scatter(parts, AXIS_NAME, scatter_dimension=0, tiled=True, axis_index_groups=column_groups)

        places = jnp.arange(NUM_PLANES * HOT_BLOCK)
        hot_ids = (places // HOT_BLOCK * PLANE + pos) * HOT_BLOCK + places % HOT_BLOCK
        helped = (pos >= 4) & (slot_plane == 0) & (slot_rank >= OWN_GROUPS * ROW_GROUP)
        first_rank = (PLANE_GROUPS[0] - OWN_GROUPS) * ROW_GROUP + jnp.where(pos >= 6, HELP_GROUPS[0] * ROW_GROUP, 0)
        pack_owner = jnp.where(helped, pos % 2, slot_plane * PLANE + pos)
        pack_rank = jnp.where(helped, slot_rank + first_rank, slot_rank)
        keys = jnp.where(plane_cold, HOT_ROWS + plane_owner * plane_seq + plane_rank, plane_tokens)
        slot_keys = jnp.concatenate([hot_ids, HOT_ROWS + pack_owner * plane_seq + pack_rank])
        moved = dot_tokens((keys[:, None] == slot_keys[None]).astype(bf16), cot_plane)
        cot_sums = moved[:NUM_PLANES * HOT_BLOCK].reshape(NUM_PLANES, HOT_BLOCK, out_width)
        packed = moved[NUM_PLANES * HOT_BLOCK:].astype(bf16)

        n_cols, got, hot_sums, my_hot = exchange(
            backs_kernel,
            [((PLANE, seq, part), bf16), ((NUM_PLANES, SEND_GROUPS, ROW_GROUP, out_width), bf16),
             ((NUM_PLANES, HOT_BLOCK, out_width), f32), ((PLANE, HOT_BLOCK, part), bf16)],
            [(PLANE,), (PLANE,)] + [(NUM_PLANES,)] * 4 + [(), (2, NUM_PLANES), (NUM_DEV,), ()],
            n_plane.reshape(PLANE, seq, part), packed.reshape(PLANE_TOTAL, ROW_GROUP, out_width), cot_sums, hot_slices, us=40)
        hot_cot = jnp.sum(hot_sums, axis=0)
        my_hot = my_hot.reshape(PLANE, HOT_BLOCK, NUM_PLANES, block).transpose(1, 2, 0, 3).reshape(HOT_BLOCK, width)
        normed = n_cols.reshape(PLANE, seq, NUM_PLANES, block).transpose(1, 2, 0, 3).reshape(seq, width)
        my_cap = jnp.sum(jnp.where(me == jnp.arange(NUM_DEV), caps, 0))
        got_valid = ((slots[None] < jnp.sum(from_mine, axis=1, dtype=jnp.int32)[:, None]) & (slots < my_cap)[None]).reshape(-1, 1)
        got_h = picked.astype(f32) * picked_inv
        all_dn = dot_rows(jnp.concatenate(split3(hot_cot) + [got.reshape(-1, out_width)]), w_full)
        got_dn = jnp.where(got_valid, all_dn[3 * HOT_BLOCK:], 0.0)
        got_dx = norm_backward(got_dn, got_h, picked_inv, gain_full)

        my_hot_inv, hot_h = norm_forward(my_hot.astype(f32))
        hot_dn3 = all_dn[:3 * HOT_BLOCK].reshape(3, HOT_BLOCK, width)
        hot_dn = hot_dn3[0] + hot_dn3[1] + hot_dn3[2]
        hot_dx = norm_backward(hot_dn, hot_h, my_hot_inv, gain_full)

        gain_part = jnp.sum(got_dn * got_h, axis=0) + jnp.sum(hot_dn * hot_h, axis=0)
        gain_part = jnp.pad(gain_part.reshape(NUM_DEV, 1, block), ((0, 0), (0, 0), (0, 128 - block)))
        place_ids = jnp.where(got_valid[:, 0], pick_ids, vocab_local)
        place = (jnp.arange(vocab_local)[:, None] == jnp.concatenate([place_ids] * 3)[None]).astype(bf16)
        cold_grad = jnp.dot(place, jnp.concatenate(split3(got_dx)), preferred_element_type=f32)
        hot_dx, gain_part, cold_grad = lax.optimization_barrier((hot_dx, gain_part, cold_grad))
        hot_back, gain_back = exchange(
            collect_kernel, [((NUM_DEV, HOT_BLOCK, width), f32), ((NUM_DEV, 1, 128), f32)],
            [(), (NUM_DEV,), (NUM_DEV,), (NUM_DEV,), ()], hot_dx, gain_part, us=30)

        def ring_sums(_):
            my_ids = tokens[0]

            def fetch(_, carry):
                ids, rows = carry
                mine = ids // vocab_local == me
                own = rounded(embed_shard[jnp.where(mine, ids - me * vocab_local, 0)]).astype(bf16)
                rows = jnp.where(mine[:, None], own, rows)
                return lax.ppermute(ids, AXIS_NAME, ring), lax.ppermute(rows, AXIS_NAME, ring)
            x_rows = lax.fori_loop(0, NUM_DEV, fetch, (my_ids, jnp.zeros((seq, width), bf16)))[1].astype(f32)
            inv_rms, h_rows = norm_forward(x_rows)
            d_normed = dot_rows(cot_mine, w_full)
            d_gain = lax.psum(jnp.sum(d_normed * h_rows, axis=0), AXIS_NAME)
            d_x = norm_backward(d_normed, h_rows, inv_rms, gain_full)

            def hop(_, carry):
                ids, rows, total = carry
                mine = ids // vocab_local == me
                total = total.at[jnp.where(mine, ids - me * vocab_local, vocab_local)].add(rows, mode="drop")
                return lax.ppermute(ids, AXIS_NAME, ring), lax.ppermute(rows, AXIS_NAME, ring), total
            total = lax.fori_loop(0, NUM_DEV, hop, (my_ids, d_x, jnp.zeros(embed_shard.shape, f32)))[2]
            return total, lax.dynamic_slice_in_dim(d_gain, me * block, block)

        top = jnp.where(me == 0, hot_back.reshape(HOT_ROWS, width), cold_grad[:HOT_ROWS])
        sums = (fits, cold_grad.at[:HOT_ROWS].set(top), jnp.sum(gain_back[:, 0, :block], axis=0))
        _, d_embed, d_norm_gain = lax.while_loop(lambda v: jnp.logical_not(v[0]), lambda v: (True,) + ring_sums(v), sums)

        proj = jnp.dot(normed, w_full, preferred_element_type=f32).astype(bf16)[None]
        return (proj[..., :q_width], proj[..., q_width:q_width + kv_width], proj[..., q_width + kv_width:], d_embed, d_norm_gain,
                d_w[:, :q_width], d_w[:, q_width:q_width + kv_width], d_w[:, q_width + kv_width:])

    row_spec = P(AXIS_NAME, None)
    act_spec = P(AXIS_NAME, None, None)
    vec_spec = P(AXIS_NAME)
    return jax.shard_map(local_step, mesh=mesh,
                         in_specs=(row_spec, row_spec, vec_spec, row_spec, row_spec, row_spec, act_spec, act_spec, act_spec),
                         out_specs=(act_spec, act_spec, act_spec, row_spec, vec_spec, row_spec, row_spec, row_spec),
                         check_vma=False)
```
